32 devices in a mesh: dom: 16 (over z, x, core), feat: 2 (over y).
Axes of the slice: x: 2, y: 2, z: 4, core: 2. Of those that a mesh axis runs over, the one named last changes fastest.
Arguments:
- features: bfloat16 [512, 49152], P('feat', 'dom'), may hold values from -6 to 6
- weights: bfloat16 [2, 512, 512], replicated, may hold values from -0.1875 to 0.1875
- tile_values: bfloat16 [1152, 128, 128], P('dom'), may hold values from 0 to 0.099609375
- tile_blocks: int32 [1152, 2], P('dom'), may hold values from 0 to 25
- tile_counts: int32 [16], P('dom'), may hold values from 36 to 72
- replica: int32 [16, 16, 16], P('dom'), may hold values from -1 to 3071, as said below
- cotangent: bfloat16 [512, 49152], P(None, ('dom', 'feat')), may hold values from -6 to 6
Outputs:
- output: bfloat16 [512, 49152], P(None, ('dom', 'feat'))
- feature_grad: bfloat16 [512, 49152], P('feat', 'dom')
- weight_grad: float32 [2, 512, 512], P(None, 'feat')
The draws below stay inside these ranges and needn't reach their ends.
Inputs may be any that keep to these rules, and one draw needn't show every extreme that they name: `tile_blocks`: column 0 names a tile's source block and column 1 its destination block. replica[q, p, k] is the master slot on partition q of the vertex in mirror slot q * 16 + k of partition p, or -1 for an unused slot; the used slots of a pair (q, p) come first; no partition mirrors its own masters; each master partition fills all 16 slots toward at least one partition.
All inputs are finite; a program needn't handle non-finite values.
Results may differ from the reference program's by a relative error of at most 0.0058.
Values may be sent and summed in bfloat16 or wider, within the bound.
No kernel may reach another device: no remote copies, remote signals or barrier semaphores. Data moves between devices by JAX's collectives and lax.ppermute only.
A program may use at most 64 MiB of HBM per device.

```python
import jax
import jax.numpy as jnp
from jax import lax

D = 512
TILE = 128
MAST = 3072
SLOTS = 16
TILES = 72
VERT = 49152
NB = 26
N_DOM = 16


def draw_replica(key, part):
    base = jax.random.fold_in(key, 11)
    key_slots, key_used = jax.random.split(base, 2)
    slot_draw = jax.random.randint(key_slots, (N_DOM, N_DOM, SLOTS), 0, MAST)
    used_count = jax.random.randint(key_used, (N_DOM, N_DOM, 1), SLOTS // 4, SLOTS + 1)
    master_part = jnp.arange(N_DOM)[:, None, None]
    mirror_part = jnp.arange(N_DOM)[None, :, None]
    used_count = jnp.where(mirror_part == (master_part * 7 + 3) % N_DOM, SLOTS, used_count)
    used_count = jnp.where(mirror_part == master_part, 0, used_count)
    position = jnp.arange(SLOTS)[None, None, :]
    return jnp.where(position < used_count, slot_draw, -1).astype(jnp.int32)


def place_ends(values, own_key, low, high):
    dims = values.shape
    place = [jax.random.randint(jax.random.fold_in(own_key, axis), (), 0, dims[axis]) for axis in range(len(dims))]
    values = values.at[tuple(place)].set(low)
    longest = dims.index(max(dims))
    place[longest] = (place[longest] + 1) % dims[longest]
    return values.at[tuple(place)].set(high)


def strengthened(values, key, source, target, parts, factor):
    def block_of(dim):
        return (jnp.arange(values.shape[dim]) // (values.shape[dim] // parts)).reshape((-1,) + (1,) * (values.ndim - 1 - dim))

    one_side = jax.random.permutation(key, parts)[block_of(target)]
    far = (block_of(target) + parts // 2) % parts
    return jnp.where((block_of(source) == one_side) | (block_of(source) == far), factor * values, values)


def block_levels(own_key, shape, shards, smallest, largest):
    level, own = 1.0, jax.random.fold_in(own_key, 6)
    for dim, blocks in shards:
        heights = jnp.exp(jax.random.uniform(jax.random.fold_in(own, dim), (blocks,), jnp.float32, smallest / len(shards), largest / len(shards)))
        level = level * jnp.repeat(heights, shape[dim] // blocks).reshape([-1 if axis == dim else 1 for axis in range(len(shape))])
    return level


def scatter_about(own_key, shape, width, limit, pieces=(), kind=jnp.bfloat16):
    array = width * jax.random.normal(own_key, shape, jnp.float32)
    if pieces:
        array = array * block_levels(own_key, shape, pieces, -0.22, 0.18)
    return jnp.clip(array, -limit, limit).astype(kind)


def gaussian_with(rng, dims, width, reach, pieces, heavy, kind=jnp.bfloat16):
    array = width * jax.random.normal(rng, dims, jnp.float32)
    if pieces:
        array = array * block_levels(rng, dims, pieces, -0.22, 0.18)
    return jnp.clip(strengthened(array, jax.random.fold_in(rng, 3), *heavy), -reach, reach).astype(kind)


def setup_inputs(seed: int = 0) -> dict:
    keys = jax.random.split(jax.random.key(seed), 8)
    return {
        "features": gaussian_with(keys[0], (D, VERT), 1.0, 6.0, ((0, 2), (1, 16)), (1, 0, 16, 2.0)),
        "weights": scatter_about(keys[1], (2, D, D), (2 * D) ** -0.5, 0.1875),
        "tile_values": jnp.clip(0.099609375 * jax.random.uniform(keys[2], (N_DOM * TILES, TILE, TILE), jnp.float32) ** block_levels(keys[2], (N_DOM * TILES, TILE, TILE), ((0, 16),), -0.2, 0.2), 0.0, 0.099609375).astype(jnp.bfloat16),
        "tile_blocks": place_ends(jax.random.randint(keys[3], (N_DOM * TILES, 2), 0, NB), jax.random.fold_in(keys[3], 1), 0, NB - 1).astype(jnp.int32),
        "tile_counts": place_ends(jax.random.randint(keys[4], (N_DOM,), TILES // 2, TILES + 1), jax.random.fold_in(keys[4], 1), TILES // 2, TILES).astype(jnp.int32),
        "replica": draw_replica(jax.random.fold_in(keys[7], 71), 0),
        "cotangent": scatter_about(keys[6], (D, VERT), 1.0, 6.0, ((1, 32),)),
    }


def spread_field(values_in, tile_values, tile_blocks, tile_live, replica, forward):
    nblocks = (MAST + N_DOM * SLOTS) // TILE
    vertices = MAST * N_DOM
    edge_values = tile_values.reshape(N_DOM, TILES, TILE, TILE).astype(jnp.float32)
    block_pairs = tile_blocks.reshape(N_DOM, TILES, 2)
    feat_width = values_in.shape[0]

    def advance(summed, source):
        rows_here = replica[:, source, :]
        slot_used = (rows_here >= 0).reshape(-1)
        master_base = (jnp.arange(N_DOM, dtype=jnp.int32) * MAST)[:, None]
        global_cols = (master_base + jnp.where(rows_here >= 0, rows_here, 0)).reshape(-1).astype(jnp.int32)
        mirrors = jnp.where(slot_used[None, :], jnp.take(values_in, global_cols, axis=1), jnp.zeros((), values_in.dtype))
        own_cols = lax.dynamic_slice_in_dim(values_in, (source * MAST).astype(jnp.int32), MAST, 1)
        local_cols = jnp.concatenate([own_cols, mirrors], 1).astype(jnp.float32).reshape(feat_width, nblocks, TILE)
        source_blocks = block_pairs[source, :, 0]
        target_blocks = block_pairs[source, :, 1]
        if forward:
            picked = jnp.take(local_cols, source_blocks, axis=1)
            contrib = jnp.einsum('fts,tsd->ftd', picked, edge_values[source], precision=lax.Precision.HIGHEST)
            segment = target_blocks
        else:
            picked = jnp.take(local_cols, target_blocks, axis=1)
            contrib = jnp.einsum('ftd,tsd->fts', picked, edge_values[source], precision=lax.Precision.HIGHEST)
            segment = source_blocks
        contrib = contrib * tile_live[source][None, :, None]
        partial_value = jax.ops.segment_sum(jnp.moveaxis(contrib, 1, 0), segment, num_segments=nblocks)
        partial_value = jnp.moveaxis(partial_value, 0, 1).reshape(feat_width, nblocks * TILE)
        target_cols = jnp.concatenate([source * MAST + jnp.arange(MAST, dtype=jnp.int32),
                                       jnp.where(slot_used, global_cols, vertices).astype(jnp.int32)])
        summed = summed.at[:, target_cols].add(partial_value, mode="drop")
        return summed, None

    summed, _ = lax.scan(advance, jnp.zeros((feat_width, vertices), jnp.float32), jnp.arange(N_DOM, dtype=jnp.int32))
    return summed


def reference(features, weights, tile_values, tile_blocks, tile_counts, replica, cotangent):
    tile_live = (jnp.arange(TILES, dtype=jnp.int32)[None, :] < tile_counts[:, None]).astype(jnp.float32)
    aggregate = spread_field(features, tile_values, tile_blocks, tile_live, replica, True).astype(jnp.bfloat16)
    w_self = weights[0]
    w_neigh = weights[1]
    preact = jnp.dot(w_self.T, features, preferred_element_type=jnp.float32) + jnp.dot(w_neigh.T, aggregate, preferred_element_type=jnp.float32)
    sigmoid_z = jax.nn.sigmoid(preact)
    output = (preact * sigmoid_z).astype(jnp.bfloat16)
    slope = sigmoid_z * (1.0 + preact * (1.0 - sigmoid_z))
    pre_grad = (cotangent.astype(jnp.float32) * slope).astype(jnp.bfloat16)
    weight_grad = jnp.stack([jnp.dot(features, pre_grad.T, preferred_element_type=jnp.float32),
                             jnp.dot(aggregate, pre_grad.T, preferred_element_type=jnp.float32)])
    self_grad = jnp.dot(w_self, pre_grad, preferred_element_type=jnp.float32).astype(jnp.bfloat16)
    agg_grad = jnp.dot(w_neigh, pre_grad, preferred_element_type=jnp.float32).astype(jnp.bfloat16)
    back_terms = spread_field(agg_grad, tile_values, tile_blocks, tile_live, replica, False)
    feature_grad = (self_grad.astype(jnp.float32) + back_terms).astype(jnp.bfloat16)
    return (output, feature_grad, weight_grad)
```

```python
import functools

import jax
import jax.numpy as jnp
from jax import lax
from jax.experimental import pallas as pl
from jax.experimental.pallas import tpu as pltpu
from jax.sharding import PartitionSpec as P

BF = jnp.bfloat16
F32 = jnp.float32
GROUP = 4


def dot(a, b, ca=1, cb=0):
    return lax.dot_general(a, b, (((ca,), (cb,)), ((), ())), preferred_element_type=F32)


def eye(n):
    rows = lax.broadcasted_iota(jnp.int32, (n, n), 0)
    cols = lax.broadcasted_iota(jnp.int32, (n, n), 1)
    return jnp.where(rows == cols, 1.0, 0.0).astype(BF)


def onehot(slots, start, width):
    cols = lax.broadcasted_iota(jnp.int32, (slots.shape[0], width), 1) + start
    return jnp.where(cols == slots, 1.0, 0.0).astype(BF)


def full(shape):
    return pl.BlockSpec(shape, lambda *_: (0,) * len(shape))


SMEM = pl.BlockSpec(memory_space=pltpu.SMEM)
ANY = pl.BlockSpec(memory_space=pl.ANY)


def cost(flops, nbytes):
    return pl.CostEstimate(flops=int(flops), bytes_accessed=int(nbytes), transcendentals=0)


def block_of(n):
    return next(b for b in (512, 256, 128) if n % b == 0)


def list_tiles(blocks, count, lists, source_col, chosen, trash):
    tiles, sources, targets = lists

    def step(t, n):
        source = blocks[t, source_col]
        tiles[n] = t
        sources[n] = source
        targets[n] = blocks[t, 1 - source_col]
        return n + chosen(source).astype(jnp.int32)

    n = lax.fori_loop(0, count, step, jnp.int32(0))
    for u in range(GROUP):
        tiles[n + u] = 0
        sources[n + u] = -1
        targets[n + u] = trash
    return n


def run_tiles(n, lists, values, tile_dim, source_of, acc, tile):
    tiles, sources, targets = lists

    def step(g, _):
        for u in range(GROUP):
            at = g * GROUP + u
            picked = source_of(sources[at])
            part = dot(picked, values[tiles[at]], 1, tile_dim)
            col = pl.ds(pl.multiple_of(targets[at] * tile, tile), tile)
            acc[:, col] += part
        return 0

    lax.fori_loop(0, (n + GROUP - 1) // GROUP, step, 0)


def column(ref, block, tile):
    at = pl.multiple_of(jnp.maximum(block, 0) * tile, tile)
    return ref[:, pl.ds(at, tile)]


def gather_kernel(x_ref, rep_ref, out_ref, acc):
    i = pl.program_id(0)
    width = x_ref.shape[1]

    @pl.when(i == 0)
    def _():
        acc[...] = jnp.zeros_like(acc)

    acc[...] += dot(onehot(rep_ref[...], i * width, width), x_ref[...], 1, 1)

    @pl.when(i == pl.num_programs(0) - 1)
    def _():
        out_ref[...] = acc[...].astype(BF).reshape(out_ref.shape)


def spread_own(nb_own, tile, blocks, count, x_ref, values, acc, tiles, sources, targets):
    lists = (tiles, sources, targets)
    n = list_tiles(blocks, count[0], lists, 0, lambda s: s < nb_own, acc.shape[1] // tile - 1)
    acc[...] = jnp.zeros_like(acc)
    run_tiles(n, lists, values, 0, lambda s: column(x_ref, s, tile), acc, tile)


def spread_mirrors(nf, nc, nb_own, tile, blocks, count, mirrors, values, acc_in, *rest):
    own_ref, push_ref = rest[0], rest[1]
    sends = rest[2 : 2 + (nf - 1) * nc]
    acc, x_mirror, tiles, sources, targets = rest[2 + (nf - 1) * nc :]
    lists = (tiles, sources, targets)
    h = lax.axis_index("feat")
    feats, width = own_ref.shape
    masters = nb_own * tile
    slots = x_mirror.shape[1]
    acc[...] = acc_in[...]
    rows = mirrors[...].reshape(slots, feats)
    x_mirror[...] = dot(eye(feats), rows, 1, 1).astype(BF)
    n = list_tiles(blocks, count[0], lists, 0, lambda s: s >= nb_own, acc.shape[1] // tile - 1)
    run_tiles(n, lists, values, 0, lambda s: column(x_mirror, s - nb_own, tile), acc, tile)
    partial = acc[:, masters : masters + slots].astype(BF)
    push = dot(eye(slots), partial, 1, 1).astype(BF)
    push = push.reshape(push_ref.shape[0], push_ref.shape[2], feats)
    for f in range(nf):
        push_ref[:, f] = push
    own_ref[...] = acc[:, pl.ds(pl.multiple_of(h * width, 128), width)]
    part = width // nc
    for j in range(1, nf):
        for c in range(nc):
            at = pl.multiple_of(lax.rem(h + j, nf) * width + c * part, 128)
            sends[(j - 1) * nc + c][...] = acc[:, pl.ds(at, part)].astype(BF)


def dense_kernel(nf, first, nalias, start, *refs):
    rep_ref, wt_ref, w1_ref, inc_ref, cot_ref, pay_in = refs[:6]
    xs = refs[6 : 6 + nf]
    parts = refs[6 + nf : 6 + 2 * nf]
    refs = refs[6 + 2 * nf + nalias :]
    rows_ref, out_ref, g_ref, own_ref, pay_ref = refs[:5]
    sends = refs[5 : 4 + nf]
    ag, pay = refs[4 + nf :]
    h = lax.axis_index("feat")
    i = pl.program_id(0)
    feats, width = own_ref.shape
    wide = out_ref.shape[0]
    slots = rep_ref.shape[0]
    per_device, offset = start
    pick = onehot(rep_ref[...], h * per_device + offset + i * width, width)
    for j in range(nf):
        f = lax.rem(h - j + nf, nf)
        at = pl.multiple_of(f * feats, feats)
        inc = inc_ref[:, f].reshape(slots, feats)
        total = parts[j][...].astype(F32) + dot(inc, pick, 0, 0)
        rows_ref[pl.ds(at, feats), :] = xs[j][...]
        rows_ref[pl.ds(wide + at, feats), :] = total.astype(BF)
    z = dot(wt_ref[...], rows_ref[...])
    s = jax.nn.sigmoid(z)
    out_ref[...] = (z * s).astype(BF)
    g = (cot_ref[...].astype(F32) * (s * (1.0 + z * (1.0 - s)))).astype(BF)
    g_ref[...] = g
    ag[...] = dot(w1_ref[...], g).astype(BF)
    own_ref[...] = ag[pl.ds(pl.multiple_of(h * feats, feats), feats), :]
    for j in range(1, nf):
        at = pl.multiple_of(lax.rem(h + j, nf) * feats, feats)
        sends[j - 1][...] = ag[pl.ds(at, feats), :]

    @pl.when(i == 0)
    def _():
        pay[...] = jnp.zeros_like(pay)

    pay[...] += dot(pick, ag[...], 1, 1)

    @pl.when(i == pl.num_programs(0) - 1)
    def _():
        for f in range(nf):
            mine = pay[:, f * feats : (f + 1) * feats]
            mine = mine.reshape(pay_ref.shape[0], pay_ref.shape[2], feats)
            if not first:
                mine = mine + pay_in[:, f].astype(F32)
            pay_ref[:, f] = mine.astype(BF)


def self_kernel(nf, w0_ref, g_ref, own_ref, *rest):
    sends, sg = rest[:-1], rest[-1]
    h = lax.axis_index("feat")
    feats = own_ref.shape[0]
    sg[...] = dot(w0_ref[...], g_ref[...]).astype(BF)
    own_ref[...] = sg[pl.ds(pl.multiple_of(h * feats, feats), feats), :]
    for j in range(1, nf):
        at = pl.multiple_of(lax.rem(h + j, nf) * feats, feats)
        sends[j - 1][...] = sg[pl.ds(at, feats), :]


def weight_kernel(nf, rows_ref, g_ref, out_ref, acc):
    h = lax.axis_index("feat")
    i = pl.program_id(0)
    wide = g_ref.shape[0]
    feats = wide // nf

    @pl.when(i == 0)
    def _():
        acc[...] = jnp.zeros_like(acc)

    acc[...] += dot(rows_ref[...], g_ref[...], 1, 1)

    @pl.when(i == pl.num_programs(0) - 1)
    def _():
        for j in range(nf):
            at = pl.multiple_of(lax.rem(h + j, nf) * feats, feats)
            out_ref[j, :feats] = acc[pl.ds(at, feats), :].astype(BF)
            out_ref[j, feats:] = acc[pl.ds(wide + at, feats), :].astype(BF)


def back_own(nf, tile, blocks, count, x_ref, values, acc, tiles, sources, targets):
    lists = (tiles, sources, targets)
    h = lax.axis_index("feat")
    nbv = x_ref.shape[1] // tile
    low = h * nbv
    n = list_tiles(
        blocks,
        count[0],
        lists,
        1,
        lambda s: jnp.logical_and(s >= low, s < low + nbv),
        acc.shape[1] // tile - 1,
    )
    acc[...] = jnp.zeros_like(acc)
    run_tiles(n, lists, values, 1, lambda s: column(x_ref, s - low, tile), acc, tile)


def back_rest(nf, nc, tile, blocks, count, mirrors, values, acc_in, *rest):
    recvs = rest[: (nf - 1) * nc]
    own_acc, push_ref, acc, x_all, tiles, sources, targets = rest[(nf - 1) * nc :]
    lists = (tiles, sources, targets)
    h = lax.axis_index("feat")
    feats, masters = own_acc.shape
    slots = mirrors.shape[0] * mirrors.shape[2]
    width = masters // nf
    part = width // nc
    nbv = width // tile
    low = h * nbv
    acc[...] = acc_in[...]
    total = mirrors[:, 0].astype(F32)
    for f in range(1, nf):
        total = total + mirrors[:, f].astype(F32)
    rows = total.astype(BF).reshape(slots, feats)
    x_all[:, masters:] = dot(eye(feats), rows, 1, 1).astype(BF)
    for j in range(1, nf):
        for c in range(nc):
            at = pl.multiple_of(lax.rem(h - j + nf, nf) * width + c * part, 128)
            x_all[:, pl.ds(at, part)] = recvs[(j - 1) * nc + c][...]
    n = list_tiles(
        blocks,
        count[0],
        lists,
        1,
        lambda s: jnp.logical_or(s < low, s >= low + nbv),
        acc.shape[1] // tile - 1,
    )
    filler = masters // tile

    def source_of(s):
        return column(x_all, jnp.where(s < 0, filler, s), tile)

    run_tiles(n, lists, values, 1, source_of, acc, tile)
    partial = acc[:, masters : masters + slots].astype(BF)
    push_ref[...] = dot(eye(slots), partial, 1, 1).astype(BF).reshape(push_ref.shape)
    own_acc[...] = acc[:, :masters]


def final_kernel(nf, rep_ref, inc_ref, acc_ref, own_ref, *rest):
    recvs, out_ref = rest[: nf - 1], rest[nf - 1]
    h = lax.axis_index("feat")
    feats, width = own_ref.shape
    slots = rep_ref.shape[0]
    inc = inc_ref[...].reshape(slots, feats)
    for j in range(nf):
        at = pl.multiple_of(lax.rem(h - j + nf, nf) * width, 128)
        own = (own_ref if j == 0 else recvs[j - 1])[...].astype(F32)
        back = acc_ref[:, pl.ds(at, width)] + dot(inc, onehot(rep_ref[...], at, width), 0, 0)
        out_ref[:, pl.ds(at, width)] = (own + back).astype(BF)


def local(nd, nf, features, weights, tile_values, tile_blocks, tile_counts, replica, cotangent):
    feats, masters = features.shape
    wide = weights.shape[1]
    ntiles, tile, _ = tile_values.shape
    per = replica.shape[2]
    slots = nd * per
    width = masters // nf
    nb_own = masters // tile
    cols = masters + slots + tile
    nc = 2 if width % (2 * tile) == 0 else 1
    part = width // nc
    h = lax.axis_index("feat")
    d = lax.axis_index("dom")
    sd = jax.ShapeDtypeStruct
    lists = [pltpu.SMEM((ntiles + GROUP,), jnp.int32)] * 3
    rep = replica.reshape(slots, 1)
    tile_flops = 2 * ntiles * feats * tile * tile
    value_spec = full(tile_values.shape)

    def turn(j):
        return [(i, (i + j) % nf) for i in range(nf)]

    def to_peer(x, j):
        return lax.ppermute(x, "feat", turn(j))

    def half(x, j):
        return lax.dynamic_slice_in_dim(x, lax.rem(h + j, nf) * width, width, 1)

    x_recv = [to_peer(half(features, j), j) for j in range(1, nf)]
    x_parts = [half(features, 0)] + x_recv

    gb = block_of(masters)
    pull = pl.pallas_call(
        gather_kernel,
        grid=(masters // gb,),
        in_specs=[pl.BlockSpec((feats, gb), lambda i: (0, i)), full((slots, 1))],
        out_specs=full((nd, per, feats)),
        out_shape=sd((nd, per, feats), BF),
        scratch_shapes=[pltpu.VMEM((slots, feats), F32)],
        cost_estimate=cost(2 * slots * feats * masters, 2 * feats * masters),
        name="gather",
    )(features, rep)
    mirrors = lax.all_to_all(pull, "dom", 0, 0, tiled=True)

    acc = pl.pallas_call(
        functools.partial(spread_own, nb_own, tile),
        in_specs=[SMEM, SMEM, full(features.shape), value_spec],
        out_specs=full((feats, cols)),
        out_shape=sd((feats, cols), F32),
        scratch_shapes=lists,
        cost_estimate=cost(tile_flops, 2 * tile_values.size),
        name="spread_own",
    )(tile_blocks, tile_counts, features, tile_values)

    nsend = (nf - 1) * nc
    got = pl.pallas_call(
        functools.partial(spread_mirrors, nf, nc, nb_own, tile),
        in_specs=[SMEM, SMEM, full((nd, per, feats)), value_spec, full((feats, cols))],
        out_specs=[full((feats, width)), full((nd, nf, per, feats))] + [full((feats, part))] * nsend,
        out_shape=[sd((feats, width), F32), sd((nd, nf, per, feats), BF)]
        + [sd((feats, part), BF)] * nsend,
        scratch_shapes=[pltpu.VMEM((feats, cols), F32), pltpu.VMEM((feats, slots), BF)] + lists,
        cost_estimate=cost(tile_flops // 4, 2 * tile_values.size),
        name="spread_mirrors",
    )(tile_blocks, tile_counts, mirrors, tile_values, acc)
    own_part, push, part_sends = got[0], got[1], got[2:]

    def exchange_all(x):
        flat = x.reshape(nd * nf, per, feats)
        return lax.all_to_all(flat, ("dom", "feat"), 0, 0, tiled=True).reshape(x.shape)

    incoming = exchange_all(push)
    part_recv = [[to_peer(part_sends[(j - 1) * nc + c], j) for c in range(nc)] for j in range(1, nf)]

    wt = weights.reshape(2 * wide, wide).T
    vb = 256 if part % 256 == 0 else 128
    steps = part // vb
    outs = None
    pay = push
    ag_recv = [[] for _ in range(nf - 1)]
    for c in range(nc):

        def block(rows, c=c):
            return pl.BlockSpec((rows, vb), lambda i: (0, c * steps + i))

        def chunk(rows):
            return pl.BlockSpec((rows, vb), lambda i: (0, i))

        aliased = [] if c == 0 else list(outs)
        base = 6 + 2 * nf
        res = pl.pallas_call(
            functools.partial(dense_kernel, nf, c == 0, len(aliased), (width, c * part)),
            grid=(steps,),
            in_specs=[
                full((slots, 1)),
                full((wide, 2 * wide)),
                pl.BlockSpec((None, wide, wide), lambda i: (1, 0, 0)),
                full((nd, nf, per, feats)),
                block(wide),
                full((nd, nf, per, feats)),
            ]
            + [block(feats)] * nf
            + [block(feats)]
            + [chunk(feats)] * (nf - 1)
            + [ANY] * len(aliased),
            out_specs=[
                block(2 * wide),
                block(wide),
                block(wide),
                block(feats),
                full((nd, nf, per, feats)),
            ]
            + [chunk(feats)] * (nf - 1),
            out_shape=[
                sd((2 * wide, width), BF),
                sd((wide, width), BF),
                sd((wide, width), BF),
                sd((feats, width), BF),
                sd((nd, nf, per, feats), BF),
            ]
            + [sd((feats, part), BF)] * (nf - 1),
            scratch_shapes=[pltpu.VMEM((wide, vb), BF), pltpu.VMEM((slots, wide), F32)],
            input_output_aliases={base + k: k for k in range(len(aliased))},
            cost_estimate=cost(6 * wide * wide * part, 12 * wide * part),
            name="dense",
        )(
            rep,
            wt,
            weights,
            incoming,
            cotangent,
            pay,
            *x_parts,
            own_part,
            *[part_recv[j][c] for j in range(nf - 1)],
            *aliased,
        )
        outs = res[:4]
        pay = res[4]
        for j in range(1, nf):
            ag_recv[j - 1].append(to_peer(res[4 + j], j))
    rows, output, pre_grad, own_grad = outs
    grad_mirrors = exchange_all(pay)

    sb = block_of(width)
    got = pl.pallas_call(
        functools.partial(self_kernel, nf),
        grid=(width // sb,),
        in_specs=[
            pl.BlockSpec((None, wide, wide), lambda i: (0, 0, 0)),
            pl.BlockSpec((wide, sb), lambda i: (0, i)),
        ],
        out_specs=[pl.BlockSpec((feats, sb), lambda i: (0, i))] * nf,
        out_shape=[sd((feats, width), BF)] * nf,
        scratch_shapes=[pltpu.VMEM((wide, sb), BF)],
        cost_estimate=cost(2 * wide * wide * width, 4 * wide * width),
        name="self_grad",
    )(weights, pre_grad)
    self_own = got[0]
    self_recv = [to_peer(got[j], j) for j in range(1, nf)]

    terms = pl.pallas_call(
        functools.partial(weight_kernel, nf),
        grid=(width // sb,),
        in_specs=[
            pl.BlockSpec((2 * wide, sb), lambda i: (0, i)),
            pl.BlockSpec((wide, sb), lambda i: (0, i)),
        ],
        out_specs=full((nf, 2 * feats, wide)),
        out_shape=sd((nf, 2 * feats, wide), BF),
        scratch_shapes=[pltpu.VMEM((2 * wide, wide), F32)],
        cost_estimate=cost(4 * wide * wide * width, 6 * wide * width),
        name="weight_grad",
    )(rows, pre_grad)

    acc = pl.pallas_call(
        functools.partial(back_own, nf, tile),
        in_specs=[SMEM, SMEM, full((feats, width)), value_spec],
        out_specs=full((feats, cols)),
        out_shape=sd((feats, cols), F32),
        scratch_shapes=lists,
        cost_estimate=cost(tile_flops // 2, 2 * tile_values.size),
        name="back_own",
    )(tile_blocks, tile_counts, own_grad, tile_values)

    flat_recv = [ag_recv[j][c] for j in range(nf - 1) for c in range(nc)]
    acc, push = pl.pallas_call(
        functools.partial(back_rest, nf, nc, tile),
        in_specs=[SMEM, SMEM, full((nd, nf, per, feats)), value_spec, full((feats, cols))]
        + [full((feats, part))] * nsend,
        out_specs=[full((feats, masters)), full((nd, per, feats))],
        out_shape=[sd((feats, masters), F32), sd((nd, per, feats), BF)],
        scratch_shapes=[pltpu.VMEM((feats, cols), F32), pltpu.VMEM((feats, masters + slots), BF)]
        + lists,
        cost_estimate=cost(tile_flops // 2, 2 * tile_values.size),
        name="back_rest",
    )(tile_blocks, tile_counts, grad_mirrors, tile_values, acc, *flat_recv)
    back_in = lax.all_to_all(push, "dom", 0, 0, tiled=True)

    bits = []
    step = 1
    while step < nd:
        bits.append(step)
        step *= 2

    def swap(x, b):
        return lax.ppermute(x, "dom", [(i, i ^ b) for i in range(nd)])

    cur = terms
    for b in bits:
        keep_rows = cur.shape[1] // 2
        bit = lax.rem(d // b, 2)
        keep = lax.dynamic_slice_in_dim(cur, bit * keep_rows, keep_rows, 1)
        send = lax.dynamic_slice_in_dim(cur, (1 - bit) * keep_rows, keep_rows, 1)
        cur = (keep.astype(F32) + swap(send, b).astype(F32)).astype(BF)
    total = cur[0].astype(F32)
    for j in range(1, nf):
        total = total + to_peer(cur[j], j).astype(F32)
    total = total.astype(BF)
    for b in reversed(bits):
        bit = lax.rem(d // b, 2)
        other = swap(total, b)
        total = jnp.where(
            bit == 0, jnp.concatenate([total, other], 0), jnp.concatenate([other, total], 0)
        )
    weight_grad = total.reshape(2, feats, wide).astype(F32)

    feature_grad = pl.pallas_call(
        functools.partial(final_kernel, nf),
        in_specs=[full((slots, 1)), full((nd, per, feats)), full((feats, masters))]
        + [full((feats, width))] * nf,
        out_specs=full((feats, masters)),
        out_shape=sd((feats, masters), BF),
        cost_estimate=cost(2 * slots * feats * masters, 10 * feats * masters),
        name="final",
    )(rep, back_in, acc, self_own, *self_recv)
    return output, feature_grad, weight_grad


def solution(mesh):
    return jax.shard_map(
        functools.partial(local, mesh.shape["dom"], mesh.shape["feat"]),
        mesh=mesh,
        in_specs=(
            P("feat", "dom"),
            P(),
            P("dom", None, None),
            P("dom", None),
            P("dom"),
            P("dom", None, None),
            P(None, ("dom", "feat")),
        ),
        out_specs=(P(None, ("dom", "feat")), P("feat", "dom"), P(None, "feat", None)),
        check_vma=False,
    )
```

```python
import functools

import jax
import jax.numpy as jnp
from jax import lax
from jax.experimental import pallas as pl
from jax.experimental.pallas import tpu as pltpu
from jax.sharding import PartitionSpec as P

BF = jnp.bfloat16
F32 = jnp.float32
GROUP = 8


def dot(a, b, ca=1, cb=0):
    return lax.dot_general(a, b, (((ca,), (cb,)), ((), ())), preferred_element_type=F32)


def eye(n):
    rows = lax.broadcasted_iota(jnp.int32, (n, n), 0)
    cols = lax.broadcasted_iota(jnp.int32, (n, n), 1)
    return jnp.where(rows == cols, 1.0, 0.0).astype(BF)


def picks(slots, start, height):
    rows = lax.broadcasted_iota(jnp.int32, (height, slots.shape[1]), 0) + start
    return jnp.where(rows == slots, 1.0, 0.0).astype(BF)


def flip(x):
    return dot(eye(x.shape[1]), x, 1, 1).astype(BF)


SMEM = pl.BlockSpec(memory_space=pltpu.SMEM)
ANY = pl.BlockSpec(memory_space=pl.ANY)


def full(x):
    zeros = (0,) * len(x.shape)
    return pl.BlockSpec(x.shape, lambda *_: zeros)


def cost(flops, nbytes):
    return pl.CostEstimate(flops=int(flops), bytes_accessed=int(nbytes), transcendentals=0)


def block_of(n):
    return next(b for b in (512, 256, 128) if n % b == 0)


def list_tiles(blocks, count, lists, source_col, trash):
    tiles, sources, targets = lists

    def step(t, _):
        tiles[t] = t
        sources[t] = blocks[source_col, t]
        targets[t] = blocks[1 - source_col, t]
        return 0

    lax.fori_loop(0, count, step, 0)
    for u in range(GROUP):
        tiles[count + u] = 0
        sources[count + u] = 0
        targets[count + u] = trash


def run_tiles(n, lists, values, tile_dim, x_all, acc, tile):
    tiles, sources, targets = lists

    def step(g, _):
        for u in range(GROUP):
            at = g * GROUP + u
            picked = column(x_all, sources[at], tile)
            part = dot(picked, values[tiles[at]], 1, tile_dim)
            col = pl.ds(pl.multiple_of(targets[at] * tile, tile), tile)
            acc[:, col] += part
        return 0

    lax.fori_loop(0, (n + GROUP - 1) // GROUP, step, 0)


def column(ref, block, tile):
    at = pl.multiple_of(block * tile, tile)
    return ref[:, pl.ds(at, tile)]


def prep_kernel(nf, x_ref, rep_ref, pull_ref, *halves):
    h = lax.axis_index("feat")
    _, masters = x_ref.shape
    width = halves[0].shape[1]
    step = block_of(masters)
    total = None
    for at in range(0, masters, step):
        part = dot(x_ref[:, at : at + step], picks(rep_ref[...], at, step))
        total = part if total is None else total + part
    pull_ref[...] = flip(total.astype(BF)).reshape(pull_ref.shape)
    for j in range(nf):
        at = pl.multiple_of(lax.rem(h + j, nf) * width, 128)
        halves[j][...] = x_ref[:, pl.ds(at, width)]


def spread_kernel(nf, nc, tile, blocks, count, mirrors, x_ref, values_ref, *rest):
    own_ref, push_ref = rest[:2]
    rest = rest[2:]
    sends = rest[: (nf - 1) * nc]
    acc, x_all, values, tiles, sources, targets, sems = rest[(nf - 1) * nc :]
    lists = (tiles, sources, targets)
    h = lax.axis_index("feat")
    feats, masters = x_ref.shape
    width = own_ref.shape[1]
    slots = x_all.shape[1] - masters
    copies = [
        pltpu.make_async_copy(x_ref, x_all.at[:, :masters], sems.at[0]),
        pltpu.make_async_copy(values_ref, values, sems.at[1]),
    ]
    for copy in copies:
        copy.start()
    acc[...] = jnp.zeros_like(acc)
    x_all[:, masters:] = flip(mirrors[...].reshape(slots, feats))
    list_tiles(blocks, count[0], lists, 0, acc.shape[1] // tile - 1)
    for copy in copies:
        copy.wait()
    run_tiles(count[0], lists, values, 0, x_all, acc, tile)
    part = width // nc
    for j in range(1, nf):
        for c in range(nc):
            at = pl.multiple_of(lax.rem(h + j, nf) * width + c * part, 128)
            sends[(j - 1) * nc + c][...] = acc[:, pl.ds(at, part)].astype(BF)
    push = flip(acc[:, masters : masters + slots].astype(BF))
    push = push.reshape(push_ref.shape[0], push_ref.shape[2], feats)
    for f in range(nf):
        push_ref[:, f] = push
    own_ref[...] = acc[:, pl.ds(pl.multiple_of(h * width, 128), width)].astype(BF)


def dense_kernel(nf, nc, c, *refs):
    rep_ref, wt_ref, w_ref, inc_ref, cot_ref = refs[:5]
    xs, parts = refs[5 : 5 + nf], refs[5 + nf : 5 + 2 * nf]
    refs = refs[5 + 2 * nf :]
    if c:
        pay_in = refs[0]
        refs = refs[2:]
    rows, out_ref, g_ref, pay_ref = refs[:4]
    grads, selfs = refs[4 : 4 + nf], refs[4 + nf : 4 + 2 * nf]
    both, inc, pay = refs[4 + 2 * nf :]
    h = lax.axis_index("feat")
    i = pl.program_id(0)
    feats, step = grads[0].shape
    wide = g_ref.shape[0]
    slots = rep_ref.shape[1]
    part = step * pl.num_programs(0)

    @pl.when(i == 0)
    def _():
        for f in range(nf):
            inc[f] = flip(inc_ref[:, f].reshape(slots, feats))
        pay[...] = pay_in[...].astype(F32) if c else jnp.zeros_like(pay)

    pick = picks(rep_ref[...], (h * nc + c) * part + i * step, step)
    for j in range(nf):
        f = lax.rem(h - j + nf, nf)
        at = pl.multiple_of(f * feats, feats)
        total = parts[j][...].astype(F32) + dot(inc[f], pick, 1, 1)
        rows[pl.ds(at, feats), :] = xs[j][...]
        rows[pl.ds(wide + at, feats), :] = total.astype(BF)
    z = dot(wt_ref[...], rows[...])
    s = jax.nn.sigmoid(z)
    out_ref[...] = (z * s).astype(BF)
    g = (cot_ref[...].astype(F32) * (s * (1.0 + z * (1.0 - s)))).astype(BF)
    g_ref[...] = g
    both[...] = dot(w_ref[...], g).astype(BF)
    for j in range(nf):
        at = pl.multiple_of(lax.rem(h + j, nf) * feats, feats)
        grads[j][...] = both[pl.ds(wide + at, feats), :]
        selfs[j][...] = both[pl.ds(at, feats), :]
    pay[...] += dot(both[wide:, :], pick)

    @pl.when(i == pl.num_programs(0) - 1)
    def _():
        if c + 1 < nc:
            pay_ref[...] = pay[...].astype(BF)
        else:
            for f in range(nf):
                mine = flip(pay[f * feats : (f + 1) * feats].astype(BF))
                pay_ref[:, f] = mine.reshape(pay_ref.shape[0], pay_ref.shape[2], feats)


def weight_kernel(nf, nc, *refs):
    keep_ref, send_ref, acc = refs[2 * nc :]
    h = lax.axis_index("feat")
    bit = lax.rem(lax.axis_index("dom"), 2)
    wide = acc.shape[1]
    feats = wide // nf
    total = dot(refs[0][...], refs[nc][...], 1, 1)
    for c in range(1, nc):
        total = total + dot(refs[c][...], refs[nc + c][...], 1, 1)
    acc[...] = total
    for j in range(nf):
        at = lax.rem(h + j, nf) * feats
        keep_ref[j] = acc[pl.ds(pl.multiple_of(bit * wide + at, feats), feats), :]
        send_ref[j] = acc[pl.ds(pl.multiple_of((1 - bit) * wide + at, feats), feats), :].astype(BF)


def back_kernel(nf, nc, tile, blocks, count, mirrors, values_ref, *rest):
    grads = rest[: nf * nc]
    back_ref, push_ref, acc, x_all, values, tiles, sources, targets, sems = rest[nf * nc :]
    lists = (tiles, sources, targets)
    h = lax.axis_index("feat")
    feats, masters = back_ref.shape
    slots = x_all.shape[1] - masters
    part = masters // nf // nc
    copies = [pltpu.make_async_copy(values_ref, values, sems.at[nf * nc])]
    for j in range(nf):
        for c in range(nc):
            k = j * nc + c
            at = pl.multiple_of((lax.rem(h - j + nf, nf) * nc + c) * part, 128)
            copies.append(
                pltpu.make_async_copy(grads[k], x_all.at[:, pl.ds(at, part)], sems.at[k])
            )
    for copy in copies:
        copy.start()
    acc[...] = jnp.zeros_like(acc)
    total = mirrors[:, 0].astype(F32)
    for f in range(1, nf):
        total = total + mirrors[:, f].astype(F32)
    x_all[:, masters:] = flip(total.astype(BF).reshape(slots, feats))
    list_tiles(blocks, count[0], lists, 1, acc.shape[1] // tile - 1)
    for copy in copies:
        copy.wait()
    run_tiles(count[0], lists, values, 1, x_all, acc, tile)
    partial = acc[:, masters : masters + slots].astype(BF)
    push_ref[...] = flip(partial).reshape(push_ref.shape)
    back_ref[...] = acc[:, :masters].astype(BF)


def final_kernel(nf, nc, rep_ref, inc_ref, back_ref, *rest):
    selfs, out_ref = rest[: nf * nc], rest[nf * nc]
    h = lax.axis_index("feat")
    feats, part = selfs[0].shape
    slots = rep_ref.shape[1]
    inc = flip(inc_ref[...].reshape(slots, feats))
    for j in range(nf):
        for c in range(nc):
            at = pl.multiple_of((lax.rem(h - j + nf, nf) * nc + c) * part, 128)
            back = back_ref[:, pl.ds(at, part)].astype(F32)
            back = back + dot(inc, picks(rep_ref[...], at, part), 1, 1)
            own = selfs[j * nc + c][...].astype(F32)
            out_ref[:, pl.ds(at, part)] = (own + back).astype(BF)


def local(nd, nf, features, weights, tile_values, tile_blocks, tile_counts, replica, cotangent):
    feats, masters = features.shape
    wide = weights.shape[1]
    ntiles, tile, _ = tile_values.shape
    per = replica.shape[2]
    slots = nd * per
    width = masters // nf
    cols = masters + slots + tile
    nc = 2 if width % (2 * tile) == 0 else 1
    part = width // nc
    d = lax.axis_index("dom")
    sd = jax.ShapeDtypeStruct
    lists = [pltpu.SMEM((ntiles + GROUP,), jnp.int32)] * 3
    rep = replica.reshape(1, slots)
    tile_flops = 2 * ntiles * feats * tile * tile

    def call(body, flops, args, specs, outs, scratch=(), grid=(), out_specs=None, alias={}):
        return pl.pallas_call(
            body,
            grid=grid,
            in_specs=[full(a) if p is None else p for a, p in zip(args, specs, strict=True)],
            out_specs=out_specs or [full(o) for o in outs],
            out_shape=outs,
            scratch_shapes=list(scratch),
            input_output_aliases=alias,
            cost_estimate=cost(flops, 2 * sum(a.size for a in args)),
        )(*args)

    def to_peer(x, j):
        return lax.ppermute(x, "feat", [(i, (i + j) % nf) for i in range(nf)])

    def exchange(x, axes):
        flat = x.reshape(-1, per, feats)
        return lax.all_to_all(flat, axes, 0, 0, tiled=True).reshape(x.shape)

    def tile_scratch(nsems):
        return [
            pltpu.VMEM((feats, cols), F32),
            pltpu.VMEM((feats, masters + slots), BF),
            pltpu.VMEM(tile_values.shape, BF),
            *lists,
            pltpu.SemaphoreType.DMA((nsems,)),
        ]

    vec = sd((feats, width), BF)
    pull, *x_halves = call(
        functools.partial(prep_kernel, nf),
        2 * slots * feats * masters,
        [features, rep],
        [None] * 2,
        [sd((nd, per, feats), BF)] + [vec] * nf,
    )
    mirrors = exchange(pull, "dom")
    x_parts = [x_halves[0]] + [to_peer(x_halves[j], j) for j in range(1, nf)]

    blocks = tile_blocks.T
    chunk = sd((feats, part), BF)
    own_part, push, *part_sends = call(
        functools.partial(spread_kernel, nf, nc, tile),
        tile_flops,
        [blocks, tile_counts, mirrors, features, tile_values],
        [SMEM, SMEM, None, ANY, ANY],
        [vec, sd((nd, nf, per, feats), BF)] + [chunk] * ((nf - 1) * nc),
        tile_scratch(nf * nc + 1),
    )
    part_recv = [
        [to_peer(part_sends[(j - 1) * nc + c], j) for j in range(1, nf)]
        for c in range(nc)
    ]
    incoming = exchange(push, ("dom", "feat"))

    flat_w = weights.reshape(2 * wide, wide)
    wt = flat_w.T
    rows, grads, grad_own, grad_recv, self_own, self_recv = [], [], [], [], [], []
    vb = 256 if part % 256 == 0 else 128
    steps = part // vb

    def of_all(height, c):
        return pl.BlockSpec((height, vb), lambda i: (0, c * steps + i))

    def of_chunk(height):
        return pl.BlockSpec((height, vb), lambda i: (0, i))

    for c in range(nc):
        last = c + 1 == nc
        args = [rep, wt, flat_w, incoming, cotangent, *x_parts, own_part, *part_recv[c]]
        specs = [None] * 4 + [of_all(wide, c)] + [of_all(feats, c)] * (nf + 1)
        specs += [of_chunk(feats)] * (nf - 1)
        alias = {}
        if c:
            alias = {len(args) + 1: 1}
            args += [pay, output]
            specs += [None, ANY]
        outs = [
            sd((2 * wide, part), BF),
            sd((wide, width), BF),
            sd((wide, part), BF),
            sd((nd, nf, per, feats) if last else (wide, slots), BF),
        ] + [chunk] * (2 * nf)
        out_specs = [of_chunk(2 * wide), of_all(wide, c), of_chunk(wide), full(outs[3])]
        out_specs += [of_chunk(feats)] * (2 * nf)
        rows_c, output, g_c, pay, *res = call(
            functools.partial(dense_kernel, nf, nc, c),
            8 * wide * wide * part,
            args,
            specs,
            outs,
            [
                pltpu.VMEM((2 * wide, vb), BF),
                pltpu.VMEM((nf, feats, slots), BF),
                pltpu.VMEM((wide, slots), F32),
            ],
            (steps,),
            out_specs,
            alias,
        )
        rows.append(rows_c)
        grads.append(g_c)
        grad_own.append(res[0])
        self_own.append(res[nf])
        grad_recv.append([to_peer(res[j], j) for j in range(1, nf)])
        self_recv.append([to_peer(res[nf + j], j) for j in range(1, nf)])
    grad_mirrors = exchange(pay, ("dom", "feat"))

    keep, send = call(
        functools.partial(weight_kernel, nf, nc),
        4 * wide * wide * width,
        rows + grads,
        [None] * (2 * nc),
        [sd((nf, feats, wide), F32), sd((nf, feats, wide), BF)],
        [pltpu.VMEM((2 * wide, wide), F32)],
    )

    flat_grads = grad_own + [grad_recv[c][j] for j in range(nf - 1) for c in range(nc)]
    back, push = call(
        functools.partial(back_kernel, nf, nc, tile),
        tile_flops,
        [blocks, tile_counts, grad_mirrors, tile_values, *flat_grads],
        [SMEM, SMEM, None, ANY] + [ANY] * (nf * nc),
        [sd((feats, masters), BF), sd((nd, per, feats), BF)],
        tile_scratch(nf * nc + 1),
    )
    back_in = exchange(push, "dom")

    bits = [1 << k for k in range(nd.bit_length() - 1)]

    def swap(x, b):
        return lax.ppermute(x, "dom", [(i, i ^ b) for i in range(nd)])

    for b in bits:
        cur = keep + swap(send, b).astype(F32)
        if b == bits[-1]:
            break
        bit = lax.rem(d // (2 * b), 2)
        size = cur.shape[1] // 2
        wire = F32 if 4 * b >= nd else BF
        keep = lax.dynamic_slice_in_dim(cur, bit * size, size, 1)
        send = lax.dynamic_slice_in_dim(cur, (1 - bit) * size, size, 1).astype(wire)
    total = cur[0]
    for j in range(1, nf):
        total = total + to_peer(cur[j], j)
    total = total.astype(BF)
    for b in reversed(bits):
        bit = lax.rem(d // b, 2)
        other = swap(total, b)
        total = jnp.where(
            bit == 0, jnp.concatenate([total, other], 0), jnp.concatenate([other, total], 0)
        )
    weight_grad = total.reshape(2, feats, wide).astype(F32)

    selfs = [self_own[c] for c in range(nc)]
    selfs += [self_recv[c][j] for j in range(nf - 1) for c in range(nc)]
    (feature_grad,) = call(
        functools.partial(final_kernel, nf, nc),
        2 * slots * feats * masters,
        [rep, back_in, back, *selfs],
        [None] * (3 + nf * nc),
        [sd((feats, masters), BF)],
    )
    return output, feature_grad, weight_grad


def solution(mesh):
    return jax.shard_map(
        functools.partial(local, mesh.shape["dom"], mesh.shape["feat"]),
        mesh=mesh,
        in_specs=(
            P("feat", "dom"),
            P(),
            P("dom", None, None),
            P("dom", None),
            P("dom"),
            P("dom", None, None),
            P(None, ("dom", "feat")),
        ),
        out_specs=(P(None, ("dom", "feat")), P("feat", "dom"), P(None, "feat", None)),
        check_vma=False,
    )
```

```python
import functools

import jax
import jax.numpy as jnp
from jax import lax
from jax.experimental import pallas as pl
from jax.experimental.pallas import tpu as pltpu
from jax.sharding import PartitionSpec as P

BF = jnp.bfloat16
F32 = jnp.float32
GROUP = 8


def dot(a, b, ca=1, cb=0):
    return lax.dot_general(a, b, (((ca,), (cb,)), ((), ())), preferred_element_type=F32)


def eye(n):
    rows = lax.broadcasted_iota(jnp.int32, (n, n), 0)
    cols = lax.broadcasted_iota(jnp.int32, (n, n), 1)
    return jnp.where(rows == cols, 1.0, 0.0).astype(BF)


def picks(slots, start, height):
    rows = lax.broadcasted_iota(jnp.int32, (height, slots.shape[1]), 0) + start
    return jnp.where(rows == slots, 1.0, 0.0).astype(BF)


def flip(x):
    return dot(eye(x.shape[1]), x, 1, 1).astype(BF)


SMEM = pl.BlockSpec(memory_space=pltpu.SMEM)
ANY = pl.BlockSpec(memory_space=pl.ANY)


def full(x):
    zeros = (0,) * len(x.shape)
    return pl.BlockSpec(x.shape, lambda *_: zeros)


def cost(flops, nbytes):
    return pl.CostEstimate(flops=int(flops), bytes_accessed=int(nbytes), transcendentals=0)


def block_of(n):
    return next(b for b in (512, 256, 128) if n % b == 0)


def list_tiles(blocks, count, lists, source_col, trash):
    tiles, sources, targets = lists

    def step(t, _):
        tiles[t] = t
        sources[t] = blocks[source_col, t]
        targets[t] = blocks[1 - source_col, t]
        return 0

    lax.fori_loop(0, count, step, 0)
    for u in range(GROUP):
        tiles[count + u] = 0
        sources[count + u] = 0
        targets[count + u] = trash


def run_tiles(n, lists, values, tile_dim, x_all, acc, tile):
    tiles, sources, targets = lists

    def step(g, _):
        for u in range(GROUP):
            at = g * GROUP + u
            picked = column(x_all, sources[at], tile)
            part = dot(picked, values[tiles[at]], 1, tile_dim)
            col = pl.ds(pl.multiple_of(targets[at] * tile, tile), tile)
            acc[:, col] += part
        return 0

    lax.fori_loop(0, (n + GROUP - 1) // GROUP, step, 0)


def column(ref, block, tile):
    at = pl.multiple_of(block * tile, tile)
    return ref[:, pl.ds(at, tile)]


def prep_kernel(nf, x_ref, rep_ref, pull_ref, *halves):
    h = lax.axis_index("feat")
    _, masters = x_ref.shape
    width = halves[0].shape[1]
    step = block_of(masters)
    total = None
    for at in range(0, masters, step):
        part = dot(x_ref[:, at : at + step], picks(rep_ref[...], at, step))
        total = part if total is None else total + part
    pull_ref[...] = flip(total.astype(BF)).reshape(pull_ref.shape)
    for j in range(nf):
        at = pl.multiple_of(lax.rem(h + j, nf) * width, 128)
        halves[j][...] = x_ref[:, pl.ds(at, width)]


def spread_kernel(nf, nc, tile, blocks, count, mirrors, x_ref, values_ref, *rest):
    own_ref, push_ref = rest[:2]
    rest = rest[2:]
    sends = rest[: (nf - 1) * nc]
    acc, x_all, values, tiles, sources, targets, sems = rest[(nf - 1) * nc :]
    lists = (tiles, sources, targets)
    h = lax.axis_index("feat")
    feats, masters = x_ref.shape
    width = own_ref.shape[1]
    slots = x_all.shape[1] - masters
    copies = [
        pltpu.make_async_copy(x_ref, x_all.at[:, :masters], sems.at[0]),
        pltpu.make_async_copy(values_ref, values, sems.at[1]),
    ]
    for copy in copies:
        copy.start()
    acc[...] = jnp.zeros_like(acc)
    x_all[:, masters:] = flip(mirrors[...].reshape(slots, feats))
    list_tiles(blocks, count[0], lists, 0, acc.shape[1] // tile - 1)
    for copy in copies:
        copy.wait()
    run_tiles(count[0], lists, values, 0, x_all, acc, tile)
    part = width // nc
    for j in range(1, nf):
        for c in range(nc):
            at = pl.multiple_of(lax.rem(h + j, nf) * width + c * part, 128)
            sends[(j - 1) * nc + c][...] = acc[:, pl.ds(at, part)].astype(BF)
    push = flip(acc[:, masters : masters + slots].astype(BF))
    push = push.reshape(push_ref.shape[0], push_ref.shape[2], feats)
    for f in range(nf):
        push_ref[:, f] = push
    own_ref[...] = acc[:, pl.ds(pl.multiple_of(h * width, 128), width)].astype(BF)


def dense_kernel(nf, nc, c, *refs):
    rep_ref, wt_ref, w_ref, inc_ref, cot_ref = refs[:5]
    xs, parts = refs[5 : 5 + nf], refs[5 + nf : 5 + 2 * nf]
    refs = refs[5 + 2 * nf :]
    if c:
        pay_in = refs[0]
        refs = refs[2:]
    agg_ref, out_ref, g_ref, pay_ref = refs[:4]
    grads, selfs = refs[4 : 4 + nf], refs[4 + nf : 4 + 2 * nf]
    rows, both, inc, pay = refs[4 + 2 * nf :]
    h = lax.axis_index("feat")
    i = pl.program_id(0)
    feats, step = grads[0].shape
    wide = g_ref.shape[0]
    slots = rep_ref.shape[1]
    part = step * pl.num_programs(0)

    @pl.when(i == 0)
    def _():
        for f in range(nf):
            inc[f] = flip(inc_ref[:, f].reshape(slots, feats))
        pay[...] = pay_in[...].astype(F32) if c else jnp.zeros_like(pay)

    pick = picks(rep_ref[...], (h * nc + c) * part + i * step, step)
    for j in range(nf):
        f = lax.rem(h - j + nf, nf)
        at = pl.multiple_of(f * feats, feats)
        total = parts[j][...].astype(F32) + dot(inc[f], pick, 1, 1)
        rows[pl.ds(at, feats), :] = xs[j][...]
        rows[pl.ds(wide + at, feats), :] = total.astype(BF)
    agg_ref[...] = rows[wide:, :]
    z = dot(wt_ref[...], rows[...])
    s = 0.5 + 0.5 * jnp.tanh(0.5 * z)
    out_ref[...] = (z * s).astype(BF)
    g = (cot_ref[...].astype(F32) * (s * (1.0 + z * (1.0 - s)))).astype(BF)
    g_ref[...] = g
    both[...] = dot(w_ref[...], g).astype(BF)
    for j in range(nf):
        at = pl.multiple_of(lax.rem(h + j, nf) * feats, feats)
        grads[j][...] = both[pl.ds(wide + at, feats), :]
        selfs[j][...] = both[pl.ds(at, feats), :]
    pay[...] += dot(both[wide:, :], pick)

    @pl.when(i == pl.num_programs(0) - 1)
    def _():
        if c + 1 < nc:
            pay_ref[...] = pay[...].astype(BF)
        else:
            for f in range(nf):
                mine = flip(pay[f * feats : (f + 1) * feats].astype(BF))
                pay_ref[:, f] = mine.reshape(pay_ref.shape[0], pay_ref.shape[2], feats)


def weight_kernel(nf, nc, *refs):
    xs, aggs, grads = refs[:nf], refs[nf : nf + nc], refs[nf + nc : nf + 2 * nc]
    keep_ref, send_ref, acc = refs[nf + 2 * nc :]
    h = lax.axis_index("feat")
    bit = lax.rem(lax.axis_index("dom"), 2)
    wide = acc.shape[1]
    feats = wide // nf
    part = grads[0].shape[1]

    def summed(terms):
        total = None
        for left, right in terms:
            term = dot(left, right, 1, 1)
            total = term if total is None else total + term
        return total

    acc[wide:, :] = summed((aggs[c][...], grads[c][...]) for c in range(nc))
    for j in range(nf):
        at = pl.multiple_of(lax.rem(h - j + nf, nf) * feats, feats)
        acc[pl.ds(at, feats), :] = summed(
            (xs[j][:, c * part : (c + 1) * part], grads[c][...]) for c in range(nc)
        )
    for j in range(nf):
        at = lax.rem(h + j, nf) * feats
        keep_ref[j] = acc[pl.ds(pl.multiple_of(bit * wide + at, feats), feats), :]
        send_ref[j] = acc[pl.ds(pl.multiple_of((1 - bit) * wide + at, feats), feats), :].astype(BF)


def radices_of(n):
    radices = [2] * min(2, n.bit_length() - 1)
    n //= 1 << len(radices)
    while n > 1:
        radices.append(4 if n % 4 == 0 else 2)
        n //= radices[-1]
    return tuple(radices)


def unit_of(radices, k):
    unit = 1
    for r in radices[:k]:
        unit *= r
    return unit


def relative(radices, m):
    number = 0
    size = unit_of(radices, len(radices))
    for k, r in enumerate(radices):
        size //= r
        number += (m // size) % r * unit_of(radices, k)
    return number


def assemble_kernel(radices, own_ref, other_ref, out_ref):
    d = lax.axis_index("dom")
    nd = 1
    for r in radices:
        nd *= r
    rows = out_ref.shape[0] // nd
    half = nd // 2
    for m in range(nd):
        at, owner, height = 0, d ^ relative(radices, m), out_ref.shape[0]
        for r in radices:
            height //= r
            at = at + lax.rem(owner, r) * height
            owner = owner // r
        ref, k = (own_ref, m) if m < half else (other_ref, m - half)
        piece = ref[k * rows : (k + 1) * rows, :]
        out_ref[pl.ds(pl.multiple_of(at, rows), rows), :] = piece.astype(F32)


def back_kernel(nf, nc, tile, blocks, count, mirrors, values_ref, *rest):
    grads = rest[: nf * nc]
    back_ref, push_ref, acc, x_all, values, tiles, sources, targets, sems = rest[nf * nc :]
    lists = (tiles, sources, targets)
    h = lax.axis_index("feat")
    feats, masters = back_ref.shape
    slots = x_all.shape[1] - masters
    part = masters // nf // nc
    copies = [pltpu.make_async_copy(values_ref, values, sems.at[nf * nc])]
    for j in range(nf):
        for c in range(nc):
            k = j * nc + c
            at = pl.multiple_of((lax.rem(h - j + nf, nf) * nc + c) * part, 128)
            copies.append(
                pltpu.make_async_copy(grads[k], x_all.at[:, pl.ds(at, part)], sems.at[k])
            )
    for copy in copies:
        copy.start()
    acc[...] = jnp.zeros_like(acc)
    total = mirrors[:, 0].astype(F32)
    for f in range(1, nf):
        total = total + mirrors[:, f].astype(F32)
    x_all[:, masters:] = flip(total.astype(BF).reshape(slots, feats))
    list_tiles(blocks, count[0], lists, 1, acc.shape[1] // tile - 1)
    for copy in copies:
        copy.wait()
    run_tiles(count[0], lists, values, 1, x_all, acc, tile)
    partial = acc[:, masters : masters + slots].astype(BF)
    push_ref[...] = flip(partial).reshape(push_ref.shape)
    back_ref[...] = acc[:, :masters].astype(BF)


def final_kernel(nf, nc, rep_ref, inc_ref, back_ref, *rest):
    selfs, out_ref = rest[: nf * nc], rest[nf * nc]
    h = lax.axis_index("feat")
    feats, part = selfs[0].shape
    slots = rep_ref.shape[1]
    inc = flip(inc_ref[...].reshape(slots, feats))
    for j in range(nf):
        for c in range(nc):
            at = pl.multiple_of((lax.rem(h - j + nf, nf) * nc + c) * part, 128)
            back = back_ref[:, pl.ds(at, part)].astype(F32)
            back = back + dot(inc, picks(rep_ref[...], at, part), 1, 1)
            own = selfs[j * nc + c][...].astype(F32)
            out_ref[:, pl.ds(at, part)] = (own + back).astype(BF)


def local(nd, nf, features, weights, tile_values, tile_blocks, tile_counts, replica, cotangent):
    feats, masters = features.shape
    wide = weights.shape[1]
    ntiles, tile, _ = tile_values.shape
    per = replica.shape[2]
    slots = nd * per
    width = masters // nf
    cols = masters + slots + tile
    nc = 2 if width % (2 * tile) == 0 else 1
    part = width // nc
    d = lax.axis_index("dom")
    sd = jax.ShapeDtypeStruct
    lists = [pltpu.SMEM((ntiles + GROUP,), jnp.int32)] * 3
    rep = replica.reshape(1, slots)
    tile_flops = 2 * ntiles * feats * tile * tile

    def call(body, flops, args, specs, outs, scratch=(), grid=(), out_specs=None, alias={}):
        return pl.pallas_call(
            body,
            grid=grid,
            in_specs=[full(a) if p is None else p for a, p in zip(args, specs, strict=True)],
            out_specs=out_specs or [full(o) for o in outs],
            out_shape=outs,
            scratch_shapes=list(scratch),
            input_output_aliases=alias,
            cost_estimate=cost(flops, 2 * sum(a.size for a in args)),
        )(*args)

    def to_peer(x, j):
        return lax.ppermute(x, "feat", [(i, (i + j) % nf) for i in range(nf)])

    def exchange(x, axes):
        flat = x.reshape(-1, per, feats)
        return lax.all_to_all(flat, axes, 0, 0, tiled=True).reshape(x.shape)

    def tile_scratch(nsems):
        return [
            pltpu.VMEM((feats, cols), F32),
            pltpu.VMEM((feats, masters + slots), BF),
            pltpu.VMEM(tile_values.shape, BF),
            *lists,
            pltpu.SemaphoreType.DMA((nsems,)),
        ]

    vec = sd((feats, width), BF)
    pull, *x_halves = call(
        functools.partial(prep_kernel, nf),
        2 * slots * feats * masters,
        [features, rep],
        [None] * 2,
        [sd((nd, per, feats), BF)] + [vec] * nf,
    )
    mirrors = exchange(pull, "dom")
    x_parts = [x_halves[0]] + [to_peer(x_halves[j], j) for j in range(1, nf)]

    blocks = tile_blocks.T
    chunk = sd((feats, part), BF)
    own_part, push, *part_sends = call(
        functools.partial(spread_kernel, nf, nc, tile),
        tile_flops,
        [blocks, tile_counts, mirrors, features, tile_values],
        [SMEM, SMEM, None, ANY, ANY],
        [vec, sd((nd, nf, per, feats), BF)] + [chunk] * ((nf - 1) * nc),
        tile_scratch(nf * nc + 1),
    )
    part_recv = [
        [to_peer(part_sends[(j - 1) * nc + c], j) for j in range(1, nf)]
        for c in range(nc)
    ]
    incoming = exchange(push, ("dom", "feat"))

    flat_w = weights.reshape(2 * wide, wide)
    wt = flat_w.T
    rows, grads, grad_own, grad_recv, self_own, self_recv = [], [], [], [], [], []
    vb = 256 if part % 256 == 0 else 128
    steps = part // vb

    def of_all(height, c):
        return pl.BlockSpec((height, vb), lambda i: (0, c * steps + i))

    def of_chunk(height):
        return pl.BlockSpec((height, vb), lambda i: (0, i))

    for c in range(nc):
        last = c + 1 == nc
        args = [rep, wt, flat_w, incoming, cotangent, *x_parts, own_part, *part_recv[c]]
        specs = [None] * 4 + [of_all(wide, c)] + [of_all(feats, c)] * (nf + 1)
        specs += [of_chunk(feats)] * (nf - 1)
        alias = {}
        if c:
            alias = {len(args) + 1: 1}
            args += [pay, output]
            specs += [None, ANY]
        outs = [
            sd((wide, part), BF),
            sd((wide, width), BF),
            sd((wide, part), BF),
            sd((nd, nf, per, feats) if last else (wide, slots), BF),
        ] + [chunk] * (2 * nf)
        out_specs = [of_chunk(wide), of_all(wide, c), of_chunk(wide), full(outs[3])]
        out_specs += [of_chunk(feats)] * (2 * nf)
        rows_c, output, g_c, pay, *res = call(
            functools.partial(dense_kernel, nf, nc, c),
            8 * wide * wide * part,
            args,
            specs,
            outs,
            [
                pltpu.VMEM((2 * wide, vb), BF),
                pltpu.VMEM((2 * wide, vb), BF),
                pltpu.VMEM((nf, feats, slots), BF),
                pltpu.VMEM((wide, slots), F32),
            ],
            (steps,),
            out_specs,
            alias,
        )
        rows.append(rows_c)
        grads.append(g_c)
        grad_own.append(res[0])
        self_own.append(res[nf])
        grad_recv.append([to_peer(res[j], j) for j in range(1, nf)])
        self_recv.append([to_peer(res[nf + j], j) for j in range(1, nf)])
    grad_mirrors = exchange(pay, ("dom", "feat"))

    keep, send = call(
        functools.partial(weight_kernel, nf, nc),
        4 * wide * wide * width,
        x_parts + rows + grads,
        [None] * (nf + 2 * nc),
        [sd((nf, feats, wide), F32), sd((nf, feats, wide), BF)],
        [pltpu.VMEM((2 * wide, wide), F32)],
    )

    flat_grads = grad_own + [grad_recv[c][j] for j in range(nf - 1) for c in range(nc)]
    back, push = call(
        functools.partial(back_kernel, nf, nc, tile),
        tile_flops,
        [blocks, tile_counts, grad_mirrors, tile_values, *flat_grads],
        [SMEM, SMEM, None, ANY] + [ANY] * (nf * nc),
        [sd((feats, masters), BF), sd((nd, per, feats), BF)],
        tile_scratch(nf * nc + 1),
    )
    back_in = exchange(push, "dom")

    radices = radices_of(nd)

    def swap(x, b):
        return lax.ppermute(x, "dom", [(i, i ^ b) for i in range(nd)])

    sends = [send]
    for k, r in enumerate(radices):
        unit = unit_of(radices, k)
        cur = keep
        for m in range(1, r):
            cur = cur + swap(sends[m - 1], m * unit).astype(F32)
        if k + 1 == len(radices):
            break
        size = cur.shape[1] // radices[k + 1]
        digit = lax.rem(d // unit_of(radices, k + 1), radices[k + 1])
        pieces = [
            lax.dynamic_slice_in_dim(cur, (digit ^ m) * size, size, 1)
            for m in range(radices[k + 1])
        ]
        keep, sends = pieces[0], [piece.astype(BF) for piece in pieces[1:]]
    total = cur[0]
    for j in range(1, nf):
        total = total + to_peer(cur[j], j)
    total = total.astype(BF)
    for k in reversed(range(1, len(radices))):
        unit = unit_of(radices, k)
        others = [swap(total, m * unit) for m in range(1, radices[k])]
        total = jnp.concatenate([total, *others], 0)
    other = swap(total, 1)
    if total.shape[0] * 2 // nd % 8 == 0:
        (weight_grad,) = call(
            functools.partial(assemble_kernel, radices),
            0,
            [total, other],
            [None] * 2,
            [sd((2 * feats, wide), F32)],
        )
    else:
        total = jnp.concatenate([total, other], 0).reshape(nd, -1, wide)
        owners = jnp.arange(nd)
        place, rest = jnp.zeros_like(owners), owners
        for r in radices:
            place, rest = place * r + rest % r, rest // r
        held = jnp.zeros_like(owners).at[place].set(owners) ^ d
        numbers = jnp.array([relative(radices, m) for m in range(nd)])
        index = jnp.zeros_like(owners).at[numbers].set(jnp.arange(nd))[held]
        weight_grad = total[index].reshape(2 * feats, wide).astype(F32)
    weight_grad = weight_grad.reshape(2, feats, wide)

    selfs = [self_own[c] for c in range(nc)]
    selfs += [self_recv[c][j] for j in range(nf - 1) for c in range(nc)]
    (feature_grad,) = call(
        functools.partial(final_kernel, nf, nc),
        2 * slots * feats * masters,
        [rep, back_in, back, *selfs],
        [None] * (3 + nf * nc),
        [sd((feats, masters), BF)],
    )
    return output, feature_grad, weight_grad


def solution(mesh):
    return jax.shard_map(
        functools.partial(local, mesh.shape["dom"], mesh.shape["feat"]),
        mesh=mesh,
        in_specs=(
            P("feat", "dom"),
            P(),
            P("dom", None, None),
            P("dom", None),
            P("dom"),
            P("dom", None, None),
            P(None, ("dom", "feat")),
        ),
        out_specs=(P(None, ("dom", "feat")), P("feat", "dom"), P(None, "feat", None)),
        check_vma=False,
    )
```

```python
import functools

import jax
import jax.numpy as jnp
from jax import lax
from jax.experimental import pallas as pl
from jax.experimental.pallas import tpu as pltpu
from jax.sharding import PartitionSpec as P

BF = jnp.bfloat16
F32 = jnp.float32
GROUP = 8


def dot(a, b, ca=1, cb=0):
    return lax.dot_general(a, b, (((ca,), (cb,)), ((), ())), preferred_element_type=F32)


def eye(n):
    rows = lax.broadcasted_iota(jnp.int32, (n, n), 0)
    cols = lax.broadcasted_iota(jnp.int32, (n, n), 1)
    return jnp.where(rows == cols, 1.0, 0.0).astype(BF)


def picks(slots, start, height):
    rows = lax.broadcasted_iota(jnp.int32, (height, slots.shape[1]), 0) + start
    return jnp.where(rows == slots, 1.0, 0.0).astype(BF)


def flip(x):
    return dot(eye(x.shape[1]), x, 1, 1).astype(BF)


SMEM = pl.BlockSpec(memory_space=pltpu.SMEM)
ANY = pl.BlockSpec(memory_space=pl.ANY)


def full(x):
    zeros = (0,) * len(x.shape)
    return pl.BlockSpec(x.shape, lambda *_: zeros)


def cost(flops, nbytes):
    return pl.CostEstimate(flops=int(flops), bytes_accessed=int(nbytes), transcendentals=0)


def block_of(n):
    return next(b for b in (512, 256, 128) if n % b == 0)


def list_tiles(blocks, count, lists, source_col, trash, low, high):
    tiles, sources, targets = lists

    def step(t, n):
        source = blocks[source_col, t]
        tiles[n] = t
        sources[n] = source - low
        targets[n] = blocks[1 - source_col, t]
        return n + jnp.logical_and(source >= low, source < high).astype(jnp.int32)

    n = lax.fori_loop(0, count, step, jnp.int32(0))
    for u in range(GROUP):
        tiles[n + u] = 0
        sources[n + u] = 0
        targets[n + u] = trash
    return n


def run_tiles(n, lists, values, tile_dim, x_all, acc, tile):
    tiles, sources, targets = lists

    def step(g, _):
        for u in range(GROUP):
            at = g * GROUP + u
            picked = column(x_all, sources[at], tile)
            part = dot(picked, values[tiles[at]], 1, tile_dim)
            col = pl.ds(pl.multiple_of(targets[at] * tile, tile), tile)
            acc[:, col] += part
        return 0

    lax.fori_loop(0, (n + GROUP - 1) // GROUP, step, 0)


def column(ref, block, tile):
    at = pl.multiple_of(block * tile, tile)
    return ref[:, pl.ds(at, tile)]


def prep_kernel(nf, x_ref, replica, pull_ref, rep_ref, *halves):
    rep_ref[...] = jnp.concatenate(
        [replica[0, p : p + 1, :] for p in range(replica.shape[1])], axis=1
    )
    h = lax.axis_index("feat")
    _, masters = x_ref.shape
    width = halves[0].shape[1]
    step = block_of(masters)
    total = None
    for at in range(0, masters, step):
        part = dot(x_ref[:, at : at + step], picks(rep_ref[...], at, step))
        total = part if total is None else total + part
    pull_ref[...] = flip(total.astype(BF)).reshape(pull_ref.shape)
    for j in range(nf):
        at = pl.multiple_of(lax.rem(h + j, nf) * width, 128)
        halves[j][...] = x_ref[:, pl.ds(at, width)]


def spread_own(tile, blocks, count, x_ref, values_ref, out_ref, acc, x, values, *rest):
    lists, sems = rest[:3], rest[3]
    masters = x.shape[1]
    copies = [
        pltpu.make_async_copy(x_ref, x, sems.at[0]),
        pltpu.make_async_copy(values_ref, values, sems.at[1]),
    ]
    for copy in copies:
        copy.start()
    acc[...] = jnp.zeros_like(acc)
    n = list_tiles(blocks, count[0], lists, 0, acc.shape[1] // tile - 1, 0, masters // tile)
    for copy in copies:
        copy.wait()
    run_tiles(n, lists, values, 0, x, acc, tile)
    out_ref[...] = acc[:, : out_ref.shape[1]].astype(BF)


def spread_mirrors(nf, nc, tile, blocks, count, mirrors, values_ref, own_ref, *rest):
    part_ref, push_ref = rest[:2]
    sends = rest[2 : 2 + (nf - 1) * nc]
    acc, own, x, values, *lists, sems = rest[2 + (nf - 1) * nc :]
    h = lax.axis_index("feat")
    feats, width = part_ref.shape
    slots = x.shape[1]
    masters = own.shape[1] - slots
    copies = [
        pltpu.make_async_copy(values_ref, values, sems.at[0]),
        pltpu.make_async_copy(own_ref, own, sems.at[1]),
    ]
    for copy in copies:
        copy.start()
    acc[...] = jnp.zeros_like(acc)
    x[...] = flip(mirrors[...].reshape(slots, feats))
    low = masters // tile
    n = list_tiles(
        blocks, count[0], lists, 0, acc.shape[1] // tile - 1, low, own.shape[1] // tile
    )
    for copy in copies:
        copy.wait()
    run_tiles(n, lists, values, 0, x, acc, tile)

    def total(at, size):
        return (own[:, pl.ds(at, size)].astype(F32) + acc[:, pl.ds(at, size)]).astype(BF)

    part = width // nc
    for j in range(1, nf):
        for c in range(nc):
            at = pl.multiple_of(lax.rem(h + j, nf) * width + c * part, 128)
            sends[(j - 1) * nc + c][...] = total(at, part)
    push = flip(total(masters, slots))
    push = push.reshape(push_ref.shape[0], push_ref.shape[2], feats)
    for f in range(nf):
        push_ref[:, f] = push
    part_ref[...] = total(pl.multiple_of(h * width, 128), width)


def dense_kernel(nf, nc, c, *refs):
    rep_ref, inc_ref, wt_hbm, w_hbm, cot_hbm = refs[:5]
    xs, parts = refs[5 : 5 + nf], refs[5 + nf : 5 + 2 * nf]
    refs = refs[5 + 2 * nf :]
    if c:
        pay_in = refs[0]
        refs = refs[2:]
    agg_hbm, out_hbm, g_hbm, pay_ref = refs[:4]
    grads, selfs = refs[4 : 4 + nf], refs[4 + nf : 4 + 2 * nf]
    wt, w, cot, rows, terms, out, g_all, both, in_sems, out_sems = refs[4 + 2 * nf :]
    h = lax.axis_index("feat")
    feats, part = grads[0].shape
    wide = w.shape[1]
    slots = rep_ref.shape[1]
    chunk = pl.ds(c * part, part)

    def place(f):
        return pl.ds(pl.multiple_of(f * feats, feats), feats)

    early, late = [], []
    for j in range(nf):
        f = lax.rem(h - j + nf, nf)
        term = parts[j].at[:, chunk] if j == 0 else parts[j]
        early.append(pltpu.make_async_copy(term, terms.at[j], in_sems.at[j]))
        x = xs[j].at[:, chunk]
        early.append(pltpu.make_async_copy(x, rows.at[place(f)], in_sems.at[nf + j]))
    late.append(pltpu.make_async_copy(wt_hbm, wt, in_sems.at[2 * nf]))
    late.append(pltpu.make_async_copy(cot_hbm.at[:, chunk], cot, in_sems.at[2 * nf + 1]))
    late.append(pltpu.make_async_copy(w_hbm, w, in_sems.at[2 * nf + 2]))
    for copy in early + late:
        copy.start()
    pick = picks(rep_ref[...], (h * nc + c) * part, part)
    incs = [flip(inc_ref[:, lax.rem(h - j + nf, nf)].reshape(slots, feats)) for j in range(nf)]
    adds = [dot(inc, pick, 1, 1) for inc in incs]
    for copy in early:
        copy.wait()
    for j in range(nf):
        f = lax.rem(h - j + nf, nf)
        total = terms[j].astype(F32) + adds[j]
        rows[pl.ds(pl.multiple_of(wide + f * feats, feats), feats), :] = total.astype(BF)
    out_copies = []

    def put(src, dst):
        copy = pltpu.make_async_copy(src, dst, out_sems.at[len(out_copies)])
        copy.start()
        out_copies.append(copy)

    put(rows.at[wide:], agg_hbm)
    for copy in late:
        copy.wait()
    step = 256 if part % 256 == 0 else 128
    for b in range(0, part, step):
        cols = slice(b, b + step)
        z = dot(wt[...], rows[:, cols])
        s = 0.5 + 0.5 * jnp.tanh(0.5 * z)
        out[:, cols] = (z * s).astype(BF)
        g = (cot[:, cols].astype(F32) * (s * (1.0 + z * (1.0 - s)))).astype(BF)
        g_all[:, cols] = g
        both[:, cols] = dot(w[...], g).astype(BF)
        for j in range(nf):
            at = lax.rem(h + j, nf)
            peer = pl.ds(pl.multiple_of(wide + at * feats, feats), feats)
            put(both.at[peer, cols], grads[j].at[:, cols])
            put(both.at[place(at), cols], selfs[j].at[:, cols])
        put(g_all.at[:, cols], g_hbm.at[:, cols])
        put(out.at[:, cols], out_hbm.at[:, pl.ds(c * part + b, step)])
    pay = dot(both[wide:, :], pick)
    if c:
        pay = pay + pay_in[...].astype(F32)
    pay = pay.astype(BF)
    if c + 1 < nc:
        pay_ref[...] = pay
    else:
        for f in range(nf):
            mine = flip(pay[f * feats : (f + 1) * feats])
            pay_ref[:, f] = mine.reshape(pay_ref.shape[0], pay_ref.shape[2], feats)
    for copy in out_copies:
        copy.wait()


def weight_kernel(nf, nc, *refs):
    xs, aggs, grads = refs[:nf], refs[nf : nf + nc], refs[nf + nc : nf + 2 * nc]
    keep_ref, send_ref, acc = refs[nf + 2 * nc :]
    h = lax.axis_index("feat")
    bit = lax.rem(lax.axis_index("dom"), 2)
    wide = acc.shape[1]
    feats = wide // nf
    part = grads[0].shape[1]

    def summed(terms):
        total = None
        for left, right in terms:
            term = dot(left, right, 1, 1)
            total = term if total is None else total + term
        return total

    acc[wide:, :] = summed((aggs[c][...], grads[c][...]) for c in range(nc))
    for j in range(nf):
        at = pl.multiple_of(lax.rem(h - j + nf, nf) * feats, feats)
        acc[pl.ds(at, feats), :] = summed(
            (xs[j][:, c * part : (c + 1) * part], grads[c][...]) for c in range(nc)
        )
    for j in range(nf):
        at = lax.rem(h + j, nf) * feats
        keep_ref[j] = acc[pl.ds(pl.multiple_of(bit * wide + at, feats), feats), :]
        send_ref[j] = acc[pl.ds(pl.multiple_of((1 - bit) * wide + at, feats), feats), :].astype(BF)


def radices_of(n):
    radices = [2] * min(2, n.bit_length() - 1)
    n //= 1 << len(radices)
    while n > 1:
        radices.append(4 if n % 4 == 0 else 2)
        n //= radices[-1]
    return tuple(radices)


def unit_of(radices, k):
    unit = 1
    for r in radices[:k]:
        unit *= r
    return unit


def relative(radices, m):
    number = 0
    size = unit_of(radices, len(radices))
    for k, r in enumerate(radices):
        size //= r
        number += (m // size) % r * unit_of(radices, k)
    return number


def assemble_kernel(radices, own_ref, other_ref, out_ref):
    d = lax.axis_index("dom")
    nd = 1
    for r in radices:
        nd *= r
    rows = out_ref.shape[0] // nd
    half = nd // 2
    for m in range(nd):
        at, owner, height = 0, d ^ relative(radices, m), out_ref.shape[0]
        for r in radices:
            height //= r
            at = at + lax.rem(owner, r) * height
            owner = owner // r
        ref, k = (own_ref, m) if m < half else (other_ref, m - half)
        piece = ref[k * rows : (k + 1) * rows, :]
        out_ref[pl.ds(pl.multiple_of(at, rows), rows), :] = piece.astype(F32)


def back_kernel(nf, nc, tile, blocks, count, mirrors, values_ref, *rest):
    grads = rest[: nf * nc]
    back_ref, push_ref, acc, x_all, values, tiles, sources, targets, sems = rest[nf * nc :]
    lists = (tiles, sources, targets)
    h = lax.axis_index("feat")
    feats, masters = back_ref.shape
    slots = x_all.shape[1] - masters
    part = masters // nf // nc
    copies = [pltpu.make_async_copy(values_ref, values, sems.at[nf * nc])]
    for j in range(nf):
        for c in range(nc):
            k = j * nc + c
            at = pl.multiple_of((lax.rem(h - j + nf, nf) * nc + c) * part, 128)
            copies.append(
                pltpu.make_async_copy(grads[k], x_all.at[:, pl.ds(at, part)], sems.at[k])
            )
    for copy in copies:
        copy.start()
    acc[...] = jnp.zeros_like(acc)
    total = mirrors[:, 0].astype(F32)
    for f in range(1, nf):
        total = total + mirrors[:, f].astype(F32)
    x_all[:, masters:] = flip(total.astype(BF).reshape(slots, feats))
    list_tiles(blocks, count[0], lists, 1, acc.shape[1] // tile - 1, 0, x_all.shape[1] // tile)
    for copy in copies:
        copy.wait()
    run_tiles(count[0], lists, values, 1, x_all, acc, tile)
    partial = acc[:, masters : masters + slots].astype(BF)
    push_ref[...] = flip(partial).reshape(push_ref.shape)
    back_ref[...] = acc[:, :masters].astype(BF)


def final_kernel(nf, nc, rep_ref, inc_ref, back_ref, *rest):
    selfs, out_ref = rest[: nf * nc], rest[nf * nc]
    h = lax.axis_index("feat")
    feats, part = selfs[0].shape
    slots = rep_ref.shape[1]
    inc = flip(inc_ref[...].reshape(slots, feats))
    for j in range(nf):
        for c in range(nc):
            at = pl.multiple_of((lax.rem(h - j + nf, nf) * nc + c) * part, 128)
            back = back_ref[:, pl.ds(at, part)].astype(F32)
            back = back + dot(inc, picks(rep_ref[...], at, part), 1, 1)
            own = selfs[j * nc + c][...].astype(F32)
            out_ref[:, pl.ds(at, part)] = (own + back).astype(BF)


def local(nd, nf, features, weights, tile_values, tile_blocks, tile_counts, replica, cotangent):
    feats, masters = features.shape
    wide = weights.shape[1]
    ntiles, tile, _ = tile_values.shape
    per = replica.shape[2]
    slots = nd * per
    width = masters // nf
    cols = masters + slots + tile
    nc = 2 if width % (2 * tile) == 0 else 1
    part = width // nc
    d = lax.axis_index("dom")
    sd = jax.ShapeDtypeStruct
    lists = [pltpu.SMEM((ntiles + GROUP,), jnp.int32)] * 3
    tile_flops = 2 * ntiles * feats * tile * tile

    def call(body, flops, args, specs, outs, scratch=(), grid=(), out_specs=None, alias={}):
        return pl.pallas_call(
            body,
            grid=grid,
            in_specs=[full(a) if p is None else p for a, p in zip(args, specs, strict=True)],
            out_specs=out_specs or [full(o) for o in outs],
            out_shape=outs,
            scratch_shapes=list(scratch),
            input_output_aliases=alias,
            cost_estimate=cost(flops, 2 * sum(a.size for a in args)),
        )(*args)

    def to_peer(x, j):
        return lax.ppermute(x, "feat", [(i, (i + j) % nf) for i in range(nf)])

    def exchange(x, axes):
        flat = x.reshape(-1, per, feats)
        return lax.all_to_all(flat, axes, 0, 0, tiled=True).reshape(x.shape)

    def tile_scratch(nsems):
        return [
            pltpu.VMEM((feats, cols), F32),
            pltpu.VMEM((feats, masters + slots), BF),
            pltpu.VMEM(tile_values.shape, BF),
            *lists,
            pltpu.SemaphoreType.DMA((nsems,)),
        ]

    vec = sd((feats, width), BF)
    pull, rep, *x_halves = call(
        functools.partial(prep_kernel, nf),
        2 * slots * feats * masters,
        [features, replica],
        [None] * 2,
        [sd((nd, per, feats), BF), sd((1, slots), jnp.int32)] + [vec] * nf,
    )
    mirrors = exchange(pull, "dom")
    x_parts = [x_halves[0]] + [to_peer(x_halves[j], j) for j in range(1, nf)]

    blocks = tile_blocks.T
    chunk = sd((feats, part), BF)
    sums = pltpu.VMEM((feats, cols), F32)
    all_values = pltpu.VMEM(tile_values.shape, BF)
    pair = pltpu.SemaphoreType.DMA((2,))
    (own_sums,) = call(
        functools.partial(spread_own, tile),
        tile_flops,
        [blocks, tile_counts, features, tile_values],
        [SMEM, SMEM, ANY, ANY],
        [sd((feats, masters + slots), BF)],
        [sums, pltpu.VMEM((feats, masters), BF), all_values, *lists, pair],
    )
    own_part, push, *part_sends = call(
        functools.partial(spread_mirrors, nf, nc, tile),
        tile_flops // 4,
        [blocks, tile_counts, mirrors, tile_values, own_sums],
        [SMEM, SMEM, None, ANY, ANY],
        [vec, sd((nd, nf, per, feats), BF)] + [chunk] * ((nf - 1) * nc),
        [
            sums,
            pltpu.VMEM((feats, masters + slots), BF),
            pltpu.VMEM((feats, slots), BF),
            all_values,
            *lists,
            pair,
        ],
    )
    part_recv = [
        [to_peer(part_sends[(j - 1) * nc + c], j) for j in range(1, nf)]
        for c in range(nc)
    ]
    incoming = exchange(push, ("dom", "feat"))

    flat_w = weights.reshape(2 * wide, wide)
    wt = flat_w.T
    rows, grads, grad_own, grad_recv, self_own, self_recv = [], [], [], [], [], []
    step = 256 if part % 256 == 0 else 128
    for c in range(nc):
        last = c + 1 == nc
        args = [rep, incoming, wt, flat_w, cotangent, *x_parts, own_part, *part_recv[c]]
        specs = [None] * 2 + [ANY] * (len(args) - 2)
        alias = {}
        if c:
            alias = {len(args) + 1: 1}
            args += [pay, output]
            specs += [None, ANY]
        outs = [
            sd((wide, part), BF),
            sd((wide, width), BF),
            sd((wide, part), BF),
            sd((nd, nf, per, feats) if last else (wide, slots), BF),
        ] + [chunk] * (2 * nf)
        rows_c, output, g_c, pay, *res = call(
            functools.partial(dense_kernel, nf, nc, c),
            8 * wide * wide * part,
            args,
            specs,
            outs,
            [
                pltpu.VMEM((wide, 2 * wide), BF),
                pltpu.VMEM((2 * wide, wide), BF),
                pltpu.VMEM((wide, part), BF),
                pltpu.VMEM((2 * wide, part), BF),
                pltpu.VMEM((nf, feats, part), BF),
                pltpu.VMEM((wide, part), BF),
                pltpu.VMEM((wide, part), BF),
                pltpu.VMEM((2 * wide, part), BF),
                pltpu.SemaphoreType.DMA((2 * nf + 3,)),
                pltpu.SemaphoreType.DMA((1 + (part // step) * (2 * nf + 2),)),
            ],
            (),
            [ANY] * 3 + [full(outs[3])] + [ANY] * (2 * nf),
            alias,
        )
        rows.append(rows_c)
        grads.append(g_c)
        grad_own.append(res[0])
        self_own.append(res[nf])
        grad_recv.append([to_peer(res[j], j) for j in range(1, nf)])
        self_recv.append([to_peer(res[nf + j], j) for j in range(1, nf)])
    grad_mirrors = exchange(pay, ("dom", "feat"))

    keep, send = call(
        functools.partial(weight_kernel, nf, nc),
        4 * wide * wide * width,
        x_parts + rows + grads,
        [None] * (nf + 2 * nc),
        [sd((nf, feats, wide), F32), sd((nf, feats, wide), BF)],
        [pltpu.VMEM((2 * wide, wide), F32)],
    )

    flat_grads = grad_own + [grad_recv[c][j] for j in range(nf - 1) for c in range(nc)]
    back, push = call(
        functools.partial(back_kernel, nf, nc, tile),
        tile_flops,
        [blocks, tile_counts, grad_mirrors, tile_values, *flat_grads],
        [SMEM, SMEM, None, ANY] + [ANY] * (nf * nc),
        [sd((feats, masters), BF), sd((nd, per, feats), BF)],
        tile_scratch(nf * nc + 1),
    )
    back_in = exchange(push, "dom")

    radices = radices_of(nd)

    def swap(x, b):
        return lax.ppermute(x, "dom", [(i, i ^ b) for i in range(nd)])

    sends = [send]
    for k, r in enumerate(radices):
        unit = unit_of(radices, k)
        cur = keep
        for m in range(1, r):
            cur = cur + swap(sends[m - 1], m * unit).astype(F32)
        if k + 1 == len(radices):
            break
        size = cur.shape[1] // radices[k + 1]
        digit = lax.rem(d // unit_of(radices, k + 1), radices[k + 1])
        pieces = [
            lax.dynamic_slice_in_dim(cur, (digit ^ m) * size, size, 1)
            for m in range(radices[k + 1])
        ]
        keep, sends = pieces[0], [piece.astype(BF) for piece in pieces[1:]]
    total = cur[0]
    for j in range(1, nf):
        total = total + to_peer(cur[j], j)
    total = total.astype(BF)
    for k in reversed(range(1, len(radices))):
        unit = unit_of(radices, k)
        others = [swap(total, m * unit) for m in range(1, radices[k])]
        total = jnp.concatenate([total, *others], 0)
    other = swap(total, 1)
    if total.shape[0] * 2 // nd % 8 == 0:
        (weight_grad,) = call(
            functools.partial(assemble_kernel, radices),
            0,
            [total, other],
            [None] * 2,
            [sd((2 * feats, wide), F32)],
        )
    else:
        total = jnp.concatenate([total, other], 0).reshape(nd, -1, wide)
        owners = jnp.arange(nd)
        place, rest = jnp.zeros_like(owners), owners
        for r in radices:
            place, rest = place * r + rest % r, rest // r
        held = jnp.zeros_like(owners).at[place].set(owners) ^ d
        numbers = jnp.array([relative(radices, m) for m in range(nd)])
        index = jnp.zeros_like(owners).at[numbers].set(jnp.arange(nd))[held]
        weight_grad = total[index].reshape(2 * feats, wide).astype(F32)
    weight_grad = weight_grad.reshape(2, feats, wide)

    selfs = [self_own[c] for c in range(nc)]
    selfs += [self_recv[c][j] for j in range(nf - 1) for c in range(nc)]
    (feature_grad,) = call(
        functools.partial(final_kernel, nf, nc),
        2 * slots * feats * masters,
        [rep, back_in, back, *selfs],
        [None] * (3 + nf * nc),
        [sd((feats, masters), BF)],
    )
    return output, feature_grad, weight_grad


def solution(mesh):
    return jax.shard_map(
        functools.partial(local, mesh.shape["dom"], mesh.shape["feat"]),
        mesh=mesh,
        in_specs=(
            P("feat", "dom"),
            P(),
            P("dom", None, None),
            P("dom", None),
            P("dom"),
            P("dom", None, None),
            P(None, ("dom", "feat")),
        ),
        out_specs=(P(None, ("dom", "feat")), P("feat", "dom"), P(None, "feat", None)),
        check_vma=False,
    )
```

```python
import functools

import jax
import jax.numpy as jnp
from jax import lax
from jax.experimental import pallas as pl
from jax.experimental.pallas import tpu as pltpu
from jax.sharding import PartitionSpec as P

BF = jnp.bfloat16
F32 = jnp.float32
GROUP = 8
SMALL = 24 * 1024 * 1024


def dot(a, b, ca=1, cb=0):
    return lax.dot_general(a, b, (((ca,), (cb,)), ((), ())), preferred_element_type=F32)


def eye(n):
    rows = lax.broadcasted_iota(jnp.int32, (n, n), 0)
    cols = lax.broadcasted_iota(jnp.int32, (n, n), 1)
    return jnp.where(rows == cols, 1.0, 0.0).astype(BF)


def picks(slots, start, height):
    rows = lax.broadcasted_iota(jnp.int32, (height, slots.shape[1]), 0) + start
    return jnp.where(rows == slots, 1.0, 0.0).astype(BF)


def flip(x):
    return dot(eye(x.shape[1]), x, 1, 1).astype(BF)


SMEM = pl.BlockSpec(memory_space=pltpu.SMEM)
ANY = pl.BlockSpec(memory_space=pl.ANY)


def full(x):
    zeros = (0,) * len(x.shape)
    return pl.BlockSpec(x.shape, lambda *_: zeros)


def cost(flops, nbytes):
    return pl.CostEstimate(flops=int(flops), bytes_accessed=int(nbytes), transcendentals=0)


def block_of(n):
    return next(b for b in (512, 256, 128) if n % b == 0)


def list_tiles(blocks, count, lists, source_col, trash, low, high):
    tiles, sources, targets = lists

    def step(t, n):
        source = blocks[source_col, t]
        tiles[n] = t
        sources[n] = source - low
        targets[n] = blocks[1 - source_col, t]
        return n + jnp.logical_and(source >= low, source < high).astype(jnp.int32)

    n = lax.fori_loop(0, count, step, jnp.int32(0))
    for u in range(GROUP):
        tiles[n + u] = 0
        sources[n + u] = 0
        targets[n + u] = trash
    return n


def run_tiles(n, lists, values, tile_dim, x_all, acc, tile):
    tiles, sources, targets = lists

    def step(g, _):
        for u in range(GROUP):
            at = g * GROUP + u
            picked = column(x_all, sources[at], tile)
            part = dot(picked, values[tiles[at]], 1, tile_dim)
            col = pl.ds(pl.multiple_of(targets[at] * tile, tile), tile)
            acc[:, col] += part
        return 0

    lax.fori_loop(0, (n + GROUP - 1) // GROUP, step, 0)


def column(ref, block, tile):
    at = pl.multiple_of(block * tile, tile)
    return ref[:, pl.ds(at, tile)]


def prep_kernel(nf, x_ref, replica, pull_ref, rep_ref, *halves):
    rep_ref[...] = jnp.concatenate(
        [replica[0, p : p + 1, :] for p in range(replica.shape[1])], axis=1
    )
    h = lax.axis_index("feat")
    _, masters = x_ref.shape
    width = halves[0].shape[1]
    step = block_of(masters)
    total = None
    for at in range(0, masters, step):
        part = dot(x_ref[:, at : at + step], picks(rep_ref[...], at, step))
        total = part if total is None else total + part
    pull_ref[...] = flip(total.astype(BF)).reshape(pull_ref.shape)
    for j in range(nf):
        at = pl.multiple_of(lax.rem(h + j, nf) * width, 128)
        halves[j][...] = x_ref[:, pl.ds(at, width)]


def spread_own(tile, blocks, count, x_ref, values_ref, out_ref, acc, x, values, *rest):
    lists, sems = rest[:3], rest[3]
    masters = x.shape[1]
    copies = [
        pltpu.make_async_copy(x_ref, x, sems.at[0]),
        pltpu.make_async_copy(values_ref, values, sems.at[1]),
    ]
    for copy in copies:
        copy.start()
    acc[...] = jnp.zeros_like(acc)
    n = list_tiles(blocks, count[0], lists, 0, acc.shape[1] // tile - 1, 0, masters // tile)
    for copy in copies:
        copy.wait()
    run_tiles(n, lists, values, 0, x, acc, tile)
    out_ref[...] = acc[:, : out_ref.shape[1]].astype(BF)


def spread_mirrors(nf, nc, tile, blocks, count, mirrors, values_ref, own_ref, *rest):
    part_ref, push_ref = rest[:2]
    sends = rest[2 : 2 + (nf - 1) * nc]
    acc, own, x, values, *lists, sems = rest[2 + (nf - 1) * nc :]
    h = lax.axis_index("feat")
    feats, width = part_ref.shape
    slots = x.shape[1]
    masters = own.shape[1] - slots
    copies = [
        pltpu.make_async_copy(values_ref, values, sems.at[0]),
        pltpu.make_async_copy(own_ref, own, sems.at[1]),
    ]
    for copy in copies:
        copy.start()
    acc[...] = jnp.zeros_like(acc)
    x[...] = flip(mirrors[...].reshape(slots, feats))
    low = masters // tile
    n = list_tiles(
        blocks, count[0], lists, 0, acc.shape[1] // tile - 1, low, own.shape[1] // tile
    )
    for copy in copies:
        copy.wait()
    run_tiles(n, lists, values, 0, x, acc, tile)

    def total(at, size):
        return (own[:, pl.ds(at, size)].astype(F32) + acc[:, pl.ds(at, size)]).astype(BF)

    part = width // nc
    for j in range(1, nf):
        for c in range(nc):
            at = pl.multiple_of(lax.rem(h + j, nf) * width + c * part, 128)
            sends[(j - 1) * nc + c][...] = total(at, part)
    push = flip(total(masters, slots))
    push = push.reshape(push_ref.shape[0], push_ref.shape[2], feats)
    for f in range(nf):
        push_ref[:, f] = push
    part_ref[...] = total(pl.multiple_of(h * width, 128), width)


def dense_kernel(nf, nc, c, *refs):
    rep_ref, inc_ref, wt_hbm, w_hbm, cot_hbm = refs[:5]
    xs, parts = refs[5 : 5 + nf], refs[5 + nf : 5 + 2 * nf]
    refs = refs[5 + 2 * nf :]
    if c:
        pay_in = refs[0]
        refs = refs[2 + nf :]
    agg_hbm, out_hbm, g_hbm, pay_ref = refs[:4]
    grads, selfs = refs[4 : 4 + nf], refs[4 + nf : 4 + 2 * nf]
    wt, w, cot, rows, terms, out, g_all, both, in_sems, out_sems = refs[4 + 2 * nf :]
    h = lax.axis_index("feat")
    feats, part = grads[0].shape
    wide = w.shape[1]
    slots = rep_ref.shape[1]
    chunk = pl.ds(c * part, part)

    def place(f):
        return pl.ds(pl.multiple_of(f * feats, feats), feats)

    early, late = [], []
    for j in range(nf):
        f = lax.rem(h - j + nf, nf)
        term = parts[j].at[:, chunk] if j == 0 else parts[j]
        early.append(pltpu.make_async_copy(term, terms.at[j], in_sems.at[j]))
        x = xs[j].at[:, chunk]
        early.append(pltpu.make_async_copy(x, rows.at[place(f)], in_sems.at[nf + j]))
    late.append(pltpu.make_async_copy(wt_hbm, wt, in_sems.at[2 * nf]))
    late.append(pltpu.make_async_copy(cot_hbm.at[:, chunk], cot, in_sems.at[2 * nf + 1]))
    late.append(pltpu.make_async_copy(w_hbm, w, in_sems.at[2 * nf + 2]))
    for copy in early + late:
        copy.start()
    pick = picks(rep_ref[...], (h * nc + c) * part, part)
    incs = [flip(inc_ref[:, lax.rem(h - j + nf, nf)].reshape(slots, feats)) for j in range(nf)]
    adds = [dot(inc, pick, 1, 1) for inc in incs]
    for copy in early:
        copy.wait()
    for j in range(nf):
        f = lax.rem(h - j + nf, nf)
        total = terms[j].astype(F32) + adds[j]
        rows[pl.ds(pl.multiple_of(wide + f * feats, feats), feats), :] = total.astype(BF)
    out_copies = []

    def put(src, dst):
        copy = pltpu.make_async_copy(src, dst, out_sems.at[len(out_copies)])
        copy.start()
        out_copies.append(copy)

    put(rows.at[wide:], agg_hbm)
    for copy in late:
        copy.wait()
    step = 256 if part % 256 == 0 else 128
    for b in range(0, part, step):
        cols = slice(b, b + step)
        z = dot(wt[...], rows[:, cols])
        s = 0.5 + 0.5 * jnp.tanh(0.5 * z)
        out[:, cols] = (z * s).astype(BF)
        g = (cot[:, cols].astype(F32) * (s * (1.0 + z * (1.0 - s)))).astype(BF)
        g_all[:, cols] = g
        both[:, cols] = dot(w[...], g).astype(BF)
        for j in range(nf):
            at = lax.rem(h + j, nf)
            peer = pl.ds(pl.multiple_of(wide + at * feats, feats), feats)
            put(both.at[peer, cols], grads[j].at[:, cols])
            put(both.at[place(at), cols], selfs[j].at[:, pl.ds(c * part + b, step)])
        put(g_all.at[:, cols], g_hbm.at[:, cols])
        put(out.at[:, cols], out_hbm.at[:, pl.ds(c * part + b, step)])
    pay = dot(both[wide:, :], pick)
    if c:
        pay = pay + pay_in[...].astype(F32)
    pay = pay.astype(BF)
    if c + 1 < nc:
        pay_ref[...] = pay
    else:
        for f in range(nf):
            mine = flip(pay[f * feats : (f + 1) * feats])
            pay_ref[:, f] = mine.reshape(pay_ref.shape[0], pay_ref.shape[2], feats)
    for copy in out_copies:
        copy.wait()


def weight_kernel(nf, nc, *refs):
    ins = refs[: nf + 2 * nc]
    keep_ref, send_ref, acc = refs[nf + 2 * nc : nf + 2 * nc + 3]
    held, sems = refs[nf + 2 * nc + 3 : -1], refs[-1]
    h = lax.axis_index("feat")
    bit = lax.rem(lax.axis_index("dom"), 2)
    wide = acc.shape[1]
    feats = wide // nf
    copies = [pltpu.make_async_copy(a, b, sems.at[k]) for k, (a, b) in enumerate(zip(ins, held))]
    order = [[nf + nc + c, nf + c] for c in range(nc)]
    order[0] += list(range(nf))
    for group in order:
        for k in group:
            copies[k].start()
    xs, aggs, grads = held[:nf], held[nf : nf + nc], held[nf + nc :]
    part = grads[0].shape[1]
    for c in range(nc):
        for k in order[c]:
            copies[k].wait()
        terms = [(pl.ds(wide, wide), aggs[c][...])]
        for j in range(nf):
            at = pl.multiple_of(lax.rem(h - j + nf, nf) * feats, feats)
            terms.append((pl.ds(at, feats), xs[j][:, c * part : (c + 1) * part]))
        for at, left in terms:
            term = dot(left, grads[c][...], 1, 1)
            acc[at, :] = term if c == 0 else acc[at, :] + term
    for j in range(nf):
        at = lax.rem(h + j, nf) * feats
        keep_ref[j] = acc[pl.ds(pl.multiple_of(bit * wide + at, feats), feats), :]
        send_ref[j] = acc[pl.ds(pl.multiple_of((1 - bit) * wide + at, feats), feats), :].astype(BF)


def radices_of(n):
    radices = [2] * min(2, n.bit_length() - 1)
    n //= 1 << len(radices)
    while n > 1:
        radices.append(4 if n % 4 == 0 else 2)
        n //= radices[-1]
    return tuple(radices)


def unit_of(radices, k):
    unit = 1
    for r in radices[:k]:
        unit *= r
    return unit


def relative(radices, m):
    number = 0
    size = unit_of(radices, len(radices))
    for k, r in enumerate(radices):
        size //= r
        number += (m // size) % r * unit_of(radices, k)
    return number


def assemble_kernel(radices, own_ref, other_ref, out_ref):
    d = lax.axis_index("dom")
    nd = 1
    for r in radices:
        nd *= r
    rows = out_ref.shape[0] // nd
    half = nd // 2
    for m in range(nd):
        at, owner, height = 0, d ^ relative(radices, m), out_ref.shape[0]
        for r in radices:
            height //= r
            at = at + lax.rem(owner, r) * height
            owner = owner // r
        ref, k = (own_ref, m) if m < half else (other_ref, m - half)
        piece = ref[k * rows : (k + 1) * rows, :]
        out_ref[pl.ds(pl.multiple_of(at, rows), rows), :] = piece.astype(F32)


def back_kernel(nf, nc, tile, blocks, count, mirrors, values_ref, *rest):
    grads = rest[: nf * nc]
    back_ref, push_ref, acc, x_all, values, tiles, sources, targets, sems = rest[nf * nc :]
    lists = (tiles, sources, targets)
    h = lax.axis_index("feat")
    feats, masters = back_ref.shape
    slots = x_all.shape[1] - masters
    part = masters // nf // nc
    copies = [pltpu.make_async_copy(values_ref, values, sems.at[nf * nc])]
    for j in range(nf):
        for c in range(nc):
            k = j * nc + c
            at = pl.multiple_of((lax.rem(h - j + nf, nf) * nc + c) * part, 128)
            copies.append(
                pltpu.make_async_copy(grads[k], x_all.at[:, pl.ds(at, part)], sems.at[k])
            )
    for copy in copies:
        copy.start()
    acc[...] = jnp.zeros_like(acc)
    total = mirrors[:, 0].astype(F32)
    for f in range(1, nf):
        total = total + mirrors[:, f].astype(F32)
    x_all[:, masters:] = flip(total.astype(BF).reshape(slots, feats))
    list_tiles(blocks, count[0], lists, 1, acc.shape[1] // tile - 1, 0, x_all.shape[1] // tile)
    for copy in copies:
        copy.wait()
    run_tiles(count[0], lists, values, 1, x_all, acc, tile)
    partial = acc[:, masters : masters + slots].astype(BF)
    push_ref[...] = flip(partial).reshape(push_ref.shape)
    back_ref[...] = acc[:, :masters].astype(BF)


def final_kernel(nf, nc, rep_ref, inc_ref, back_ref, *rest):
    selfs, out_ref = rest[:nf], rest[nf]
    h = lax.axis_index("feat")
    feats, width = selfs[0].shape
    part = width // nc
    slots = rep_ref.shape[1]
    inc = flip(inc_ref[...].reshape(slots, feats))
    for j in range(nf):
        for c in range(nc):
            at = pl.multiple_of((lax.rem(h - j + nf, nf) * nc + c) * part, 128)
            back = back_ref[:, pl.ds(at, part)].astype(F32)
            back = back + dot(inc, picks(rep_ref[...], at, part), 1, 1)
            own = selfs[j][:, c * part : (c + 1) * part].astype(F32)
            out_ref[:, pl.ds(at, part)] = (own + back).astype(BF)


def local(nd, nf, features, weights, tile_values, tile_blocks, tile_counts, replica, cotangent):
    feats, masters = features.shape
    wide = weights.shape[1]
    ntiles, tile, _ = tile_values.shape
    per = replica.shape[2]
    slots = nd * per
    width = masters // nf
    cols = masters + slots + tile
    nc = 2 if width % (2 * tile) == 0 else 1
    part = width // nc
    d = lax.axis_index("dom")
    sd = jax.ShapeDtypeStruct
    lists = [pltpu.SMEM((ntiles + GROUP,), jnp.int32)] * 3
    tile_flops = 2 * ntiles * feats * tile * tile

    def call(body, flops, args, specs, outs, scratch=(), grid=(), out_specs=None, alias={}, limit=None):
        return pl.pallas_call(
            body,
            grid=grid,
            in_specs=[full(a) if p is None else p for a, p in zip(args, specs, strict=True)],
            out_specs=out_specs or [full(o) for o in outs],
            out_shape=outs,
            scratch_shapes=list(scratch),
            input_output_aliases=alias,
            compiler_params=pltpu.CompilerParams(vmem_limit_bytes=limit),
            cost_estimate=cost(flops, 2 * sum(a.size for a in args)),
        )(*args)

    def to_peer(x, j):
        return lax.ppermute(x, "feat", [(i, (i + j) % nf) for i in range(nf)])

    def exchange(x, axes):
        flat = x.reshape(-1, per, feats)
        return lax.all_to_all(flat, axes, 0, 0, tiled=True).reshape(x.shape)

    def tile_scratch(nsems):
        return [
            pltpu.VMEM((feats, cols), F32),
            pltpu.VMEM((feats, masters + slots), BF),
            pltpu.VMEM(tile_values.shape, BF),
            *lists,
            pltpu.SemaphoreType.DMA((nsems,)),
        ]

    vec = sd((feats, width), BF)
    pull, rep, *x_halves = call(
        functools.partial(prep_kernel, nf),
        2 * slots * feats * masters,
        [features, replica],
        [None] * 2,
        [sd((nd, per, feats), BF), sd((1, slots), jnp.int32)] + [vec] * nf,
    )
    mirrors = exchange(pull, "dom")
    x_parts = [x_halves[0]] + [to_peer(x_halves[j], j) for j in range(1, nf)]

    blocks = tile_blocks.T
    chunk = sd((feats, part), BF)
    sums = pltpu.VMEM((feats, cols), F32)
    all_values = pltpu.VMEM(tile_values.shape, BF)
    pair = pltpu.SemaphoreType.DMA((2,))
    (own_sums,) = call(
        functools.partial(spread_own, tile),
        tile_flops,
        [blocks, tile_counts, features, tile_values],
        [SMEM, SMEM, ANY, ANY],
        [sd((feats, masters + slots), BF)],
        [sums, pltpu.VMEM((feats, masters), BF), all_values, *lists, pair],
    )
    own_part, push, *part_sends = call(
        functools.partial(spread_mirrors, nf, nc, tile),
        tile_flops // 4,
        [blocks, tile_counts, mirrors, tile_values, own_sums],
        [SMEM, SMEM, None, ANY, ANY],
        [vec, sd((nd, nf, per, feats), BF)] + [chunk] * ((nf - 1) * nc),
        [
            sums,
            pltpu.VMEM((feats, masters + slots), BF),
            pltpu.VMEM((feats, slots), BF),
            all_values,
            *lists,
            pair,
        ],
    )
    part_recv = [
        [to_peer(part_sends[(j - 1) * nc + c], j) for j in range(1, nf)]
        for c in range(nc)
    ]
    incoming = exchange(push, ("dom", "feat"))

    flat_w = weights.reshape(2 * wide, wide)
    wt = flat_w.T
    rows, grads, grad_own, grad_recv = [], [], [], []
    step = 256 if part % 256 == 0 else 128
    for c in range(nc):
        last = c + 1 == nc
        args = [rep, incoming, wt, flat_w, cotangent, *x_parts, own_part, *part_recv[c]]
        specs = [None] * 2 + [ANY] * (len(args) - 2)
        alias = {}
        if c:
            alias = {len(args) + 1: 1}
            alias |= {len(args) + 2 + j: 4 + nf + j for j in range(nf)}
            args += [pay, output, *selfs]
            specs += [None] + [ANY] * (1 + nf)
        outs = [
            sd((wide, part), BF),
            sd((wide, width), BF),
            sd((wide, part), BF),
            sd((nd, nf, per, feats) if last else (wide, slots), BF),
        ] + [chunk] * nf + [vec] * nf
        rows_c, output, g_c, pay, *res = call(
            functools.partial(dense_kernel, nf, nc, c),
            8 * wide * wide * part,
            args,
            specs,
            outs,
            [
                pltpu.VMEM((wide, 2 * wide), BF),
                pltpu.VMEM((2 * wide, wide), BF),
                pltpu.VMEM((wide, part), BF),
                pltpu.VMEM((2 * wide, part), BF),
                pltpu.VMEM((nf, feats, part), BF),
                pltpu.VMEM((wide, part), BF),
                pltpu.VMEM((wide, part), BF),
                pltpu.VMEM((2 * wide, part), BF),
                pltpu.SemaphoreType.DMA((2 * nf + 3,)),
                pltpu.SemaphoreType.DMA((1 + (part // step) * (2 * nf + 2),)),
            ],
            (),
            [ANY] * 3 + [full(outs[3])] + [ANY] * (2 * nf),
            alias,
        )
        rows.append(rows_c)
        grads.append(g_c)
        grad_own.append(res[0])
        selfs = res[nf:]
        grad_recv.append([to_peer(res[j], j) for j in range(1, nf)])
    selfs = [selfs[0]] + [to_peer(selfs[j], j) for j in range(1, nf)]
    grad_mirrors = exchange(pay, ("dom", "feat"))

    keep, send = call(
        functools.partial(weight_kernel, nf, nc),
        4 * wide * wide * width,
        x_parts + rows + grads,
        [ANY] * (nf + 2 * nc),
        [sd((nf, feats, wide), F32), sd((nf, feats, wide), BF)],
        [pltpu.VMEM((2 * wide, wide), F32)]
        + [pltpu.VMEM((feats, width), BF)] * nf
        + [pltpu.VMEM((wide, part), BF)] * (2 * nc)
        + [pltpu.SemaphoreType.DMA((nf + 2 * nc,))],
    )

    flat_grads = grad_own + [grad_recv[c][j] for j in range(nf - 1) for c in range(nc)]
    back, push = call(
        functools.partial(back_kernel, nf, nc, tile),
        tile_flops,
        [blocks, tile_counts, grad_mirrors, tile_values, *flat_grads],
        [SMEM, SMEM, None, ANY] + [ANY] * (nf * nc),
        [sd((feats, masters), BF), sd((nd, per, feats), BF)],
        tile_scratch(nf * nc + 1),
    )
    back_in = exchange(push, "dom")

    radices = radices_of(nd)

    def swap(x, b):
        return lax.ppermute(x, "dom", [(i, i ^ b) for i in range(nd)])

    sends = [send]
    for k, r in enumerate(radices):
        unit = unit_of(radices, k)
        cur = keep
        for m in range(1, r):
            cur = cur + swap(sends[m - 1], m * unit).astype(F32)
        if k + 1 == len(radices):
            break
        size = cur.shape[1] // radices[k + 1]
        digit = lax.rem(d // unit_of(radices, k + 1), radices[k + 1])
        pieces = [
            lax.dynamic_slice_in_dim(cur, (digit ^ m) * size, size, 1)
            for m in range(radices[k + 1])
        ]
        keep, sends = pieces[0], [piece.astype(BF) for piece in pieces[1:]]
    total = cur[0]
    for j in range(1, nf):
        total = total + to_peer(cur[j], j)
    total = total.astype(BF)
    for k in reversed(range(1, len(radices))):
        unit = unit_of(radices, k)
        others = [swap(total, m * unit) for m in range(1, radices[k])]
        total = jnp.concatenate([total, *others], 0)
    other = swap(total, 1)
    if total.shape[0] * 2 // nd % 8 == 0:
        (weight_grad,) = call(
            functools.partial(assemble_kernel, radices),
            0,
            [total, other],
            [None] * 2,
            [sd((2 * feats, wide), F32)],
            limit=SMALL,
        )
    else:
        total = jnp.concatenate([total, other], 0).reshape(nd, -1, wide)
        owners = jnp.arange(nd)
        place, rest = jnp.zeros_like(owners), owners
        for r in radices:
            place, rest = place * r + rest % r, rest // r
        held = jnp.zeros_like(owners).at[place].set(owners) ^ d
        numbers = jnp.array([relative(radices, m) for m in range(nd)])
        index = jnp.zeros_like(owners).at[numbers].set(jnp.arange(nd))[held]
        weight_grad = total[index].reshape(2 * feats, wide).astype(F32)
    weight_grad = weight_grad.reshape(2, feats, wide)

    (feature_grad,) = call(
        functools.partial(final_kernel, nf, nc),
        2 * slots * feats * masters,
        [rep, back_in, back, *selfs],
        [None] * (3 + nf),
        [sd((feats, masters), BF)],
        limit=SMALL,
    )
    return output, feature_grad, weight_grad


def solution(mesh):
    return jax.shard_map(
        functools.partial(local, mesh.shape["dom"], mesh.shape["feat"]),
        mesh=mesh,
        in_specs=(
            P("feat", "dom"),
            P(),
            P("dom", None, None),
            P("dom", None),
            P("dom"),
            P("dom", None, None),
            P(None, ("dom", "feat")),
        ),
        out_specs=(P(None, ("dom", "feat")), P("feat", "dom"), P(None, "feat", None)),
        check_vma=False,
    )
```

```python
import functools

import jax
import jax.numpy as jnp
from jax import lax
from jax.experimental import pallas as pl
from jax.experimental.pallas import tpu as pltpu
from jax.sharding import PartitionSpec as P

BF = jnp.bfloat16
F32 = jnp.float32
GROUP = 8
SMALL = 24 * 1024 * 1024


def dot(a, b, ca=1, cb=0):
    return lax.dot_general(a, b, (((ca,), (cb,)), ((), ())), preferred_element_type=F32)


def eye(n):
    rows = lax.broadcasted_iota(jnp.int32, (n, n), 0)
    cols = lax.broadcasted_iota(jnp.int32, (n, n), 1)
    return jnp.where(rows == cols, 1.0, 0.0).astype(BF)


def picks(slots, start, height):
    rows = lax.broadcasted_iota(jnp.int32, (height, slots.shape[1]), 0) + start
    return jnp.where(rows == slots, 1.0, 0.0).astype(BF)


def flip(x):
    return dot(eye(x.shape[1]), x, 1, 1).astype(BF)


SMEM = pl.BlockSpec(memory_space=pltpu.SMEM)
ANY = pl.BlockSpec(memory_space=pl.ANY)


def full(x):
    zeros = (0,) * len(x.shape)
    return pl.BlockSpec(x.shape, lambda *_: zeros)


def cost(flops, nbytes):
    return pl.CostEstimate(flops=int(flops), bytes_accessed=int(nbytes), transcendentals=0)


def list_tiles(blocks, count, lists, source_col, trash, low, high):
    tiles, sources, targets = lists

    def step(t, n):
        source = blocks[source_col, t]
        tiles[n] = t
        sources[n] = source - low
        targets[n] = blocks[1 - source_col, t]
        return n + jnp.logical_and(source >= low, source < high).astype(jnp.int32)

    n = lax.fori_loop(0, count, step, jnp.int32(0))
    for u in range(GROUP):
        tiles[n + u] = 0
        sources[n + u] = 0
        targets[n + u] = trash
    return n


def blocks_of(width, body, size=256):
    size = size if width % size == 0 else 128

    def step(i, _):
        body(pl.ds(pl.multiple_of(i * size, size), size))
        return 0

    lax.fori_loop(0, width // size, step, 0)


def clear(acc):
    def zero(cols):
        acc[:, cols] = jnp.zeros((acc.shape[0], cols.size), acc.dtype)

    blocks_of(acc.shape[1], zero)


def run_tiles(n, lists, values, tile_dim, x_all, acc, tile):
    tiles, sources, targets = lists

    def step(g, _):
        for u in range(GROUP):
            at = g * GROUP + u
            picked = column(x_all, sources[at], tile)
            part = dot(picked, values[tiles[at]], 1, tile_dim)
            col = pl.ds(pl.multiple_of(targets[at] * tile, tile), tile)
            acc[:, col] += part
        return 0

    lax.fori_loop(0, (n + GROUP - 1) // GROUP, step, 0)


def column(ref, block, tile):
    at = pl.multiple_of(block * tile, tile)
    return ref[:, pl.ds(at, tile)]


def prep_kernel(nf, x_ref, replica, pull_ref, rep_ref, *rest):
    halves, total = rest[:nf], rest[nf]
    rep_ref[...] = jnp.concatenate(
        [replica[0, p : p + 1, :] for p in range(replica.shape[1])], axis=1
    )
    h = lax.axis_index("feat")
    width = halves[0].shape[1]
    total[...] = jnp.zeros_like(total)

    def gather(cols):
        total[...] += dot(x_ref[:, cols], picks(rep_ref[...], cols.start, cols.size))

    blocks_of(x_ref.shape[1], gather, 512)
    pull_ref[...] = flip(total[...].astype(BF)).reshape(pull_ref.shape)
    for j in range(nf):
        at = pl.multiple_of(lax.rem(h + j, nf) * width, 128)

        def take(cols, j=j, at=at):
            halves[j][:, cols] = x_ref[:, pl.ds(pl.multiple_of(at + cols.start, 128), cols.size)]

        blocks_of(width, take)


def spread_own(tile, blocks, count, x_ref, values_ref, out_ref, acc, x, values, *rest):
    lists, sems = rest[:3], rest[3]
    masters = x.shape[1]
    copies = [
        pltpu.make_async_copy(x_ref, x, sems.at[0]),
        pltpu.make_async_copy(values_ref, values, sems.at[1]),
    ]
    for copy in copies:
        copy.start()
    clear(acc)
    n = list_tiles(blocks, count[0], lists, 0, acc.shape[1] // tile - 1, 0, masters // tile)
    for copy in copies:
        copy.wait()
    run_tiles(n, lists, values, 0, x, acc, tile)

    def store(cols):
        out_ref[:, cols] = acc[:, cols].astype(BF)

    blocks_of(out_ref.shape[1], store)


def spread_mirrors(nf, nc, tile, blocks, count, mirrors, values_ref, own_ref, *rest):
    part_ref, push_ref = rest[:2]
    sends = rest[2 : 2 + (nf - 1) * nc]
    acc, own, x, values, *lists, sems = rest[2 + (nf - 1) * nc :]
    h = lax.axis_index("feat")
    feats, width = part_ref.shape
    slots = x.shape[1]
    masters = own.shape[1] - slots
    copies = [
        pltpu.make_async_copy(values_ref, values, sems.at[0]),
        pltpu.make_async_copy(own_ref, own, sems.at[1]),
    ]
    for copy in copies:
        copy.start()
    clear(acc)
    x[...] = flip(mirrors[...].reshape(slots, feats))
    low = masters // tile
    n = list_tiles(
        blocks, count[0], lists, 0, acc.shape[1] // tile - 1, low, own.shape[1] // tile
    )
    for copy in copies:
        copy.wait()
    run_tiles(n, lists, values, 0, x, acc, tile)

    def total(at, size):
        return (own[:, pl.ds(at, size)].astype(F32) + acc[:, pl.ds(at, size)]).astype(BF)

    part = width // nc

    def store(ref, at):
        def block(cols):
            ref[:, cols] = total(pl.multiple_of(at + cols.start, 128), cols.size)

        blocks_of(ref.shape[1], block)

    for j in range(1, nf):
        for c in range(nc):
            store(sends[(j - 1) * nc + c], lax.rem(h + j, nf) * width + c * part)
    push = flip(total(masters, slots))
    push = push.reshape(push_ref.shape[0], push_ref.shape[2], feats)
    for f in range(nf):
        push_ref[:, f] = push
    store(part_ref, h * width)


def dense_kernel(nf, nc, c, *refs):
    rep_ref, inc_ref, wt_hbm, w_hbm, cot_hbm = refs[:5]
    xs, parts = refs[5 : 5 + nf], refs[5 + nf : 5 + 2 * nf]
    refs = refs[5 + 2 * nf :]
    if c:
        pay_in = refs[0]
        refs = refs[2 + nf :]
    agg_hbm, out_hbm, g_hbm, pay_ref = refs[:4]
    grads, selfs = refs[4 : 4 + nf], refs[4 + nf : 4 + 2 * nf]
    wt, w, cot, rows, terms, out, g_all, both, incs, pay, in_sems, out_sems = refs[4 + 2 * nf :]
    h = lax.axis_index("feat")
    feats, part = grads[0].shape
    wide = w.shape[1]
    slots = rep_ref.shape[1]
    chunk = pl.ds(c * part, part)

    def place(f):
        return pl.ds(pl.multiple_of(f * feats, feats), feats)

    def place_agg(f):
        return pl.ds(pl.multiple_of(wide + f * feats, feats), feats)

    copies = []
    for j in range(nf):
        f = lax.rem(h - j + nf, nf)
        term = parts[j].at[:, chunk] if j == 0 else parts[j]
        copies.append(pltpu.make_async_copy(term, terms.at[j], in_sems.at[j]))
        x = xs[j].at[:, chunk]
        copies.append(pltpu.make_async_copy(x, rows.at[place(f)], in_sems.at[nf + j]))
    copies.append(pltpu.make_async_copy(wt_hbm, wt, in_sems.at[2 * nf]))
    copies.append(pltpu.make_async_copy(cot_hbm.at[:, chunk], cot, in_sems.at[2 * nf + 1]))
    copies.append(pltpu.make_async_copy(w_hbm, w, in_sems.at[2 * nf + 2]))
    for copy in copies:
        copy.start()
    for j in range(nf):
        incs[j] = flip(inc_ref[:, lax.rem(h - j + nf, nf)].reshape(slots, feats))
    pay[...] = pay_in[...].astype(F32) if c else jnp.zeros_like(pay)
    for copy in copies:
        copy.wait()
    size = 256 if part % 256 == 0 else 128

    def outputs(b, at):
        cols = pl.ds(at, size)
        whole = pl.ds(pl.multiple_of(c * part + at, 128), size)
        pairs = [
            (rows.at[wide:, cols], agg_hbm.at[:, cols]),
            (g_all.at[:, cols], g_hbm.at[:, cols]),
            (out.at[:, cols], out_hbm.at[:, whole]),
        ]
        for j in range(nf):
            f = lax.rem(h + j, nf)
            pairs.append((both.at[place_agg(f), cols], grads[j].at[:, cols]))
            pairs.append((both.at[place(f), cols], selfs[j].at[:, whole]))
        return [
            pltpu.make_async_copy(a, o, out_sems.at[k, b]) for k, (a, o) in enumerate(pairs)
        ]

    def step(b, _):
        at = pl.multiple_of(b * size, size)
        cols = pl.ds(at, size)
        pick = picks(rep_ref[...], (h * nc + c) * part + at, size)
        for j in range(nf):
            total = terms[j, :, cols].astype(F32) + dot(incs[j], pick, 1, 1)
            rows[place_agg(lax.rem(h - j + nf, nf)), cols] = total.astype(BF)
        z = dot(wt[...], rows[:, cols])
        s = 0.5 + 0.5 * jnp.tanh(0.5 * z)
        out[:, cols] = (z * s).astype(BF)
        g = (cot[:, cols].astype(F32) * (s * (1.0 + z * (1.0 - s)))).astype(BF)
        g_all[:, cols] = g
        both[:, cols] = dot(w[...], g).astype(BF)
        for copy in outputs(b, at):
            copy.start()
        pay[...] += dot(both[wide:, cols], pick)
        return 0

    lax.fori_loop(0, part // size, step, 0)
    if c + 1 < nc:
        pay_ref[...] = pay[...].astype(BF)
    else:
        for f in range(nf):
            mine = flip(pay[f * feats : (f + 1) * feats].astype(BF))
            pay_ref[:, f] = mine.reshape(pay_ref.shape[0], pay_ref.shape[2], feats)
    for b in range(part // size):
        for copy in outputs(b, b * size):
            copy.wait()


def weight_kernel(nf, nc, *refs):
    ins = refs[: nf + 2 * nc]
    keep_ref, send_ref, acc = refs[nf + 2 * nc : nf + 2 * nc + 3]
    held, sems = refs[nf + 2 * nc + 3 : -1], refs[-1]
    h = lax.axis_index("feat")
    bit = lax.rem(lax.axis_index("dom"), 2)
    wide = acc.shape[1]
    feats = wide // nf
    copies = [pltpu.make_async_copy(a, b, sems.at[k]) for k, (a, b) in enumerate(zip(ins, held))]
    order = [[nf + nc + c, nf + c] for c in range(nc)]
    order[0] += list(range(nf))
    for group in order:
        for k in group:
            copies[k].start()
    xs, aggs, grads = held[:nf], held[nf : nf + nc], held[nf + nc :]
    part = grads[0].shape[1]
    size = min(256, feats)
    for c in range(nc):
        for k in order[c]:
            copies[k].wait()

        def add(at, left, c=c):
            term = dot(left, grads[c][...], 1, 1)
            acc[at, :] = term if c == 0 else acc[at, :] + term

        def step(i, _, c=c):
            at = pl.multiple_of(i * size, size)
            add(pl.ds(wide + at, size), aggs[c][pl.ds(at, size), :])
            return 0

        lax.fori_loop(0, wide // size, step, 0)
        for j in range(nf):
            at = pl.multiple_of(lax.rem(h - j + nf, nf) * feats, feats)
            add(pl.ds(at, feats), xs[j][:, c * part : (c + 1) * part])
    for j in range(nf):
        at = lax.rem(h + j, nf) * feats
        keep_ref[j] = acc[pl.ds(pl.multiple_of(bit * wide + at, feats), feats), :]
        send_ref[j] = acc[pl.ds(pl.multiple_of((1 - bit) * wide + at, feats), feats), :].astype(BF)


def combine_kernel(nf, radix, digit, keep_ref, *rest):
    recvs, out_ref, sends = rest[: -radix], rest[-radix], rest[-radix + 1 :]
    unit, base = digit
    mine = lax.rem(lax.axis_index("dom") // unit, base)
    size = out_ref.shape[1]
    for j in range(nf):
        for m in range(radix):
            at = pl.ds(pl.multiple_of(jnp.bitwise_xor(mine, m) * size, size), size)
            total = keep_ref[j, at, :]
            for recv in recvs:
                total = total + recv[j, at, :].astype(F32)
            if m == 0:
                out_ref[j] = total
            else:
                sends[m - 1][j] = total.astype(BF)


def radices_of(n):
    radices = [2] * min(2, n.bit_length() - 1)
    n //= 1 << len(radices)
    while n > 1:
        radices.append(4 if n % 4 == 0 else 2)
        n //= radices[-1]
    return tuple(radices)


def unit_of(radices, k):
    unit = 1
    for r in radices[:k]:
        unit *= r
    return unit


def relative(radices, m):
    number = 0
    size = unit_of(radices, len(radices))
    for k, r in enumerate(radices):
        size //= r
        number += (m // size) % r * unit_of(radices, k)
    return number


def assemble_kernel(radices, own_ref, other_ref, out_ref):
    d = lax.axis_index("dom")
    nd = 1
    for r in radices:
        nd *= r
    rows = out_ref.shape[0] // nd
    half = nd // 2
    for m in range(nd):
        at, owner, height = 0, d ^ relative(radices, m), out_ref.shape[0]
        for r in radices:
            height //= r
            at = at + lax.rem(owner, r) * height
            owner = owner // r
        ref, k = (own_ref, m) if m < half else (other_ref, m - half)
        piece = ref[k * rows : (k + 1) * rows, :]
        out_ref[pl.ds(pl.multiple_of(at, rows), rows), :] = piece.astype(F32)


def back_kernel(nf, nc, tile, blocks, count, mirrors, values_ref, *rest):
    grads = rest[: nf * nc]
    back_ref, push_ref, acc, x_all, values, tiles, sources, targets, sems = rest[nf * nc :]
    lists = (tiles, sources, targets)
    h = lax.axis_index("feat")
    feats, masters = back_ref.shape
    slots = x_all.shape[1] - masters
    part = masters // nf // nc
    copies = [pltpu.make_async_copy(values_ref, values, sems.at[nf * nc])]
    for j in range(nf):
        for c in range(nc):
            k = j * nc + c
            at = pl.multiple_of((lax.rem(h - j + nf, nf) * nc + c) * part, 128)
            copies.append(
                pltpu.make_async_copy(grads[k], x_all.at[:, pl.ds(at, part)], sems.at[k])
            )
    for copy in copies:
        copy.start()
    clear(acc)
    total = mirrors[:, 0].astype(F32)
    for f in range(1, nf):
        total = total + mirrors[:, f].astype(F32)
    x_all[:, masters:] = flip(total.astype(BF).reshape(slots, feats))
    list_tiles(blocks, count[0], lists, 1, acc.shape[1] // tile - 1, 0, x_all.shape[1] // tile)
    for copy in copies:
        copy.wait()
    run_tiles(count[0], lists, values, 1, x_all, acc, tile)
    partial = acc[:, masters : masters + slots].astype(BF)
    push_ref[...] = flip(partial).reshape(push_ref.shape)

    def store(cols):
        back_ref[:, cols] = acc[:, cols].astype(BF)

    blocks_of(masters, store)


def final_kernel(nf, rep_ref, inc_ref, back_ref, *rest):
    selfs, out_ref = rest[:nf], rest[nf]
    h = lax.axis_index("feat")
    feats, width = selfs[0].shape
    slots = rep_ref.shape[1]
    inc = flip(inc_ref[...].reshape(slots, feats))
    for j in range(nf):
        start = lax.rem(h - j + nf, nf) * width

        def block(cols, j=j, start=start):
            at = pl.multiple_of(start + cols.start, 128)
            here = pl.ds(at, cols.size)
            back = back_ref[:, here].astype(F32)
            back = back + dot(inc, picks(rep_ref[...], at, cols.size), 1, 1)
            out_ref[:, here] = (selfs[j][:, cols].astype(F32) + back).astype(BF)

        blocks_of(width, block)


def local(nd, nf, features, weights, tile_values, tile_blocks, tile_counts, replica, cotangent):
    feats, masters = features.shape
    wide = weights.shape[1]
    ntiles, tile, _ = tile_values.shape
    per = replica.shape[2]
    slots = nd * per
    width = masters // nf
    cols = masters + slots + tile
    nc = 2 if width % (2 * tile) == 0 else 1
    part = width // nc
    d = lax.axis_index("dom")
    sd = jax.ShapeDtypeStruct
    lists = [pltpu.SMEM((ntiles + GROUP,), jnp.int32)] * 3
    tile_flops = 2 * ntiles * feats * tile * tile

    def call(body, flops, args, specs, outs, scratch=(), grid=(), out_specs=None, alias={}, limit=None):
        return pl.pallas_call(
            body,
            grid=grid,
            in_specs=[full(a) if p is None else p for a, p in zip(args, specs, strict=True)],
            out_specs=out_specs or [full(o) for o in outs],
            out_shape=outs,
            scratch_shapes=list(scratch),
            input_output_aliases=alias,
            compiler_params=pltpu.CompilerParams(vmem_limit_bytes=limit),
            cost_estimate=cost(flops, 2 * sum(a.size for a in args)),
        )(*args)

    def to_peer(x, j):
        return lax.ppermute(x, "feat", [(i, (i + j) % nf) for i in range(nf)])

    def exchange(x, axes):
        flat = x.reshape(-1, per, feats)
        return lax.all_to_all(flat, axes, 0, 0, tiled=True).reshape(x.shape)

    def tile_scratch(nsems):
        return [
            pltpu.VMEM((feats, cols), F32),
            pltpu.VMEM((feats, masters + slots), BF),
            pltpu.VMEM(tile_values.shape, BF),
            *lists,
            pltpu.SemaphoreType.DMA((nsems,)),
        ]

    vec = sd((feats, width), BF)
    pull, rep, *x_halves = call(
        functools.partial(prep_kernel, nf),
        2 * slots * feats * masters,
        [features, replica],
        [None] * 2,
        [sd((nd, per, feats), BF), sd((1, slots), jnp.int32)] + [vec] * nf,
        [pltpu.VMEM((feats, slots), F32)],
    )
    mirrors = exchange(pull, "dom")
    x_parts = [x_halves[0]] + [to_peer(x_halves[j], j) for j in range(1, nf)]

    blocks = tile_blocks.T
    chunk = sd((feats, part), BF)
    sums = pltpu.VMEM((feats, cols), F32)
    all_values = pltpu.VMEM(tile_values.shape, BF)
    pair = pltpu.SemaphoreType.DMA((2,))
    (own_sums,) = call(
        functools.partial(spread_own, tile),
        tile_flops,
        [blocks, tile_counts, features, tile_values],
        [SMEM, SMEM, ANY, ANY],
        [sd((feats, masters + slots), BF)],
        [sums, pltpu.VMEM((feats, masters), BF), all_values, *lists, pair],
    )
    own_part, push, *part_sends = call(
        functools.partial(spread_mirrors, nf, nc, tile),
        tile_flops // 4,
        [blocks, tile_counts, mirrors, tile_values, own_sums],
        [SMEM, SMEM, None, ANY, ANY],
        [vec, sd((nd, nf, per, feats), BF)] + [chunk] * ((nf - 1) * nc),
        [
            sums,
            pltpu.VMEM((feats, masters + slots), BF),
            pltpu.VMEM((feats, slots), BF),
            all_values,
            *lists,
            pair,
        ],
    )
    part_recv = [
        [to_peer(part_sends[(j - 1) * nc + c], j) for j in range(1, nf)]
        for c in range(nc)
    ]
    incoming = exchange(push, ("dom", "feat"))

    flat_w = weights.reshape(2 * wide, wide)
    wt = flat_w.T
    rows, grads, grad_own, grad_recv = [], [], [], []
    step = 256 if part % 256 == 0 else 128
    for c in range(nc):
        last = c + 1 == nc
        args = [rep, incoming, wt, flat_w, cotangent, *x_parts, own_part, *part_recv[c]]
        specs = [None] * 2 + [ANY] * (len(args) - 2)
        alias = {}
        if c:
            alias = {len(args) + 1: 1}
            alias |= {len(args) + 2 + j: 4 + nf + j for j in range(nf)}
            args += [pay, output, *selfs]
            specs += [None] + [ANY] * (1 + nf)
        outs = [
            sd((wide, part), BF),
            sd((wide, width), BF),
            sd((wide, part), BF),
            sd((nd, nf, per, feats) if last else (wide, slots), BF),
        ] + [chunk] * nf + [vec] * nf
        rows_c, output, g_c, pay, *res = call(
            functools.partial(dense_kernel, nf, nc, c),
            8 * wide * wide * part,
            args,
            specs,
            outs,
            [
                pltpu.VMEM((wide, 2 * wide), BF),
                pltpu.VMEM((2 * wide, wide), BF),
                pltpu.VMEM((wide, part), BF),
                pltpu.VMEM((2 * wide, part), BF),
                pltpu.VMEM((nf, feats, part), BF),
                pltpu.VMEM((wide, part), BF),
                pltpu.VMEM((wide, part), BF),
                pltpu.VMEM((2 * wide, part), BF),
                pltpu.VMEM((nf, feats, slots), BF),
                pltpu.VMEM((wide, slots), F32),
                pltpu.SemaphoreType.DMA((2 * nf + 3,)),
                pltpu.SemaphoreType.DMA((2 * nf + 3, part // step)),
            ],
            (),
            [ANY] * 3 + [full(outs[3])] + [ANY] * (2 * nf),
            alias,
        )
        rows.append(rows_c)
        grads.append(g_c)
        grad_own.append(res[0])
        selfs = res[nf:]
        grad_recv.append([to_peer(res[j], j) for j in range(1, nf)])
    selfs = [selfs[0]] + [to_peer(selfs[j], j) for j in range(1, nf)]
    grad_mirrors = exchange(pay, ("dom", "feat"))

    keep, send = call(
        functools.partial(weight_kernel, nf, nc),
        4 * wide * wide * width,
        x_parts + rows + grads,
        [ANY] * (nf + 2 * nc),
        [sd((nf, feats, wide), F32), sd((nf, feats, wide), BF)],
        [pltpu.VMEM((2 * wide, wide), F32)]
        + [pltpu.VMEM((feats, width), BF)] * nf
        + [pltpu.VMEM((wide, part), BF)] * (2 * nc)
        + [pltpu.SemaphoreType.DMA((nf + 2 * nc,))],
    )

    flat_grads = grad_own + [grad_recv[c][j] for j in range(nf - 1) for c in range(nc)]
    back, push = call(
        functools.partial(back_kernel, nf, nc, tile),
        tile_flops,
        [blocks, tile_counts, grad_mirrors, tile_values, *flat_grads],
        [SMEM, SMEM, None, ANY] + [ANY] * (nf * nc),
        [sd((feats, masters), BF), sd((nd, per, feats), BF)],
        tile_scratch(nf * nc + 1),
    )
    back_in = exchange(push, "dom")

    radices = radices_of(nd)

    def swap(x, b):
        return lax.ppermute(x, "dom", [(i, i ^ b) for i in range(nd)])

    sends = [send]
    for k, r in enumerate(radices):
        unit = unit_of(radices, k)
        recvs = [swap(sends[m - 1], m * unit) for m in range(1, r)]
        if k + 1 < len(radices) and keep.shape[1] // radices[k + 1] % 16 == 0:
            size = keep.shape[1] // radices[k + 1]
            digit = unit_of(radices, k + 1), radices[k + 1]
            keep, *sends = call(
                functools.partial(combine_kernel, nf, radices[k + 1], digit),
                0,
                [keep, *recvs],
                [None] * r,
                [sd((nf, size, wide), F32)] + [sd((nf, size, wide), BF)] * (radices[k + 1] - 1),
            )
            continue
        cur = keep
        for recv in recvs:
            cur = cur + recv.astype(F32)
        if k + 1 == len(radices):
            break
        size = cur.shape[1] // radices[k + 1]
        digit = lax.rem(d // unit_of(radices, k + 1), radices[k + 1])
        pieces = [
            lax.dynamic_slice_in_dim(cur, (digit ^ m) * size, size, 1)
            for m in range(radices[k + 1])
        ]
        keep, sends = pieces[0], [piece.astype(BF) for piece in pieces[1:]]
    total = cur[0]
    for j in range(1, nf):
        total = total + to_peer(cur[j], j)
    total = total.astype(BF)
    for k in reversed(range(1, len(radices))):
        unit = unit_of(radices, k)
        others = [swap(total, m * unit) for m in range(1, radices[k])]
        total = jnp.concatenate([total, *others], 0)
    other = swap(total, 1)
    if total.shape[0] * 2 // nd % 8 == 0:
        (weight_grad,) = call(
            functools.partial(assemble_kernel, radices),
            0,
            [total, other],
            [None] * 2,
            [sd((2 * feats, wide), F32)],
            limit=SMALL,
        )
    else:
        total = jnp.concatenate([total, other], 0).reshape(nd, -1, wide)
        owners = jnp.arange(nd)
        place, rest = jnp.zeros_like(owners), owners
        for r in radices:
            place, rest = place * r + rest % r, rest // r
        held = jnp.zeros_like(owners).at[place].set(owners) ^ d
        numbers = jnp.array([relative(radices, m) for m in range(nd)])
        index = jnp.zeros_like(owners).at[numbers].set(jnp.arange(nd))[held]
        weight_grad = total[index].reshape(2 * feats, wide).astype(F32)
    weight_grad = weight_grad.reshape(2, feats, wide)

    (feature_grad,) = call(
        functools.partial(final_kernel, nf),
        2 * slots * feats * masters,
        [rep, back_in, back, *selfs],
        [None] * (3 + nf),
        [sd((feats, masters), BF)],
        limit=SMALL,
    )
    return output, feature_grad, weight_grad


def solution(mesh):
    return jax.shard_map(
        functools.partial(local, mesh.shape["dom"], mesh.shape["feat"]),
        mesh=mesh,
        in_specs=(
            P("feat", "dom"),
            P(),
            P("dom", None, None),
            P("dom", None),
            P("dom"),
            P("dom", None, None),
            P(None, ("dom", "feat")),
        ),
        out_specs=(P(None, ("dom", "feat")), P("feat", "dom"), P(None, "feat", None)),
        check_vma=False,
    )
```

```python
import functools

import jax
import jax.numpy as jnp
from jax import lax
from jax.experimental import pallas as pl
from jax.experimental.pallas import tpu as pltpu
from jax.sharding import PartitionSpec as P

BF = jnp.bfloat16
F32 = jnp.float32
GROUP = 16
SMALL = 24 * 1024 * 1024


def dot(a, b, ca=1, cb=0):
    return lax.dot_general(a, b, (((ca,), (cb,)), ((), ())), preferred_element_type=F32)


def eye(n):
    rows = lax.broadcasted_iota(jnp.int32, (n, n), 0)
    cols = lax.broadcasted_iota(jnp.int32, (n, n), 1)
    return jnp.where(rows == cols, 1.0, 0.0).astype(BF)


def picks(slots, start, height):
    rows = lax.broadcasted_iota(jnp.int32, (height, slots.shape[1]), 0) + start
    return jnp.where(rows == slots, 1.0, 0.0).astype(BF)


def flip(x):
    return dot(eye(x.shape[1]), x, 1, 1).astype(BF)


SMEM = pl.BlockSpec(memory_space=pltpu.SMEM)
ANY = pl.BlockSpec(memory_space=pl.ANY)


def full(x):
    zeros = (0,) * len(x.shape)
    return pl.BlockSpec(x.shape, lambda *_: zeros)


def cost(flops, nbytes):
    return pl.CostEstimate(flops=int(flops), bytes_accessed=int(nbytes), transcendentals=0)


def block_of(n):
    return next(b for b in (512, 256, 128) if n % b == 0)


def list_tiles(blocks, count, lists, source_col, trash, low, high):
    tiles, sources, targets = lists

    def step(t, n):
        source = blocks[source_col, t]
        tiles[n] = t
        sources[n] = source - low
        targets[n] = blocks[1 - source_col, t]
        return n + jnp.logical_and(source >= low, source < high).astype(jnp.int32)

    n = lax.fori_loop(0, count, step, jnp.int32(0))
    for u in range(GROUP):
        tiles[n + u] = 0
        sources[n + u] = 0
        targets[n + u] = trash
    return n


def run_tiles(n, lists, values, tile_dim, x_all, acc, tile):
    tiles, sources, targets = lists

    def step(g, _):
        for u in range(GROUP):
            at = g * GROUP + u
            picked = column(x_all, sources[at], tile)
            part = dot(picked, values[tiles[at]], 1, tile_dim)
            col = pl.ds(pl.multiple_of(targets[at] * tile, tile), tile)
            acc[:, col] += part
        return 0

    lax.fori_loop(0, (n + GROUP - 1) // GROUP, step, 0)


def column(ref, block, tile):
    at = pl.multiple_of(block * tile, tile)
    return ref[:, pl.ds(at, tile)]


def prep_kernel(nf, x_ref, replica, pull_ref, rep_ref, *halves):
    rep_ref[...] = jnp.concatenate(
        [replica[0, p : p + 1, :] for p in range(replica.shape[1])], axis=1
    )
    h = lax.axis_index("feat")
    _, masters = x_ref.shape
    width = halves[0].shape[1]
    step = block_of(masters)
    total = None
    for at in range(0, masters, step):
        part = dot(x_ref[:, at : at + step], picks(rep_ref[...], at, step))
        total = part if total is None else total + part
    pull_ref[...] = flip(total.astype(BF)).reshape(pull_ref.shape)
    for j in range(nf):
        at = pl.multiple_of(lax.rem(h + j, nf) * width, 128)
        halves[j][...] = x_ref[:, pl.ds(at, width)]


def spread_own(tile, blocks, count, x_ref, values_ref, out_ref, acc, x, values, *rest):
    lists, sems = rest[:3], rest[3]
    masters = x.shape[1]
    copies = [
        pltpu.make_async_copy(x_ref, x, sems.at[0]),
        pltpu.make_async_copy(values_ref, values, sems.at[1]),
    ]
    for copy in copies:
        copy.start()
    acc[...] = jnp.zeros_like(acc)
    n = list_tiles(blocks, count[0], lists, 0, acc.shape[1] // tile - 1, 0, masters // tile)
    for copy in copies:
        copy.wait()
    run_tiles(n, lists, values, 0, x, acc, tile)
    out_ref[...] = acc[:, : out_ref.shape[1]].astype(BF)


def spread_mirrors(nf, nc, tile, blocks, count, mirrors, values_ref, own_ref, *rest):
    part_ref, push_ref = rest[:2]
    sends = rest[2 : 2 + (nf - 1) * nc]
    acc, own, x, values, *lists, sems, held_part, held_push = rest[2 + (nf - 1) * nc :][:10]
    held_sends = rest[2 + (nf - 1) * nc :][10:]
    h = lax.axis_index("feat")
    feats, width = part_ref.shape
    outs = []

    def put(src, dst):
        outs.append(pltpu.make_async_copy(src, dst, sems.at[2 + len(outs)]))
        outs[-1].start()

    slots = x.shape[1]
    masters = own.shape[1] - slots
    copies = [
        pltpu.make_async_copy(values_ref, values, sems.at[0]),
        pltpu.make_async_copy(own_ref, own, sems.at[1]),
    ]
    for copy in copies:
        copy.start()
    acc[...] = jnp.zeros_like(acc)
    x[...] = flip(mirrors[...].reshape(slots, feats))
    low = masters // tile
    n = list_tiles(
        blocks, count[0], lists, 0, acc.shape[1] // tile - 1, low, own.shape[1] // tile
    )
    for copy in copies:
        copy.wait()
    run_tiles(n, lists, values, 0, x, acc, tile)

    def total(at, size):
        return (own[:, pl.ds(at, size)].astype(F32) + acc[:, pl.ds(at, size)]).astype(BF)

    part = width // nc
    for j in range(1, nf):
        for c in range(nc):
            at = pl.multiple_of(lax.rem(h + j, nf) * width + c * part, 128)
            held_sends[(j - 1) * nc + c][...] = total(at, part)
            put(held_sends[(j - 1) * nc + c], sends[(j - 1) * nc + c])
    push = flip(total(masters, slots))
    push = push.reshape(push_ref.shape[0], push_ref.shape[2], feats)
    for f in range(nf):
        held_push[:, f] = push
    put(held_push, push_ref)
    held_part[...] = total(pl.multiple_of(h * width, 128), width)
    put(held_part, part_ref)
    for copy in outs:
        copy.wait()


def own_term_kernel(nf, wt_ref, *refs):
    xs, out_ref, rows = refs[:nf], refs[nf], refs[nf + 1]
    h = lax.axis_index("feat")
    feats, width = xs[0].shape
    for j in range(nf):
        f = lax.rem(h - j + nf, nf)
        rows[pl.ds(pl.multiple_of(f * feats, feats), feats), :] = xs[j][...]
    step = 512 if width % 512 == 0 else 128
    for b in range(0, width, step):
        out_ref[:, b : b + step] = dot(wt_ref[...], rows[:, b : b + step])


def dense_kernel(nf, nc, c, *refs):
    rep_ref, inc_ref, wt_hbm, w_hbm, cot_hbm, z_hbm = refs[:6]
    parts = refs[6 : 6 + nf]
    refs = refs[6 + nf :]
    if c:
        pay_in = refs[0]
        refs = refs[2 + nf :]
    agg_hbm, out_hbm, g_hbm, pay_ref = refs[:4]
    grads, selfs = refs[4 : 4 + nf], refs[4 + nf : 4 + 2 * nf]
    wt, w, cot, z_own, rows, terms, out, g_all, both, held_pay, in_sems, out_sems = refs[4 + 2 * nf :]
    h = lax.axis_index("feat")
    feats, part = grads[0].shape
    wide = w.shape[1]
    slots = rep_ref.shape[1]
    chunk = pl.ds(c * part, part)

    def place(f):
        return pl.ds(pl.multiple_of(f * feats, feats), feats)

    early, late = [], []
    for j in range(nf):
        term = parts[j].at[:, chunk] if j == 0 else parts[j]
        early.append(pltpu.make_async_copy(term, terms.at[j], in_sems.at[j]))
    late.append(pltpu.make_async_copy(wt_hbm, wt, in_sems.at[nf]))
    late.append(pltpu.make_async_copy(z_hbm.at[:, chunk], z_own, in_sems.at[nf + 1]))
    late.append(pltpu.make_async_copy(cot_hbm.at[:, chunk], cot, in_sems.at[nf + 2]))
    late.append(pltpu.make_async_copy(w_hbm, w, in_sems.at[nf + 3]))
    for copy in early + late:
        copy.start()
    pick = picks(rep_ref[...], (h * nc + c) * part, part)
    incs = [flip(inc_ref[:, lax.rem(h - j + nf, nf)].reshape(slots, feats)) for j in range(nf)]
    adds = [dot(inc, pick, 1, 1) for inc in incs]
    for copy in early:
        copy.wait()
    for j in range(nf):
        f = lax.rem(h - j + nf, nf)
        total = terms[j].astype(F32) + adds[j]
        rows[place(f), :] = total.astype(BF)
    out_copies = []

    def put(src, dst):
        copy = pltpu.make_async_copy(src, dst, out_sems.at[len(out_copies)])
        copy.start()
        out_copies.append(copy)

    put(rows, agg_hbm)
    for copy in late:
        copy.wait()
    step = 256 if part % 256 == 0 else 128
    for b in range(0, part, step):
        cols = slice(b, b + step)
        z = z_own[:, cols] + dot(wt[...], rows[:, cols])
        s = 0.5 + 0.5 * jnp.tanh(0.5 * z)
        out[:, cols] = (z * s).astype(BF)
        g = (cot[:, cols].astype(F32) * (s * (1.0 + z * (1.0 - s)))).astype(BF)
        g_all[:, cols] = g
        both[:, cols] = dot(w[...], g).astype(BF)
        for j in range(nf):
            at = lax.rem(h + j, nf)
            peer = pl.ds(pl.multiple_of(wide + at * feats, feats), feats)
            put(both.at[peer, cols], grads[j].at[:, cols])
            put(both.at[place(at), cols], selfs[j].at[:, pl.ds(c * part + b, step)])
        put(g_all.at[:, cols], g_hbm.at[:, cols])
        put(out.at[:, cols], out_hbm.at[:, pl.ds(c * part + b, step)])
    pay = dot(both[wide:, :], pick)
    if c:
        pay = pay + pay_in[...].astype(F32)
    pay = pay.astype(BF)
    if c + 1 < nc:
        held_pay[...] = pay
    else:
        for f in range(nf):
            mine = flip(pay[f * feats : (f + 1) * feats])
            held_pay[:, f] = mine.reshape(pay_ref.shape[0], pay_ref.shape[2], feats)
    put(held_pay, pay_ref)
    for copy in out_copies:
        copy.wait()


def weight_kernel(nf, nc, *refs):
    ins = refs[: nf + 2 * nc]
    keep_ref, send_ref, acc = refs[nf + 2 * nc : nf + 2 * nc + 3]
    held, sems = refs[nf + 2 * nc + 3 : -1], refs[-1]
    h = lax.axis_index("feat")
    bit = lax.rem(lax.axis_index("dom"), 2)
    wide = acc.shape[1]
    feats = wide // nf
    copies = [pltpu.make_async_copy(a, b, sems.at[k]) for k, (a, b) in enumerate(zip(ins, held))]
    order = [[nf + nc + c, nf + c] for c in range(nc)]
    order[0] += list(range(nf))
    for group in order:
        for k in group:
            copies[k].start()
    xs, aggs, grads = held[:nf], held[nf : nf + nc], held[nf + nc :]
    part = grads[0].shape[1]
    for c in range(nc):
        for k in order[c]:
            copies[k].wait()
        terms = [(pl.ds(wide, wide), aggs[c][...])]
        for j in range(nf):
            at = pl.multiple_of(lax.rem(h - j + nf, nf) * feats, feats)
            terms.append((pl.ds(at, feats), xs[j][:, c * part : (c + 1) * part]))
        for at, left in terms:
            term = dot(left, grads[c][...], 1, 1)
            acc[at, :] = term if c == 0 else acc[at, :] + term
    for j in range(nf):
        at = lax.rem(h + j, nf) * feats
        keep_ref[j] = acc[pl.ds(pl.multiple_of(bit * wide + at, feats), feats), :]
        send_ref[j] = acc[pl.ds(pl.multiple_of((1 - bit) * wide + at, feats), feats), :].astype(BF)


def radices_of(n):
    radices = [2] * min(2, n.bit_length() - 1)
    n //= 1 << len(radices)
    while n > 1:
        radices.append(4 if n % 4 == 0 else 2)
        n //= radices[-1]
    return tuple(radices)


def unit_of(radices, k):
    unit = 1
    for r in radices[:k]:
        unit *= r
    return unit


def relative(radices, m):
    number = 0
    size = unit_of(radices, len(radices))
    for k, r in enumerate(radices):
        size //= r
        number += (m // size) % r * unit_of(radices, k)
    return number


def assemble_kernel(radices, own_ref, other_ref, out_ref):
    d = lax.axis_index("dom")
    nd = 1
    for r in radices:
        nd *= r
    rows = out_ref.shape[0] // nd
    half = nd // 2
    for m in range(nd):
        at, owner, height = 0, d ^ relative(radices, m), out_ref.shape[0]
        for r in radices:
            height //= r
            at = at + lax.rem(owner, r) * height
            owner = owner // r
        ref, k = (own_ref, m) if m < half else (other_ref, m - half)
        piece = ref[k * rows : (k + 1) * rows, :]
        out_ref[pl.ds(pl.multiple_of(at, rows), rows), :] = piece.astype(F32)


def back_kernel(nf, nc, tile, blocks, count, mirrors, values_ref, *rest):
    grads = rest[: nf * nc]
    back_ref, push_ref, acc, x_all, values, tiles, sources, targets, sems = rest[nf * nc : -2]
    held_back, held_push = rest[-2:]
    lists = (tiles, sources, targets)
    h = lax.axis_index("feat")
    feats, masters = back_ref.shape
    slots = x_all.shape[1] - masters
    part = masters // nf // nc
    copies = [pltpu.make_async_copy(values_ref, values, sems.at[nf * nc])]
    for j in range(nf):
        for c in range(nc):
            k = j * nc + c
            at = pl.multiple_of((lax.rem(h - j + nf, nf) * nc + c) * part, 128)
            copies.append(
                pltpu.make_async_copy(grads[k], x_all.at[:, pl.ds(at, part)], sems.at[k])
            )
    for copy in copies:
        copy.start()
    acc[...] = jnp.zeros_like(acc)
    total = mirrors[:, 0].astype(F32)
    for f in range(1, nf):
        total = total + mirrors[:, f].astype(F32)
    x_all[:, masters:] = flip(total.astype(BF).reshape(slots, feats))
    list_tiles(blocks, count[0], lists, 1, acc.shape[1] // tile - 1, 0, x_all.shape[1] // tile)
    for copy in copies:
        copy.wait()
    run_tiles(count[0], lists, values, 1, x_all, acc, tile)
    partial = acc[:, masters : masters + slots].astype(BF)
    held_push[...] = flip(partial).reshape(push_ref.shape)
    outs = [pltpu.make_async_copy(held_push, push_ref, sems.at[nf * nc + 1])]
    outs[0].start()
    held_back[...] = acc[:, :masters].astype(BF)
    outs.append(pltpu.make_async_copy(held_back, back_ref, sems.at[nf * nc + 2]))
    outs[1].start()
    for copy in outs:
        copy.wait()


def final_kernel(nf, nc, rep_ref, inc_ref, back_ref, *rest):
    selfs, out_ref = rest[:nf], rest[nf]
    h = lax.axis_index("feat")
    feats, width = selfs[0].shape
    part = width // nc
    slots = rep_ref.shape[1]
    inc = flip(inc_ref[...].reshape(slots, feats))
    for j in range(nf):
        for c in range(nc):
            at = pl.multiple_of((lax.rem(h - j + nf, nf) * nc + c) * part, 128)
            back = back_ref[:, pl.ds(at, part)].astype(F32)
            back = back + dot(inc, picks(rep_ref[...], at, part), 1, 1)
            own = selfs[j][:, c * part : (c + 1) * part].astype(F32)
            out_ref[:, pl.ds(at, part)] = (own + back).astype(BF)


def local(nd, nf, features, weights, tile_values, tile_blocks, tile_counts, replica, cotangent):
    feats, masters = features.shape
    wide = weights.shape[1]
    ntiles, tile, _ = tile_values.shape
    per = replica.shape[2]
    slots = nd * per
    width = masters // nf
    cols = masters + slots + tile
    nc = 2 if width % (2 * tile) == 0 else 1
    part = width // nc
    d = lax.axis_index("dom")
    sd = jax.ShapeDtypeStruct
    lists = [pltpu.SMEM((ntiles + GROUP,), jnp.int32)] * 3
    tile_flops = 2 * ntiles * feats * tile * tile

    def call(body, flops, args, specs, outs, scratch=(), grid=(), out_specs=None, alias={}, limit=None):
        return pl.pallas_call(
            body,
            grid=grid,
            in_specs=[full(a) if p is None else p for a, p in zip(args, specs, strict=True)],
            out_specs=out_specs or [full(o) for o in outs],
            out_shape=outs,
            scratch_shapes=list(scratch),
            input_output_aliases=alias,
            compiler_params=pltpu.CompilerParams(vmem_limit_bytes=limit),
            cost_estimate=cost(flops, 2 * sum(a.size for a in args)),
        )(*args)

    def to_peer(x, j):
        return lax.ppermute(x, "feat", [(i, (i + j) % nf) for i in range(nf)])

    def exchange(x, axes):
        flat = x.reshape(-1, per, feats)
        return lax.all_to_all(flat, axes, 0, 0, tiled=True).reshape(x.shape)

    def tile_scratch(nsems):
        return [
            pltpu.VMEM((feats, cols), F32),
            pltpu.VMEM((feats, masters + slots), BF),
            pltpu.VMEM(tile_values.shape, BF),
            *lists,
            pltpu.SemaphoreType.DMA((nsems,)),
        ]

    vec = sd((feats, width), BF)
    pull, rep, *x_halves = call(
        functools.partial(prep_kernel, nf),
        2 * slots * feats * masters,
        [features, replica],
        [None] * 2,
        [sd((nd, per, feats), BF), sd((1, slots), jnp.int32)] + [vec] * nf,
    )
    mirrors = exchange(pull, "dom")
    x_parts = [x_halves[0]] + [to_peer(x_halves[j], j) for j in range(1, nf)]

    blocks = tile_blocks.T
    chunk = sd((feats, part), BF)
    sums = pltpu.VMEM((feats, cols), F32)
    all_values = pltpu.VMEM(tile_values.shape, BF)
    pair = pltpu.SemaphoreType.DMA((2,))
    (own_sums,) = call(
        functools.partial(spread_own, tile),
        tile_flops,
        [blocks, tile_counts, features, tile_values],
        [SMEM, SMEM, ANY, ANY],
        [sd((feats, masters + slots), BF)],
        [sums, pltpu.VMEM((feats, masters), BF), all_values, *lists, pair],
    )
    own_part, push, *part_sends = call(
        functools.partial(spread_mirrors, nf, nc, tile),
        tile_flops // 4,
        [blocks, tile_counts, mirrors, tile_values, own_sums],
        [SMEM, SMEM, None, ANY, ANY],
        [vec, sd((nd, nf, per, feats), BF)] + [chunk] * ((nf - 1) * nc),
        [
            sums,
            pltpu.VMEM((feats, masters + slots), BF),
            pltpu.VMEM((feats, slots), BF),
            all_values,
            *lists,
            pltpu.SemaphoreType.DMA((4 + (nf - 1) * nc,)),
            pltpu.VMEM((feats, width), BF),
            pltpu.VMEM((nd, nf, per, feats), BF),
        ]
        + [pltpu.VMEM((feats, part), BF)] * ((nf - 1) * nc),
        out_specs=[ANY] * (2 + (nf - 1) * nc),
    )
    part_recv = [
        [to_peer(part_sends[(j - 1) * nc + c], j) for j in range(1, nf)]
        for c in range(nc)
    ]
    incoming = exchange(push, ("dom", "feat"))

    flat_w = weights.reshape(2 * wide, wide)
    wt = [weights[0].T, weights[1].T]
    (z_own,) = call(
        functools.partial(own_term_kernel, nf),
        2 * wide * wide * width,
        [wt[0], *x_parts],
        [None] * (nf + 1),
        [sd((wide, width), F32)],
        [pltpu.VMEM((wide, width), BF)],
    )
    rows, grads, grad_own, grad_recv = [], [], [], []
    step = 256 if part % 256 == 0 else 128
    for c in range(nc):
        last = c + 1 == nc
        args = [rep, incoming, wt[1], flat_w, cotangent, z_own, own_part, *part_recv[c]]
        specs = [None] * 2 + [ANY] * (len(args) - 2)
        alias = {}
        if c:
            alias = {len(args) + 1: 1}
            alias |= {len(args) + 2 + j: 4 + nf + j for j in range(nf)}
            args += [pay, output, *selfs]
            specs += [None] + [ANY] * (1 + nf)
        outs = [
            sd((wide, part), BF),
            sd((wide, width), BF),
            sd((wide, part), BF),
            sd((nd, nf, per, feats) if last else (wide, slots), BF),
        ] + [chunk] * nf + [vec] * nf
        rows_c, output, g_c, pay, *res = call(
            functools.partial(dense_kernel, nf, nc, c),
            8 * wide * wide * part,
            args,
            specs,
            outs,
            [
                pltpu.VMEM((wide, wide), BF),
                pltpu.VMEM((2 * wide, wide), BF),
                pltpu.VMEM((wide, part), BF),
                pltpu.VMEM((wide, part), F32),
                pltpu.VMEM((wide, part), BF),
                pltpu.VMEM((nf, feats, part), BF),
                pltpu.VMEM((wide, part), BF),
                pltpu.VMEM((wide, part), BF),
                pltpu.VMEM((2 * wide, part), BF),
                pltpu.VMEM(outs[3].shape, BF),
                pltpu.SemaphoreType.DMA((nf + 4,)),
                pltpu.SemaphoreType.DMA((2 + (part // step) * (2 * nf + 2),)),
            ],
            (),
            [ANY] * len(outs),
            alias,
        )
        rows.append(rows_c)
        grads.append(g_c)
        grad_own.append(res[0])
        selfs = res[nf:]
        grad_recv.append([to_peer(res[j], j) for j in range(1, nf)])
    selfs = [selfs[0]] + [to_peer(selfs[j], j) for j in range(1, nf)]
    grad_mirrors = exchange(pay, ("dom", "feat"))

    keep, send = call(
        functools.partial(weight_kernel, nf, nc),
        4 * wide * wide * width,
        x_parts + rows + grads,
        [ANY] * (nf + 2 * nc),
        [sd((nf, feats, wide), F32), sd((nf, feats, wide), BF)],
        [pltpu.VMEM((2 * wide, wide), F32)]
        + [pltpu.VMEM((feats, width), BF)] * nf
        + [pltpu.VMEM((wide, part), BF)] * (2 * nc)
        + [pltpu.SemaphoreType.DMA((nf + 2 * nc,))],
    )

    flat_grads = grad_own + [grad_recv[c][j] for j in range(nf - 1) for c in range(nc)]
    back, push = call(
        functools.partial(back_kernel, nf, nc, tile),
        tile_flops,
        [blocks, tile_counts, grad_mirrors, tile_values, *flat_grads],
        [SMEM, SMEM, None, ANY] + [ANY] * (nf * nc),
        [sd((feats, masters), BF), sd((nd, per, feats), BF)],
        tile_scratch(nf * nc + 3)
        + [pltpu.VMEM((feats, masters), BF), pltpu.VMEM((nd, per, feats), BF)],
        out_specs=[ANY] * 2,
    )
    back_in = exchange(push, "dom")

    radices = radices_of(nd)

    def swap(x, b):
        return lax.ppermute(x, "dom", [(i, i ^ b) for i in range(nd)])

    sends = [send]
    for k, r in enumerate(radices):
        unit = unit_of(radices, k)
        cur = keep
        for m in range(1, r):
            cur = cur + swap(sends[m - 1], m * unit).astype(F32)
        if k + 1 == len(radices):
            break
        size = cur.shape[1] // radices[k + 1]
        digit = lax.rem(d // unit_of(radices, k + 1), radices[k + 1])
        pieces = [
            lax.dynamic_slice_in_dim(cur, (digit ^ m) * size, size, 1)
            for m in range(radices[k + 1])
        ]
        keep, sends = pieces[0], [piece.astype(BF) for piece in pieces[1:]]
    total = cur[0]
    for j in range(1, nf):
        total = total + to_peer(cur[j], j)
    total = total.astype(BF)
    for k in reversed(range(1, len(radices))):
        unit = unit_of(radices, k)
        others = [swap(total, m * unit) for m in range(1, radices[k])]
        total = jnp.concatenate([total, *others], 0)
    other = swap(total, 1)
    if total.shape[0] * 2 // nd % 8 == 0:
        (weight_grad,) = call(
            functools.partial(assemble_kernel, radices),
            0,
            [total, other],
            [None] * 2,
            [sd((2 * feats, wide), F32)],
            limit=SMALL,
        )
    else:
        total = jnp.concatenate([total, other], 0).reshape(nd, -1, wide)
        owners = jnp.arange(nd)
        place, rest = jnp.zeros_like(owners), owners
        for r in radices:
            place, rest = place * r + rest % r, rest // r
        held = jnp.zeros_like(owners).at[place].set(owners) ^ d
        numbers = jnp.array([relative(radices, m) for m in range(nd)])
        index = jnp.zeros_like(owners).at[numbers].set(jnp.arange(nd))[held]
        weight_grad = total[index].reshape(2 * feats, wide).astype(F32)
    weight_grad = weight_grad.reshape(2, feats, wide)

    (feature_grad,) = call(
        functools.partial(final_kernel, nf, nc),
        2 * slots * feats * masters,
        [rep, back_in, back, *selfs],
        [None] * (3 + nf),
        [sd((feats, masters), BF)],
        limit=SMALL,
    )
    return output, feature_grad, weight_grad


def solution(mesh):
    return jax.shard_map(
        functools.partial(local, mesh.shape["dom"], mesh.shape["feat"]),
        mesh=mesh,
        in_specs=(
            P("feat", "dom"),
            P(),
            P("dom", None, None),
            P("dom", None),
            P("dom"),
            P("dom", None, None),
            P(None, ("dom", "feat")),
        ),
        out_specs=(P(None, ("dom", "feat")), P("feat", "dom"), P(None, "feat", None)),
        check_vma=False,
    )
```

```python
import functools

import jax
import jax.numpy as jnp
from jax import lax
from jax.experimental import pallas as pl
from jax.experimental.pallas import tpu as pltpu
from jax.sharding import PartitionSpec as P

BF = jnp.bfloat16
F32 = jnp.float32
GROUP = 16
SMALL = 24 * 1024 * 1024


def dot(a, b, ca=1, cb=0):
    return lax.dot_general(a, b, (((ca,), (cb,)), ((), ())), preferred_element_type=F32)


def eye(n):
    rows = lax.broadcasted_iota(jnp.int32, (n, n), 0)
    cols = lax.broadcasted_iota(jnp.int32, (n, n), 1)
    return jnp.where(rows == cols, 1.0, 0.0).astype(BF)


def picks(slots, start, height):
    rows = lax.broadcasted_iota(jnp.int32, (height, slots.shape[1]), 0) + start
    return jnp.where(rows == slots, 1.0, 0.0).astype(BF)


def flip(x):
    return dot(eye(x.shape[1]), x, 1, 1).astype(BF)


SMEM = pl.BlockSpec(memory_space=pltpu.SMEM)
ANY = pl.BlockSpec(memory_space=pl.ANY)


def full(x):
    zeros = (0,) * len(x.shape)
    return pl.BlockSpec(x.shape, lambda *_: zeros)


def cost(flops, nbytes):
    return pl.CostEstimate(flops=int(flops), bytes_accessed=int(nbytes), transcendentals=0)


def block_of(n):
    return next(b for b in (512, 256, 128) if n % b == 0)


def list_tiles(blocks, count, lists, source_col, trash, low, high):
    tiles, sources, targets = lists

    def step(t, n):
        source = blocks[source_col, t]
        tiles[n] = t
        sources[n] = source - low
        targets[n] = blocks[1 - source_col, t]
        return n + jnp.logical_and(source >= low, source < high).astype(jnp.int32)

    n = lax.fori_loop(0, count, step, jnp.int32(0))
    for u in range(GROUP):
        tiles[n + u] = 0
        sources[n + u] = 0
        targets[n + u] = trash
    return n


def run_tiles(n, lists, values, tile_dim, x_all, acc, tile):
    tiles, sources, targets = lists

    def step(g, _):
        for u in range(GROUP):
            at = g * GROUP + u
            picked = column(x_all, sources[at], tile)
            part = dot(picked, values[tiles[at]], 1, tile_dim)
            col = pl.ds(pl.multiple_of(targets[at] * tile, tile), tile)
            acc[:, col] += part
        return 0

    lax.fori_loop(0, (n + GROUP - 1) // GROUP, step, 0)


def column(ref, block, tile):
    at = pl.multiple_of(block * tile, tile)
    return ref[:, pl.ds(at, tile)]


def prep_kernel(nf, x_ref, replica, pull_ref, rep_ref, *halves):
    rep_ref[...] = jnp.concatenate(
        [replica[0, p : p + 1, :] for p in range(replica.shape[1])], axis=1
    )
    h = lax.axis_index("feat")
    _, masters = x_ref.shape
    width = halves[0].shape[1]
    step = block_of(masters)
    total = None
    for at in range(0, masters, step):
        part = dot(x_ref[:, at : at + step], picks(rep_ref[...], at, step))
        total = part if total is None else total + part
    pull_ref[...] = flip(total.astype(BF)).reshape(pull_ref.shape)
    for j in range(nf):
        at = pl.multiple_of(lax.rem(h + j, nf) * width, 128)
        halves[j][...] = x_ref[:, pl.ds(at, width)]


def spread_own(tile, blocks, count, x_ref, values_ref, out_ref, acc, x, values, *rest):
    lists, sems = rest[:3], rest[3]
    masters = x.shape[1]
    copies = [
        pltpu.make_async_copy(x_ref, x, sems.at[0]),
        pltpu.make_async_copy(values_ref, values, sems.at[1]),
    ]
    for copy in copies:
        copy.start()
    acc[...] = jnp.zeros_like(acc)
    n = list_tiles(blocks, count[0], lists, 0, acc.shape[1] // tile - 1, 0, masters // tile)
    for copy in copies:
        copy.wait()
    run_tiles(n, lists, values, 0, x, acc, tile)
    out_ref[...] = acc[:, : out_ref.shape[1]].astype(BF)


def spread_mirrors(nf, nc, tile, blocks, count, mirrors, values_ref, own_ref, *rest):
    part_ref, push_ref = rest[:2]
    sends = rest[2 : 2 + (nf - 1) * nc]
    acc, own, x, values, *lists, sems, held_part, held_push = rest[2 + (nf - 1) * nc :][:10]
    held_sends = rest[2 + (nf - 1) * nc :][10:]
    h = lax.axis_index("feat")
    feats, width = part_ref.shape
    outs = []

    def put(src, dst):
        outs.append(pltpu.make_async_copy(src, dst, sems.at[2 + len(outs)]))
        outs[-1].start()

    slots = x.shape[1]
    masters = own.shape[1] - slots
    copies = [
        pltpu.make_async_copy(values_ref, values, sems.at[0]),
        pltpu.make_async_copy(own_ref, own, sems.at[1]),
    ]
    for copy in copies:
        copy.start()
    acc[...] = jnp.zeros_like(acc)
    x[...] = flip(mirrors[...].reshape(slots, feats))
    low = masters // tile
    n = list_tiles(
        blocks, count[0], lists, 0, acc.shape[1] // tile - 1, low, own.shape[1] // tile
    )
    for copy in copies:
        copy.wait()
    run_tiles(n, lists, values, 0, x, acc, tile)

    def total(at, size):
        return (own[:, pl.ds(at, size)].astype(F32) + acc[:, pl.ds(at, size)]).astype(BF)

    part = width // nc
    for j in range(1, nf):
        for c in range(nc):
            at = pl.multiple_of(lax.rem(h + j, nf) * width + c * part, 128)
            held_sends[(j - 1) * nc + c][...] = total(at, part)
            put(held_sends[(j - 1) * nc + c], sends[(j - 1) * nc + c])
    push = flip(total(masters, slots))
    push = push.reshape(push_ref.shape[0], push_ref.shape[2], feats)
    for f in range(nf):
        held_push[:, f] = push
    put(held_push, push_ref)
    held_part[...] = total(pl.multiple_of(h * width, 128), width)
    put(held_part, part_ref)
    for copy in outs:
        copy.wait()


def own_term_kernel(nf, wt_ref, *refs):
    xs, out_ref, rows = refs[:nf], refs[nf], refs[nf + 1]
    h = lax.axis_index("feat")
    feats, width = xs[0].shape
    for j in range(nf):
        f = lax.rem(h - j + nf, nf)
        rows[pl.ds(pl.multiple_of(f * feats, feats), feats), :] = xs[j][...]
    step = 512 if width % 512 == 0 else 128
    for b in range(0, width, step):
        out_ref[:, b : b + step] = dot(wt_ref[:, : rows.shape[0]], rows[:, b : b + step])


def dense_kernel(nf, nc, c, *refs):
    rep_ref, inc_ref, wt_hbm, w_hbm, cot_hbm, z_hbm = refs[:6]
    parts = refs[6 : 6 + nf]
    refs = refs[6 + nf :]
    if c:
        pay_in = refs[0]
        refs = refs[2 + nf :]
    agg_hbm, out_hbm, g_hbm, pay_ref = refs[:4]
    grads, selfs = refs[4 : 4 + nf], refs[4 + nf : 4 + 2 * nf]
    wt, w, cot, z_own, rows, terms, out, g_all, both, held_pay, in_sems, out_sems = refs[4 + 2 * nf :]
    h = lax.axis_index("feat")
    feats, part = grads[0].shape
    wide = w.shape[1]
    slots = rep_ref.shape[1]
    chunk = pl.ds(c * part, part)

    def place(f):
        return pl.ds(pl.multiple_of(f * feats, feats), feats)

    early, late = [], []
    for j in range(nf):
        term = parts[j].at[:, chunk] if j == 0 else parts[j]
        early.append(pltpu.make_async_copy(term, terms.at[j], in_sems.at[j]))
    late.append(pltpu.make_async_copy(wt_hbm.at[:, wide:], wt, in_sems.at[nf]))
    late.append(pltpu.make_async_copy(z_hbm.at[:, chunk], z_own, in_sems.at[nf + 1]))
    late.append(pltpu.make_async_copy(cot_hbm.at[:, chunk], cot, in_sems.at[nf + 2]))
    late.append(pltpu.make_async_copy(w_hbm, w, in_sems.at[nf + 3]))
    for copy in early + late:
        copy.start()
    pick = picks(rep_ref[...], (h * nc + c) * part, part)
    incs = [flip(inc_ref[:, lax.rem(h - j + nf, nf)].reshape(slots, feats)) for j in range(nf)]
    adds = [dot(inc, pick, 1, 1) for inc in incs]
    for copy in early:
        copy.wait()
    for j in range(nf):
        f = lax.rem(h - j + nf, nf)
        total = terms[j].astype(F32) + adds[j]
        rows[place(f), :] = total.astype(BF)
    out_copies = []

    def put(src, dst):
        copy = pltpu.make_async_copy(src, dst, out_sems.at[len(out_copies)])
        copy.start()
        out_copies.append(copy)

    put(rows, agg_hbm)
    for copy in late:
        copy.wait()
    step = 256 if part % 256 == 0 else 128
    for b in range(0, part, step):
        cols = slice(b, b + step)
        z = z_own[:, cols] + dot(wt[...], rows[:, cols])
        s = 0.5 + 0.5 * jnp.tanh(0.5 * z)
        out[:, cols] = (z * s).astype(BF)
        g = (cot[:, cols].astype(F32) * (s * (1.0 + z * (1.0 - s)))).astype(BF)
        g_all[:, cols] = g
        both[:, cols] = dot(w[...], g).astype(BF)
        for j in range(nf):
            at = lax.rem(h + j, nf)
            peer = pl.ds(pl.multiple_of(wide + at * feats, feats), feats)
            put(both.at[peer, cols], grads[j].at[:, cols])
            put(both.at[place(at), cols], selfs[j].at[:, pl.ds(c * part + b, step)])
        put(g_all.at[:, cols], g_hbm.at[:, cols])
        put(out.at[:, cols], out_hbm.at[:, pl.ds(c * part + b, step)])
    pay = dot(both[wide:, :], pick)
    if c:
        pay = pay + pay_in[...].astype(F32)
    pay = pay.astype(BF)
    if c + 1 < nc:
        held_pay[...] = pay
    else:
        for f in range(nf):
            mine = flip(pay[f * feats : (f + 1) * feats])
            held_pay[:, f] = mine.reshape(pay_ref.shape[0], pay_ref.shape[2], feats)
    put(held_pay, pay_ref)
    for copy in out_copies:
        copy.wait()


def weight_kernel(nf, nc, *refs):
    ins = refs[: nf + 2 * nc]
    keep_ref, send_ref, acc = refs[nf + 2 * nc : nf + 2 * nc + 3]
    held, sems = refs[nf + 2 * nc + 3 : -1], refs[-1]
    h = lax.axis_index("feat")
    bit = lax.rem(lax.axis_index("dom"), 2)
    wide = acc.shape[1]
    feats = wide // nf
    copies = [pltpu.make_async_copy(a, b, sems.at[k]) for k, (a, b) in enumerate(zip(ins, held))]
    order = [[nf + nc + c, nf + c] for c in range(nc)]
    order[0] += list(range(nf))
    for group in order:
        for k in group:
            copies[k].start()
    xs, aggs, grads = held[:nf], held[nf : nf + nc], held[nf + nc :]
    part = grads[0].shape[1]
    for c in range(nc):
        for k in order[c]:
            copies[k].wait()
        terms = [(pl.ds(wide, wide), aggs[c][...])]
        for j in range(nf):
            at = pl.multiple_of(lax.rem(h - j + nf, nf) * feats, feats)
            terms.append((pl.ds(at, feats), xs[j][:, c * part : (c + 1) * part]))
        for at, left in terms:
            term = dot(left, grads[c][...], 1, 1)
            acc[at, :] = term if c == 0 else acc[at, :] + term
    for j in range(nf):
        at = lax.rem(h + j, nf) * feats
        keep_ref[j] = acc[pl.ds(pl.multiple_of(bit * wide + at, feats), feats), :]
        send_ref[j] = acc[pl.ds(pl.multiple_of((1 - bit) * wide + at, feats), feats), :].astype(BF)


def radices_of(n):
    radices = [2] * min(2, n.bit_length() - 1)
    n //= 1 << len(radices)
    while n > 1:
        radices.append(4 if n % 4 == 0 else 2)
        n //= radices[-1]
    return tuple(radices)


def unit_of(radices, k):
    unit = 1
    for r in radices[:k]:
        unit *= r
    return unit


def relative(radices, m):
    number = 0
    size = unit_of(radices, len(radices))
    for k, r in enumerate(radices):
        size //= r
        number += (m // size) % r * unit_of(radices, k)
    return number


def assemble_kernel(radices, own_ref, other_ref, out_ref):
    d = lax.axis_index("dom")
    nd = 1
    for r in radices:
        nd *= r
    rows = out_ref.shape[0] // nd
    half = nd // 2
    for m in range(nd):
        at, owner, height = 0, d ^ relative(radices, m), out_ref.shape[0]
        for r in radices:
            height //= r
            at = at + lax.rem(owner, r) * height
            owner = owner // r
        ref, k = (own_ref, m) if m < half else (other_ref, m - half)
        piece = ref[k * rows : (k + 1) * rows, :]
        out_ref[pl.ds(pl.multiple_of(at, rows), rows), :] = piece.astype(F32)


def back_kernel(nf, nc, tile, blocks, count, mirrors, values_ref, *rest):
    grads = rest[: nf * nc]
    back_ref, push_ref, acc, x_all, values, tiles, sources, targets, sems = rest[nf * nc : -2]
    held_back, held_push = rest[-2:]
    lists = (tiles, sources, targets)
    h = lax.axis_index("feat")
    feats, masters = back_ref.shape
    slots = x_all.shape[1] - masters
    part = masters // nf // nc
    copies = [pltpu.make_async_copy(values_ref, values, sems.at[nf * nc])]
    for j in range(nf):
        for c in range(nc):
            k = j * nc + c
            at = pl.multiple_of((lax.rem(h - j + nf, nf) * nc + c) * part, 128)
            copies.append(
                pltpu.make_async_copy(grads[k], x_all.at[:, pl.ds(at, part)], sems.at[k])
            )
    for copy in copies:
        copy.start()
    acc[...] = jnp.zeros_like(acc)
    total = mirrors[:, 0].astype(F32)
    for f in range(1, nf):
        total = total + mirrors[:, f].astype(F32)
    x_all[:, masters:] = flip(total.astype(BF).reshape(slots, feats))
    list_tiles(blocks, count[0], lists, 1, acc.shape[1] // tile - 1, 0, x_all.shape[1] // tile)
    for copy in copies:
        copy.wait()
    run_tiles(count[0], lists, values, 1, x_all, acc, tile)
    partial = acc[:, masters : masters + slots].astype(BF)
    held_push[...] = flip(partial).reshape(push_ref.shape)
    outs = [pltpu.make_async_copy(held_push, push_ref, sems.at[nf * nc + 1])]
    outs[0].start()
    held_back[...] = acc[:, :masters].astype(BF)
    outs.append(pltpu.make_async_copy(held_back, back_ref, sems.at[nf * nc + 2]))
    outs[1].start()
    for copy in outs:
        copy.wait()


def final_kernel(nf, nc, rep_ref, inc_ref, back_ref, *rest):
    selfs, out_ref = rest[:nf], rest[nf]
    h = lax.axis_index("feat")
    feats, width = selfs[0].shape
    part = width // nc
    slots = rep_ref.shape[1]
    inc = flip(inc_ref[...].reshape(slots, feats))
    for j in range(nf):
        for c in range(nc):
            at = pl.multiple_of((lax.rem(h - j + nf, nf) * nc + c) * part, 128)
            back = back_ref[:, pl.ds(at, part)].astype(F32)
            back = back + dot(inc, picks(rep_ref[...], at, part), 1, 1)
            own = selfs[j][:, c * part : (c + 1) * part].astype(F32)
            out_ref[:, pl.ds(at, part)] = (own + back).astype(BF)


def local(nd, nf, features, weights, tile_values, tile_blocks, tile_counts, replica, cotangent):
    feats, masters = features.shape
    wide = weights.shape[1]
    ntiles, tile, _ = tile_values.shape
    per = replica.shape[2]
    slots = nd * per
    width = masters // nf
    cols = masters + slots + tile
    nc = 2 if width % (2 * tile) == 0 else 1
    part = width // nc
    d = lax.axis_index("dom")
    sd = jax.ShapeDtypeStruct
    lists = [pltpu.SMEM((ntiles + GROUP,), jnp.int32)] * 3
    tile_flops = 2 * ntiles * feats * tile * tile

    def call(body, flops, args, specs, outs, scratch=(), grid=(), out_specs=None, alias={}, limit=None):
        return pl.pallas_call(
            body,
            grid=grid,
            in_specs=[full(a) if p is None else p for a, p in zip(args, specs, strict=True)],
            out_specs=out_specs or [full(o) for o in outs],
            out_shape=outs,
            scratch_shapes=list(scratch),
            input_output_aliases=alias,
            compiler_params=pltpu.CompilerParams(vmem_limit_bytes=limit),
            cost_estimate=cost(flops, 2 * sum(a.size for a in args)),
        )(*args)

    def to_peer(x, j):
        return lax.ppermute(x, "feat", [(i, (i + j) % nf) for i in range(nf)])

    def exchange(x, axes):
        flat = x.reshape(-1, per, feats)
        return lax.all_to_all(flat, axes, 0, 0, tiled=True).reshape(x.shape)

    def tile_scratch(nsems):
        return [
            pltpu.VMEM((feats, cols), F32),
            pltpu.VMEM((feats, masters + slots), BF),
            pltpu.VMEM(tile_values.shape, BF),
            *lists,
            pltpu.SemaphoreType.DMA((nsems,)),
        ]

    vec = sd((feats, width), BF)
    pull, rep, *x_halves = call(
        functools.partial(prep_kernel, nf),
        2 * slots * feats * masters,
        [features, replica],
        [None] * 2,
        [sd((nd, per, feats), BF), sd((1, slots), jnp.int32)] + [vec] * nf,
    )
    mirrors = exchange(pull, "dom")
    x_parts = [x_halves[0]] + [to_peer(x_halves[j], j) for j in range(1, nf)]

    blocks = tile_blocks.T
    chunk = sd((feats, part), BF)
    sums = pltpu.VMEM((feats, cols), F32)
    all_values = pltpu.VMEM(tile_values.shape, BF)
    pair = pltpu.SemaphoreType.DMA((2,))
    (own_sums,) = call(
        functools.partial(spread_own, tile),
        tile_flops,
        [blocks, tile_counts, features, tile_values],
        [SMEM, SMEM, ANY, ANY],
        [sd((feats, masters + slots), BF)],
        [sums, pltpu.VMEM((feats, masters), BF), all_values, *lists, pair],
    )
    own_part, push, *part_sends = call(
        functools.partial(spread_mirrors, nf, nc, tile),
        tile_flops // 4,
        [blocks, tile_counts, mirrors, tile_values, own_sums],
        [SMEM, SMEM, None, ANY, ANY],
        [vec, sd((nd, nf, per, feats), BF)] + [chunk] * ((nf - 1) * nc),
        [
            sums,
            pltpu.VMEM((feats, masters + slots), BF),
            pltpu.VMEM((feats, slots), BF),
            all_values,
            *lists,
            pltpu.SemaphoreType.DMA((4 + (nf - 1) * nc,)),
            pltpu.VMEM((feats, width), BF),
            pltpu.VMEM((nd, nf, per, feats), BF),
        ]
        + [pltpu.VMEM((feats, part), BF)] * ((nf - 1) * nc),
        out_specs=[ANY] * (2 + (nf - 1) * nc),
    )
    part_recv = [
        [to_peer(part_sends[(j - 1) * nc + c], j) for j in range(1, nf)]
        for c in range(nc)
    ]
    incoming = exchange(push, ("dom", "feat"))

    flat_w = weights.reshape(2 * wide, wide)
    wt = flat_w.T
    (z_own,) = call(
        functools.partial(own_term_kernel, nf),
        2 * wide * wide * width,
        [wt, *x_parts],
        [None] * (nf + 1),
        [sd((wide, width), F32)],
        [pltpu.VMEM((wide, width), BF)],
    )
    rows, grads, grad_own, grad_recv = [], [], [], []
    step = 256 if part % 256 == 0 else 128
    for c in range(nc):
        last = c + 1 == nc
        args = [rep, incoming, wt, flat_w, cotangent, z_own, own_part, *part_recv[c]]
        specs = [None] * 2 + [ANY] * (len(args) - 2)
        alias = {}
        if c:
            alias = {len(args) + 1: 1}
            alias |= {len(args) + 2 + j: 4 + nf + j for j in range(nf)}
            args += [pay, output, *selfs]
            specs += [None] + [ANY] * (1 + nf)
        outs = [
            sd((wide, part), BF),
            sd((wide, width), BF),
            sd((wide, part), BF),
            sd((nd, nf, per, feats) if last else (wide, slots), BF),
        ] + [chunk] * nf + [vec] * nf
        rows_c, output, g_c, pay, *res = call(
            functools.partial(dense_kernel, nf, nc, c),
            8 * wide * wide * part,
            args,
            specs,
            outs,
            [
                pltpu.VMEM((wide, wide), BF),
                pltpu.VMEM((2 * wide, wide), BF),
                pltpu.VMEM((wide, part), BF),
                pltpu.VMEM((wide, part), F32),
                pltpu.VMEM((wide, part), BF),
                pltpu.VMEM((nf, feats, part), BF),
                pltpu.VMEM((wide, part), BF),
                pltpu.VMEM((wide, part), BF),
                pltpu.VMEM((2 * wide, part), BF),
                pltpu.VMEM(outs[3].shape, BF),
                pltpu.SemaphoreType.DMA((nf + 4,)),
                pltpu.SemaphoreType.DMA((2 + (part // step) * (2 * nf + 2),)),
            ],
            (),
            [ANY] * len(outs),
            alias,
        )
        rows.append(rows_c)
        grads.append(g_c)
        grad_own.append(res[0])
        selfs = res[nf:]
        grad_recv.append([to_peer(res[j], j) for j in range(1, nf)])
    selfs = [selfs[0]] + [to_peer(selfs[j], j) for j in range(1, nf)]
    grad_mirrors = exchange(pay, ("dom", "feat"))

    keep, send = call(
        functools.partial(weight_kernel, nf, nc),
        4 * wide * wide * width,
        x_parts + rows + grads,
        [ANY] * (nf + 2 * nc),
        [sd((nf, feats, wide), F32), sd((nf, feats, wide), BF)],
        [pltpu.VMEM((2 * wide, wide), F32)]
        + [pltpu.VMEM((feats, width), BF)] * nf
        + [pltpu.VMEM((wide, part), BF)] * (2 * nc)
        + [pltpu.SemaphoreType.DMA((nf + 2 * nc,))],
    )

    flat_grads = grad_own + [grad_recv[c][j] for j in range(nf - 1) for c in range(nc)]
    back, push = call(
        functools.partial(back_kernel, nf, nc, tile),
        tile_flops,
        [blocks, tile_counts, grad_mirrors, tile_values, *flat_grads],
        [SMEM, SMEM, None, ANY] + [ANY] * (nf * nc),
        [sd((feats, masters), BF), sd((nd, per, feats), BF)],
        tile_scratch(nf * nc + 3)
        + [pltpu.VMEM((feats, masters), BF), pltpu.VMEM((nd, per, feats), BF)],
        out_specs=[ANY] * 2,
    )
    back_in = exchange(push, "dom")

    radices = radices_of(nd)

    def swap(x, b):
        return lax.ppermute(x, "dom", [(i, i ^ b) for i in range(nd)])

    sends = [send]
    for k, r in enumerate(radices):
        unit = unit_of(radices, k)
        cur = keep
        for m in range(1, r):
            cur = cur + swap(sends[m - 1], m * unit).astype(F32)
        if k + 1 == len(radices):
            break
        size = cur.shape[1] // radices[k + 1]
        digit = lax.rem(d // unit_of(radices, k + 1), radices[k + 1])
        pieces = [
            lax.dynamic_slice_in_dim(cur, (digit ^ m) * size, size, 1)
            for m in range(radices[k + 1])
        ]
        keep, sends = pieces[0], [piece.astype(BF) for piece in pieces[1:]]
    total = cur[0]
    for j in range(1, nf):
        total = total + to_peer(cur[j].astype(BF), j).astype(F32)
    total = total.astype(BF)
    for k in reversed(range(1, len(radices))):
        unit = unit_of(radices, k)
        others = [swap(total, m * unit) for m in range(1, radices[k])]
        total = jnp.concatenate([total, *others], 0)
    other = swap(total, 1)
    if total.shape[0] * 2 // nd % 8 == 0:
        (weight_grad,) = call(
            functools.partial(assemble_kernel, radices),
            0,
            [total, other],
            [None] * 2,
            [sd((2 * feats, wide), F32)],
            limit=SMALL,
        )
    else:
        total = jnp.concatenate([total, other], 0).reshape(nd, -1, wide)
        owners = jnp.arange(nd)
        place, rest = jnp.zeros_like(owners), owners
        for r in radices:
            place, rest = place * r + rest % r, rest // r
        held = jnp.zeros_like(owners).at[place].set(owners) ^ d
        numbers = jnp.array([relative(radices, m) for m in range(nd)])
        index = jnp.zeros_like(owners).at[numbers].set(jnp.arange(nd))[held]
        weight_grad = total[index].reshape(2 * feats, wide).astype(F32)
    weight_grad = weight_grad.reshape(2, feats, wide)

    (feature_grad,) = call(
        functools.partial(final_kernel, nf, nc),
        2 * slots * feats * masters,
        [rep, back_in, back, *selfs],
        [None] * (3 + nf),
        [sd((feats, masters), BF)],
        limit=SMALL,
    )
    return output, feature_grad, weight_grad


def solution(mesh):
    return jax.shard_map(
        functools.partial(local, mesh.shape["dom"], mesh.shape["feat"]),
        mesh=mesh,
        in_specs=(
            P("feat", "dom"),
            P(),
            P("dom", None, None),
            P("dom", None),
            P("dom"),
            P("dom", None, None),
            P(None, ("dom", "feat")),
        ),
        out_specs=(P(None, ("dom", "feat")), P("feat", "dom"), P(None, "feat", None)),
        check_vma=False,
    )
```

```python
import functools

import jax
import jax.numpy as jnp
from jax import lax
from jax.experimental import pallas as pl
from jax.experimental.pallas import tpu as pltpu
from jax.sharding import PartitionSpec as P

BF = jnp.bfloat16
F32 = jnp.float32
GROUP = 16
SMALL = 24 * 1024 * 1024


def dot(a, b, ca=1, cb=0):
    return lax.dot_general(a, b, (((ca,), (cb,)), ((), ())), preferred_element_type=F32)


def eye(n):
    rows = lax.broadcasted_iota(jnp.int32, (n, n), 0)
    cols = lax.broadcasted_iota(jnp.int32, (n, n), 1)
    return jnp.where(rows == cols, 1.0, 0.0).astype(BF)


def picks(slots, start, height):
    rows = lax.broadcasted_iota(jnp.int32, (height, slots.shape[1]), 0) + start
    return jnp.where(rows == slots, 1.0, 0.0).astype(BF)


def flip(x):
    return dot(eye(x.shape[1]), x, 1, 1).astype(BF)


SMEM = pl.BlockSpec(memory_space=pltpu.SMEM)
ANY = pl.BlockSpec(memory_space=pl.ANY)


def full(x):
    zeros = (0,) * len(x.shape)
    return pl.BlockSpec(x.shape, lambda *_: zeros)


def cost(flops, nbytes):
    return pl.CostEstimate(flops=int(flops), bytes_accessed=int(nbytes), transcendentals=0)


def block_of(n):
    return next(b for b in (512, 256, 128) if n % b == 0)


def list_tiles(blocks, count, lists, source_col, trash, low, high):
    tiles, sources, targets = lists

    def step(t, n):
        source = blocks[source_col, t]
        tiles[n] = t
        sources[n] = source - low
        targets[n] = blocks[1 - source_col, t]
        return n + jnp.logical_and(source >= low, source < high).astype(jnp.int32)

    n = lax.fori_loop(0, count, step, jnp.int32(0))
    for u in range(GROUP):
        tiles[n + u] = 0
        sources[n + u] = 0
        targets[n + u] = trash
    return n


def run_tiles(n, lists, values, tile_dim, x_all, acc, tile):
    tiles, sources, targets = lists

    def step(g, _):
        for u in range(GROUP):
            at = g * GROUP + u
            picked = column(x_all, sources[at], tile)
            part = dot(picked, values[tiles[at]], 1, tile_dim)
            col = pl.ds(pl.multiple_of(targets[at] * tile, tile), tile)
            acc[:, col] += part
        return 0

    lax.fori_loop(0, (n + GROUP - 1) // GROUP, step, 0)


def column(ref, block, tile):
    at = pl.multiple_of(block * tile, tile)
    return ref[:, pl.ds(at, tile)]


def prep_kernel(nf, x_ref, replica, pull_ref, rep_ref, *halves):
    rep_ref[...] = jnp.concatenate(
        [replica[0, p : p + 1, :] for p in range(replica.shape[1])], axis=1
    )
    h = lax.axis_index("feat")
    _, masters = x_ref.shape
    width = halves[0].shape[1]
    step = block_of(masters)
    total = None
    for at in range(0, masters, step):
        part = dot(x_ref[:, at : at + step], picks(rep_ref[...], at, step))
        total = part if total is None else total + part
    pull_ref[...] = flip(total.astype(BF)).reshape(pull_ref.shape)
    for j in range(nf):
        at = pl.multiple_of(lax.rem(h + j, nf) * width, 128)
        halves[j][...] = x_ref[:, pl.ds(at, width)]


def spread_own(tile, blocks, count, x_ref, values_ref, out_ref, acc, x, values, *rest):
    lists, sems = rest[:3], rest[3]
    masters = x.shape[1]
    copies = [
        pltpu.make_async_copy(x_ref, x, sems.at[0]),
        pltpu.make_async_copy(values_ref, values, sems.at[1]),
    ]
    for copy in copies:
        copy.start()
    acc[...] = jnp.zeros_like(acc)
    n = list_tiles(blocks, count[0], lists, 0, acc.shape[1] // tile - 1, 0, masters // tile)
    for copy in copies:
        copy.wait()
    run_tiles(n, lists, values, 0, x, acc, tile)
    out_ref[...] = acc[:, : out_ref.shape[1]].astype(BF)


def spread_mirrors(nf, nc, tile, blocks, count, mirrors, values_ref, own_ref, *rest):
    part_ref, push_ref = rest[:2]
    sends = rest[2 : 2 + (nf - 1) * nc]
    acc, own, x, values, *lists, sems, held_part, held_push = rest[2 + (nf - 1) * nc :][:10]
    held_sends = rest[2 + (nf - 1) * nc :][10:]
    h = lax.axis_index("feat")
    feats, width = part_ref.shape
    outs = []

    def put(src, dst):
        outs.append(pltpu.make_async_copy(src, dst, sems.at[2 + len(outs)]))
        outs[-1].start()

    slots = x.shape[1]
    masters = own.shape[1] - slots
    copies = [
        pltpu.make_async_copy(values_ref, values, sems.at[0]),
        pltpu.make_async_copy(own_ref, own, sems.at[1]),
    ]
    for copy in copies:
        copy.start()
    acc[...] = jnp.zeros_like(acc)
    x[...] = flip(mirrors[...].reshape(slots, feats))
    low = masters // tile
    n = list_tiles(
        blocks, count[0], lists, 0, acc.shape[1] // tile - 1, low, own.shape[1] // tile
    )
    for copy in copies:
        copy.wait()
    run_tiles(n, lists, values, 0, x, acc, tile)

    def total(at, size):
        return (own[:, pl.ds(at, size)].astype(F32) + acc[:, pl.ds(at, size)]).astype(BF)

    part = width // nc
    for j in range(1, nf):
        for c in range(nc):
            at = pl.multiple_of(lax.rem(h + j, nf) * width + c * part, 128)
            held_sends[(j - 1) * nc + c][...] = total(at, part)
            put(held_sends[(j - 1) * nc + c], sends[(j - 1) * nc + c])
    push = flip(total(masters, slots))
    push = push.reshape(push_ref.shape[0], push_ref.shape[2], feats)
    for f in range(nf):
        held_push[:, f] = push
    put(held_push, push_ref)
    held_part[...] = total(pl.multiple_of(h * width, 128), width)
    put(held_part, part_ref)
    for copy in outs:
        copy.wait()


def own_term_kernel(nf, wt_ref, *refs):
    xs, out_ref, rows = refs[:nf], refs[nf], refs[nf + 1]
    h = lax.axis_index("feat")
    feats, width = xs[0].shape
    for j in range(nf):
        f = lax.rem(h - j + nf, nf)
        rows[pl.ds(pl.multiple_of(f * feats, feats), feats), :] = xs[j][...]
    step = 512 if width % 512 == 0 else 128
    for b in range(0, width, step):
        out_ref[:, b : b + step] = dot(wt_ref[:, : rows.shape[0]], rows[:, b : b + step])


def dense_kernel(nf, nc, c, *refs):
    rep_ref, inc_ref, wt_hbm, w_hbm, cot_hbm, z_hbm = refs[:6]
    parts = refs[6 : 6 + nf]
    refs = refs[6 + nf :]
    if c:
        pay_in = refs[0]
        refs = refs[2 + nf :]
    agg_hbm, out_hbm, g_hbm, pay_ref = refs[:4]
    grads, selfs = refs[4 : 4 + nf], refs[4 + nf : 4 + 2 * nf]
    wt, w, cot, z_own, rows, terms, out, g_all, both, held_pay, in_sems, out_sems = refs[4 + 2 * nf :]
    h = lax.axis_index("feat")
    feats, part = grads[0].shape
    wide = w.shape[1]
    slots = rep_ref.shape[1]
    chunk = pl.ds(c * part, part)

    def place(f):
        return pl.ds(pl.multiple_of(f * feats, feats), feats)

    early, late = [], []
    for j in range(nf):
        term = parts[j].at[:, chunk] if j == 0 else parts[j]
        early.append(pltpu.make_async_copy(term, terms.at[j], in_sems.at[j]))
    late.append(pltpu.make_async_copy(wt_hbm.at[:, wide:], wt, in_sems.at[nf]))
    late.append(pltpu.make_async_copy(z_hbm.at[:, chunk], z_own, in_sems.at[nf + 1]))
    late.append(pltpu.make_async_copy(cot_hbm.at[:, chunk], cot, in_sems.at[nf + 2]))
    late.append(pltpu.make_async_copy(w_hbm, w, in_sems.at[nf + 3]))
    for copy in early + late:
        copy.start()
    pick = picks(rep_ref[...], (h * nc + c) * part, part)
    incs = [flip(inc_ref[:, lax.rem(h - j + nf, nf)].reshape(slots, feats)) for j in range(nf)]
    adds = [dot(inc, pick, 1, 1) for inc in incs]
    for copy in early:
        copy.wait()
    for j in range(nf):
        f = lax.rem(h - j + nf, nf)
        total = terms[j].astype(F32) + adds[j]
        rows[place(f), :] = total.astype(BF)
    out_copies = []

    def put(src, dst):
        copy = pltpu.make_async_copy(src, dst, out_sems.at[len(out_copies)])
        copy.start()
        out_copies.append(copy)

    put(rows, agg_hbm)
    for copy in late:
        copy.wait()
    step = 256 if part % 256 == 0 else 128
    for b in range(0, part, step):
        cols = slice(b, b + step)
        z = z_own[:, cols] + dot(wt[...], rows[:, cols])
        s = 0.5 + 0.5 * jnp.tanh(0.5 * z)
        out[:, cols] = (z * s).astype(BF)
        g = (cot[:, cols].astype(F32) * (s * (1.0 + z * (1.0 - s)))).astype(BF)
        g_all[:, cols] = g
        both[:, cols] = dot(w[...], g).astype(BF)
        for j in range(nf):
            at = lax.rem(h + j, nf)
            peer = pl.ds(pl.multiple_of(wide + at * feats, feats), feats)
            put(both.at[peer, cols], grads[j].at[:, cols])
            put(both.at[place(at), cols], selfs[j].at[:, pl.ds(c * part + b, step)])
        put(g_all.at[:, cols], g_hbm.at[:, cols])
        put(out.at[:, cols], out_hbm.at[:, pl.ds(c * part + b, step)])
    pay = dot(both[wide:, :], pick)
    if c:
        pay = pay + pay_in[...].astype(F32)
    pay = pay.astype(BF)
    if c + 1 < nc:
        held_pay[...] = pay
    else:
        for f in range(nf):
            mine = flip(pay[f * feats : (f + 1) * feats])
            held_pay[:, f] = mine.reshape(pay_ref.shape[0], pay_ref.shape[2], feats)
    put(held_pay, pay_ref)
    for copy in out_copies:
        copy.wait()


def weight_kernel(nf, nc, *refs):
    ins = refs[: nf + 2 * nc]
    keep_ref, send_ref, acc = refs[nf + 2 * nc : nf + 2 * nc + 3]
    held, sems = refs[nf + 2 * nc + 3 : -1], refs[-1]
    h = lax.axis_index("feat")
    bit = lax.rem(lax.axis_index("dom"), 2)
    wide = acc.shape[1]
    feats = wide // nf
    copies = [pltpu.make_async_copy(a, b, sems.at[k]) for k, (a, b) in enumerate(zip(ins, held))]
    order = [[nf + nc + c, nf + c] for c in range(nc)]
    order[0] += list(range(nf))
    for group in order:
        for k in group:
            copies[k].start()
    xs, aggs, grads = held[:nf], held[nf : nf + nc], held[nf + nc :]
    part = grads[0].shape[1]
    for c in range(nc):
        for k in order[c]:
            copies[k].wait()
        terms = [(pl.ds(wide, wide), aggs[c][...])]
        for j in range(nf):
            at = pl.multiple_of(lax.rem(h - j + nf, nf) * feats, feats)
            terms.append((pl.ds(at, feats), xs[j][:, c * part : (c + 1) * part]))
        for at, left in terms:
            term = dot(left, grads[c][...], 1, 1)
            acc[at, :] = term if c == 0 else acc[at, :] + term
    for j in range(nf):
        at = lax.rem(h + j, nf) * feats
        keep_ref[j] = acc[pl.ds(pl.multiple_of(bit * wide + at, feats), feats), :]
        send_ref[j] = acc[pl.ds(pl.multiple_of((1 - bit) * wide + at, feats), feats), :].astype(BF)


def radices_of(n):
    radices = [2] * min(2, n.bit_length() - 1)
    n //= 1 << len(radices)
    while n > 1:
        radices.append(4 if n % 4 == 0 else 2)
        n //= radices[-1]
    return tuple(radices)


def unit_of(radices, k):
    unit = 1
    for r in radices[:k]:
        unit *= r
    return unit


def relative(radices, m):
    number = 0
    size = unit_of(radices, len(radices))
    for k, r in enumerate(radices):
        size //= r
        number += (m // size) % r * unit_of(radices, k)
    return number


def assemble_kernel(radices, own_ref, other_ref, out_ref):
    d = lax.axis_index("dom")
    nd = 1
    for r in radices:
        nd *= r
    rows = out_ref.shape[0] // nd
    half = nd // 2
    for m in range(nd):
        at, owner, height = 0, d ^ relative(radices, m), out_ref.shape[0]
        for r in radices:
            height //= r
            at = at + lax.rem(owner, r) * height
            owner = owner // r
        ref, k = (own_ref, m) if m < half else (other_ref, m - half)
        piece = ref[k * rows : (k + 1) * rows, :]
        out_ref[pl.ds(pl.multiple_of(at, rows), rows), :] = piece.astype(F32)


def back_kernel(nf, nc, tile, blocks, count, mirrors, values_ref, *rest):
    grads = rest[: nf * nc]
    back_ref, push_ref, acc, x_all, values, tiles, sources, targets, sems = rest[nf * nc : -2]
    held_back, held_push = rest[-2:]
    lists = (tiles, sources, targets)
    h = lax.axis_index("feat")
    feats, masters = back_ref.shape
    slots = x_all.shape[1] - masters
    part = masters // nf // nc
    copies = [pltpu.make_async_copy(values_ref, values, sems.at[nf * nc])]
    for j in range(nf):
        for c in range(nc):
            k = j * nc + c
            at = pl.multiple_of((lax.rem(h - j + nf, nf) * nc + c) * part, 128)
            copies.append(
                pltpu.make_async_copy(grads[k], x_all.at[:, pl.ds(at, part)], sems.at[k])
            )
    for copy in copies:
        copy.start()
    acc[...] = jnp.zeros_like(acc)
    total = mirrors[:, 0].astype(F32)
    for f in range(1, nf):
        total = total + mirrors[:, f].astype(F32)
    x_all[:, masters:] = flip(total.astype(BF).reshape(slots, feats))
    list_tiles(blocks, count[0], lists, 1, acc.shape[1] // tile - 1, 0, x_all.shape[1] // tile)
    for copy in copies:
        copy.wait()
    run_tiles(count[0], lists, values, 1, x_all, acc, tile)
    partial = acc[:, masters : masters + slots].astype(BF)
    held_push[...] = flip(partial).reshape(push_ref.shape)
    outs = [pltpu.make_async_copy(held_push, push_ref, sems.at[nf * nc + 1])]
    outs[0].start()
    held_back[...] = acc[:, :masters].astype(BF)
    outs.append(pltpu.make_async_copy(held_back, back_ref, sems.at[nf * nc + 2]))
    outs[1].start()
    for copy in outs:
        copy.wait()


def final_kernel(nf, nc, rep_ref, inc_ref, back_ref, *rest):
    selfs, out_ref = rest[:nf], rest[nf]
    h = lax.axis_index("feat")
    feats, width = selfs[0].shape
    part = width // nc
    slots = rep_ref.shape[1]
    inc = flip(inc_ref[...].reshape(slots, feats))
    for j in range(nf):
        for c in range(nc):
            at = pl.multiple_of((lax.rem(h - j + nf, nf) * nc + c) * part, 128)
            back = back_ref[:, pl.ds(at, part)].astype(F32)
            back = back + dot(inc, picks(rep_ref[...], at, part), 1, 1)
            own = selfs[j][:, c * part : (c + 1) * part].astype(F32)
            out_ref[:, pl.ds(at, part)] = (own + back).astype(BF)


def local(nd, nf, features, weights, tile_values, tile_blocks, tile_counts, replica, cotangent):
    feats, masters = features.shape
    wide = weights.shape[1]
    ntiles, tile, _ = tile_values.shape
    per = replica.shape[2]
    slots = nd * per
    width = masters // nf
    cols = masters + slots + tile
    nc = 2 if width % (2 * tile) == 0 else 1
    part = width // nc
    d = lax.axis_index("dom")
    sd = jax.ShapeDtypeStruct
    lists = [pltpu.SMEM((ntiles + GROUP,), jnp.int32)] * 3
    tile_flops = 2 * ntiles * feats * tile * tile

    def call(body, flops, args, specs, outs, scratch=(), grid=(), out_specs=None, alias={}, limit=None):
        return pl.pallas_call(
            body,
            grid=grid,
            in_specs=[full(a) if p is None else p for a, p in zip(args, specs, strict=True)],
            out_specs=out_specs or [full(o) for o in outs],
            out_shape=outs,
            scratch_shapes=list(scratch),
            input_output_aliases=alias,
            compiler_params=pltpu.CompilerParams(vmem_limit_bytes=limit),
            cost_estimate=cost(flops, 2 * sum(a.size for a in args)),
        )(*args)

    def to_peer(x, j):
        return lax.ppermute(x, "feat", [(i, (i + j) % nf) for i in range(nf)])

    def exchange(x, axes):
        flat = x.reshape(-1, per, feats)
        return lax.all_to_all(flat, axes, 0, 0, tiled=True).reshape(x.shape)

    def tile_scratch(nsems):
        return [
            pltpu.VMEM((feats, cols), F32),
            pltpu.VMEM((feats, masters + slots), BF),
            pltpu.VMEM(tile_values.shape, BF),
            *lists,
            pltpu.SemaphoreType.DMA((nsems,)),
        ]

    vec = sd((feats, width), BF)
    pull, rep, *x_halves = call(
        functools.partial(prep_kernel, nf),
        2 * slots * feats * masters,
        [features, replica],
        [None] * 2,
        [sd((nd, per, feats), BF), sd((1, slots), jnp.int32)] + [vec] * nf,
    )
    mirrors = exchange(pull, "dom")
    x_parts = [x_halves[0]] + [to_peer(x_halves[j], j) for j in range(1, nf)]

    blocks = tile_blocks.T
    chunk = sd((feats, part), BF)
    sums = pltpu.VMEM((feats, cols), F32)
    all_values = pltpu.VMEM(tile_values.shape, BF)
    pair = pltpu.SemaphoreType.DMA((2,))
    (own_sums,) = call(
        functools.partial(spread_own, tile),
        tile_flops,
        [blocks, tile_counts, features, tile_values],
        [SMEM, SMEM, ANY, ANY],
        [sd((feats, masters + slots), BF)],
        [sums, pltpu.VMEM((feats, masters), BF), all_values, *lists, pair],
    )
    own_part, push, *part_sends = call(
        functools.partial(spread_mirrors, nf, nc, tile),
        tile_flops // 4,
        [blocks, tile_counts, mirrors, tile_values, own_sums],
        [SMEM, SMEM, None, ANY, ANY],
        [vec, sd((nd, nf, per, feats), BF)] + [chunk] * ((nf - 1) * nc),
        [
            sums,
            pltpu.VMEM((feats, masters + slots), BF),
            pltpu.VMEM((feats, slots), BF),
            all_values,
            *lists,
            pltpu.SemaphoreType.DMA((4 + (nf - 1) * nc,)),
            pltpu.VMEM((feats, width), BF),
            pltpu.VMEM((nd, nf, per, feats), BF),
        ]
        + [pltpu.VMEM((feats, part), BF)] * ((nf - 1) * nc),
        out_specs=[ANY] * (2 + (nf - 1) * nc),
    )
    part_recv = [
        [to_peer(part_sends[(j - 1) * nc + c], j) for j in range(1, nf)]
        for c in range(nc)
    ]
    incoming = exchange(push, ("dom", "feat"))

    flat_w = weights.reshape(2 * wide, wide)
    wt = flat_w.T
    (z_own,) = call(
        functools.partial(own_term_kernel, nf),
        2 * wide * wide * width,
        [wt, *x_parts],
        [None] * (nf + 1),
        [sd((wide, width), F32)],
        [pltpu.VMEM((wide, width), BF)],
    )
    rows, grads, grad_own, grad_recv = [], [], [], []
    step = 256 if part % 256 == 0 else 128
    for c in range(nc):
        last = c + 1 == nc
        args = [rep, incoming, wt, flat_w, cotangent, z_own, own_part, *part_recv[c]]
        specs = [None] * 2 + [ANY] * (len(args) - 2)
        alias = {}
        if c:
            alias = {len(args) + 1: 1}
            alias |= {len(args) + 2 + j: 4 + nf + j for j in range(nf)}
            args += [pay, output, *selfs]
            specs += [None] + [ANY] * (1 + nf)
        outs = [
            sd((wide, part), BF),
            sd((wide, width), BF),
            sd((wide, part), BF),
            sd((nd, nf, per, feats) if last else (wide, slots), BF),
        ] + [chunk] * nf + [vec] * nf
        rows_c, output, g_c, pay, *res = call(
            functools.partial(dense_kernel, nf, nc, c),
            8 * wide * wide * part,
            args,
            specs,
            outs,
            [
                pltpu.VMEM((wide, wide), BF),
                pltpu.VMEM((2 * wide, wide), BF),
                pltpu.VMEM((wide, part), BF),
                pltpu.VMEM((wide, part), F32),
                pltpu.VMEM((wide, part), BF),
                pltpu.VMEM((nf, feats, part), BF),
                pltpu.VMEM((wide, part), BF),
                pltpu.VMEM((wide, part), BF),
                pltpu.VMEM((2 * wide, part), BF),
                pltpu.VMEM(outs[3].shape, BF),
                pltpu.SemaphoreType.DMA((nf + 4,)),
                pltpu.SemaphoreType.DMA((2 + (part // step) * (2 * nf + 2),)),
            ],
            (),
            [ANY] * len(outs),
            alias,
        )
        rows.append(rows_c)
        grads.append(g_c)
        grad_own.append(res[0])
        selfs = res[nf:]
        grad_recv.append([to_peer(res[j], j) for j in range(1, nf)])
    selfs = [selfs[0]] + [to_peer(selfs[j], j) for j in range(1, nf)]
    grad_mirrors = exchange(pay, ("dom", "feat"))

    keep, send = call(
        functools.partial(weight_kernel, nf, nc),
        4 * wide * wide * width,
        x_parts + rows + grads,
        [ANY] * (nf + 2 * nc),
        [sd((nf, feats, wide), F32), sd((nf, feats, wide), BF)],
        [pltpu.VMEM((2 * wide, wide), F32)]
        + [pltpu.VMEM((feats, width), BF)] * nf
        + [pltpu.VMEM((wide, part), BF)] * (2 * nc)
        + [pltpu.SemaphoreType.DMA((nf + 2 * nc,))],
    )

    flat_grads = grad_own + [grad_recv[c][j] for j in range(nf - 1) for c in range(nc)]
    back, push = call(
        functools.partial(back_kernel, nf, nc, tile),
        tile_flops,
        [blocks, tile_counts, grad_mirrors, tile_values, *flat_grads],
        [SMEM, SMEM, None, ANY] + [ANY] * (nf * nc),
        [sd((feats, masters), BF), sd((nd, per, feats), BF)],
        tile_scratch(nf * nc + 3)
        + [pltpu.VMEM((feats, masters), BF), pltpu.VMEM((nd, per, feats), BF)],
        out_specs=[ANY] * 2,
    )
    back_in = exchange(push, "dom")

    radices = radices_of(nd)

    def swap(x, b):
        return lax.ppermute(x, "dom", [(i, i ^ b) for i in range(nd)])

    sends = [send]
    for k, r in enumerate(radices):
        unit = unit_of(radices, k)
        terms = [keep] + [swap(sends[m - 1], m * unit) for m in range(1, r)]
        if k + 1 == len(radices):
            break
        size = keep.shape[1] // radices[k + 1]
        digit = lax.rem(d // unit_of(radices, k + 1), radices[k + 1])
        pieces = []
        for m in range(radices[k + 1]):
            cuts = [lax.dynamic_slice_in_dim(t, (digit ^ m) * size, size, 1) for t in terms]
            pieces.append(sum(cut.astype(F32) for cut in cuts))
        keep, sends = pieces[0], [piece.astype(BF) for piece in pieces[1:]]
    cur = sum(term.astype(F32) for term in terms)
    total = cur[0]
    for j in range(1, nf):
        total = total + to_peer(cur[j].astype(BF), j).astype(F32)
    total = total.astype(BF)
    for k in reversed(range(1, len(radices))):
        unit = unit_of(radices, k)
        others = [swap(total, m * unit) for m in range(1, radices[k])]
        total = jnp.concatenate([total, *others], 0)
    other = swap(total, 1)
    if total.shape[0] * 2 // nd % 8 == 0:
        (weight_grad,) = call(
            functools.partial(assemble_kernel, radices),
            0,
            [total, other],
            [None] * 2,
            [sd((2 * feats, wide), F32)],
            limit=SMALL,
        )
    else:
        total = jnp.concatenate([total, other], 0).reshape(nd, -1, wide)
        owners = jnp.arange(nd)
        place, rest = jnp.zeros_like(owners), owners
        for r in radices:
            place, rest = place * r + rest % r, rest // r
        held = jnp.zeros_like(owners).at[place].set(owners) ^ d
        numbers = jnp.array([relative(radices, m) for m in range(nd)])
        index = jnp.zeros_like(owners).at[numbers].set(jnp.arange(nd))[held]
        weight_grad = total[index].reshape(2 * feats, wide).astype(F32)
    weight_grad = weight_grad.reshape(2, feats, wide)

    (feature_grad,) = call(
        functools.partial(final_kernel, nf, nc),
        2 * slots * feats * masters,
        [rep, back_in, back, *selfs],
        [None] * (3 + nf),
        [sd((feats, masters), BF)],
        limit=SMALL,
    )
    return output, feature_grad, weight_grad


def solution(mesh):
    return jax.shard_map(
        functools.partial(local, mesh.shape["dom"], mesh.shape["feat"]),
        mesh=mesh,
        in_specs=(
            P("feat", "dom"),
            P(),
            P("dom", None, None),
            P("dom", None),
            P("dom"),
            P("dom", None, None),
            P(None, ("dom", "feat")),
        ),
        out_specs=(P(None, ("dom", "feat")), P("feat", "dom"), P(None, "feat", None)),
        check_vma=False,
    )
```
